128 devices in a mesh: img: 8 (over y, core), cell: 16 (over z, x).
Axes of the slice: x: 4, y: 4, z: 4, core: 2. Of those that a mesh axis runs over, the one named last changes fastest.
Arguments:
- attributes: float32 [59, 1048576], P(None, ('img', 'cell')), may hold values from -5 to 2, as said below
- camera: float32 [3, 3], replicated, may hold values from -6 to 5, as said below
- target: float32 [3, 256, 4096], P(None, 'img', 'cell'), may hold values from 0 to 1
- visible_index: int32 [128, 8192], P(('img', 'cell')), may hold values from 0 to 8191
- tile_lists: int32 [16, 256, 128], P('img', 'cell'), may hold values from 0 to 8191
- tile_len: int32 [16, 256], P('img', 'cell'), may hold values from 16 to 128
Outputs:
- gradient: float32 [59, 1048576], P(None, ('img', 'cell'))
The draws below stay inside these ranges and needn't reach their ends.
Inputs may be any that keep to these rules, and one draw needn't show every extreme that they name: `attributes`: rows 0 to 2 (positions) lie within [-1, 1]. `camera`: row 2, the eye, lies 4 or more from the anchor.
All inputs are finite; a program needn't handle non-finite values.
Results may differ from the reference program's by a relative error of at most 0.0003.
Values sent between devices are 32-bit elements; how exact they have to be, the bound alone decides.
A program may use at most 64 MiB of HBM per device.

```python
import math
import jax
import jax.numpy as jnp
from jax import lax

TILE = 16
LIST = 128
PH = 32
PW = 256
G_DEV = 8192
CAP = 64
H = 256
W = 4096
TY = 16
TX = 256
GAUSS = 1048576
VIS = 8192
N_CELL = 16
DEVICES = 128


def draw_attributes(key, part):
    subkeys = jax.random.split(jax.random.fold_in(key, 11), 5)
    positions = jax.random.uniform(subkeys[0], (3, GAUSS), jnp.float32, -1.0, 1.0)
    rotations = jax.random.uniform(subkeys[2], (4, GAUSS), jnp.float32, -2.0, 2.0)
    opacity = jax.random.uniform(subkeys[3], (1, GAUSS), jnp.float32, -4.5, -1.5)
    log_scale = jax.random.uniform(subkeys[1], (3, GAUSS), jnp.float32, -1.2, 0.2)
    harmonics = jax.random.uniform(subkeys[4], (48, GAUSS), jnp.float32, -0.6, 0.6)
    return jnp.concatenate([positions, log_scale, rotations, opacity, harmonics])


def draw_camera(key, part):
    subkeys = jax.random.split(jax.random.fold_in(key, 23), 2)
    projection = jax.random.uniform(subkeys[0], (2, 3), jnp.float32, -5.0, 5.0)
    viewer = jnp.array([0.0, 0.0, -5.0], jnp.float32) + jax.random.uniform(subkeys[1], (3,), jnp.float32, -1.0, 1.0)
    return jnp.concatenate([projection, viewer[None, :]])


def set_ends(values, rng, low, high):
    place = [jax.random.randint(jax.random.fold_in(rng, axis), (), 0, length) for axis, length in enumerate(values.shape)]
    main_axis = values.shape.index(max(values.shape))
    neighbour = place[:main_axis] + [(place[main_axis] + 1) % values.shape[main_axis]] + place[main_axis + 1:]
    return values.at[tuple(place)].set(low).at[tuple(neighbour)].set(high)


def block_levels(stream_key, shape, shards, least, top_value):
    loudness, own = 1.0, jax.random.fold_in(stream_key, 6)
    for dim, parts in shards:
        draws = jnp.exp(jax.random.uniform(jax.random.fold_in(own, dim), (parts,), jnp.float32, least / len(shards), top_value / len(shards)))
        loudness = loudness * jnp.repeat(draws, shape[dim] // parts).reshape([-1 if axis == dim else 1 for axis in range(len(shape))])
    return loudness


def setup_inputs(seed: int = 0) -> dict:
    splits = jax.random.split(jax.random.key(seed), 7)
    attributes = draw_attributes(jax.random.fold_in(splits[6], 71), 0)
    camera = draw_camera(jax.random.fold_in(splits[6], 71), 0)
    target = jnp.clip(1.0 * jax.random.uniform(splits[2], (3, H, W), jnp.float32) ** block_levels(splits[2], (3, H, W), ((1, 8), (2, 16)), -0.2, 0.2), 0.0, 1.0)
    visible_index = set_ends(jax.random.randint(splits[3], (DEVICES, VIS), 0, G_DEV), jax.random.fold_in(splits[3], 1), 0, G_DEV - 1).astype(jnp.int32)
    tile_lists = set_ends(jax.random.randint(splits[4], (TY, TX, LIST), 0, VIS), jax.random.fold_in(splits[4], 1), 0, VIS - 1).astype(jnp.int32)
    tile_len = set_ends(jax.random.randint(splits[5], (TY, TX), LIST // 8, LIST + 1), jax.random.fold_in(splits[5], 1), LIST // 8, LIST).astype(jnp.int32)
    return {"attributes": attributes, "camera": camera, "target": target, "visible_index": visible_index, "tile_lists": tile_lists, "tile_len": tile_len}


WEIGHT_SSIM = 0.2
SMOOTHING = 0.01
STAB_ONE = 0.0001
STAB_TWO = 0.0009
BLUR_SIGMA = 1.5
SH_ZERO = 0.28209479177387814
SH_ONE = 0.4886025119029199
SH_TWO = (1.0925484305920792, -1.0925484305920792, 0.31539156525252005, -1.0925484305920792, 0.5462742152960396)
SH_THREE = (-0.5900435899266435, 2.890611442640554, -0.4570457994644658, 0.3731763325901154, -0.4570457994644658, 1.445305721320277, -0.5900435899266435)

def harmonic_basis(unit_x, unit_y, unit_z):
    unit_xx = unit_x * unit_x
    unit_yy = unit_y * unit_y
    unit_zz = unit_z * unit_z
    return [SH_ZERO + 0.0 * unit_x, -SH_ONE * unit_y, SH_ONE * unit_z, -SH_ONE * unit_x, SH_TWO[0] * unit_x * unit_y, SH_TWO[1] * unit_y * unit_z, SH_TWO[2] * (2.0 * unit_zz - unit_xx - unit_yy), SH_TWO[3] * unit_x * unit_z, SH_TWO[4] * (unit_xx - unit_yy), SH_THREE[0] * unit_y * (3.0 * unit_xx - unit_yy), SH_THREE[1] * unit_x * unit_y * unit_z, SH_THREE[2] * unit_y * (4.0 * unit_zz - unit_xx - unit_yy), SH_THREE[3] * unit_z * (2.0 * unit_zz - 3.0 * unit_xx - 3.0 * unit_yy), SH_THREE[4] * unit_x * (4.0 * unit_zz - unit_xx - unit_yy), SH_THREE[5] * unit_z * (unit_xx - unit_yy), SH_THREE[6] * unit_x * (unit_xx - 3.0 * unit_yy)]

def project_rows(attr_rows, camera):
    positions = [attr_rows[number] for number in range(3)]
    scales = [jnp.exp(attr_rows[3 + number]) for number in range(3)]
    quat_w = 1.5 + jnp.tanh(attr_rows[6])
    quat_x = attr_rows[7]
    quat_y = attr_rows[8]
    quat_z = attr_rows[9]
    length = jnp.sqrt(quat_w * quat_w + quat_x * quat_x + quat_y * quat_y + quat_z * quat_z)
    quat_w, quat_x, quat_y, quat_z = (quat_w / length, quat_x / length, quat_y / length, quat_z / length)
    rotation = [[1.0 - 2.0 * (quat_y * quat_y + quat_z * quat_z), 2.0 * (quat_x * quat_y - quat_w * quat_z), 2.0 * (quat_x * quat_z + quat_w * quat_y)], [2.0 * (quat_x * quat_y + quat_w * quat_z), 1.0 - 2.0 * (quat_x * quat_x + quat_z * quat_z), 2.0 * (quat_y * quat_z - quat_w * quat_x)], [2.0 * (quat_x * quat_z - quat_w * quat_y), 2.0 * (quat_y * quat_z + quat_w * quat_x), 1.0 - 2.0 * (quat_x * quat_x + quat_y * quat_y)]]
    screen_axes = [[sum((camera[screen_axis, world_axis] * rotation[world_axis][scale_axis] for world_axis in range(3))) * scales[scale_axis] for scale_axis in range(3)] for screen_axis in range(2)]
    cov_first = sum((screen_axes[0][scale_axis] * screen_axes[0][scale_axis] for scale_axis in range(3))) + 0.3
    cov_mixed = sum((screen_axes[0][scale_axis] * screen_axes[1][scale_axis] for scale_axis in range(3)))
    cov_second = sum((screen_axes[1][scale_axis] * screen_axes[1][scale_axis] for scale_axis in range(3))) + 0.3
    determinant = cov_first * cov_second - cov_mixed * cov_mixed
    centers = [8.0 + 7.0 * jnp.sin(sum((camera[screen_axis, world_axis] * positions[world_axis] for world_axis in range(3))) / 3.0) for screen_axis in range(2)]
    offsets = [positions[world_axis] - camera[2, world_axis] for world_axis in range(3)]
    distance = jnp.sqrt(offsets[0] * offsets[0] + offsets[1] * offsets[1] + offsets[2] * offsets[2])
    basis = harmonic_basis(offsets[0] / distance, offsets[1] / distance, offsets[2] / distance)
    harmonics = attr_rows[11:].reshape((3, 16) + attr_rows.shape[1:])
    colours = [0.5 + sum((basis[term] * harmonics[channel, term] for term in range(16))) for channel in range(3)]
    opacity = jax.nn.sigmoid(attr_rows[10])
    return jnp.stack(centers + [cov_second / determinant, -cov_mixed / determinant, cov_first / determinant, opacity] + colours)

def render_block(tile_feats, live_mask):
    pixels = jnp.arange(TILE * TILE, dtype=jnp.int32)
    pixel_x = (pixels % TILE).astype(jnp.float32) + 0.5
    pixel_y = (pixels // TILE).astype(jnp.float32) + 0.5
    delta_x = pixel_x[None, None, :] - tile_feats[0][:, :, None]
    delta_y = pixel_y[None, None, :] - tile_feats[1][:, :, None]
    exponent = -0.5 * (tile_feats[2][:, :, None] * delta_x * delta_x + 2.0 * tile_feats[3][:, :, None] * delta_x * delta_y + tile_feats[4][:, :, None] * delta_y * delta_y)
    opacity_map = (live_mask * tile_feats[5])[:, :, None] * jnp.exp(exponent)
    log_keep = jnp.log1p(-opacity_map)
    before = jnp.cumsum(log_keep, axis=1) - log_keep
    weight = jnp.exp(before) * opacity_map
    return jnp.einsum('cbk,bkp->cbp', tile_feats[6:9], weight, precision=lax.Precision.HIGHEST)

def render_pair(block_pair):
    return render_block(block_pair[0], block_pair[1])

def blur_taps():
    offsets = jnp.arange(11, dtype=jnp.float32) - 5.0
    taps = jnp.exp(-offsets * offsets / (2.0 * BLUR_SIGMA * BLUR_SIGMA))
    return taps / jnp.sum(taps)

def blur_image(image):
    taps = blur_taps()
    height = image.shape[1]
    breadth = image.shape[2]
    padded = jnp.pad(image, ((0, 0), (5, 5), (5, 5)))
    rows_done = sum((taps[offset] * padded[:, offset:offset + height, :] for offset in range(11)))
    return sum((taps[offset] * rows_done[:, :, offset:offset + breadth] for offset in range(11)))

def ssim_value(mean_render, mean_target, square_render, square_target, cross_term):
    spread_render = square_render - mean_render * mean_render
    spread_target = square_target - mean_target * mean_target
    covariance = cross_term - mean_render * mean_target
    upper = (2.0 * mean_render * mean_target + STAB_ONE) * (2.0 * covariance + STAB_TWO)
    lower = (mean_render * mean_render + mean_target * mean_target + STAB_ONE) * (spread_render + spread_target + STAB_TWO)
    return upper / lower

def image_loss(image, target):
    filtered = blur_image(jnp.concatenate([image, target, image * image, target * target, image * target]))
    mean_render, mean_target, square_render, square_target, cross_term = jnp.split(filtered, 5)
    similarity = ssim_value(mean_render, mean_target, square_render, square_target, cross_term)
    difference = image - target
    return jnp.sum((1.0 - WEIGHT_SSIM) * jnp.sqrt(difference * difference + SMOOTHING * SMOOTHING) + WEIGHT_SSIM * (1.0 - similarity))

def reference(attributes, camera, target, visible_index, tile_lists, tile_len):
    owner_of = jnp.arange(VIS, dtype=jnp.int32) // CAP
    global_ids = (owner_of[None, :] * G_DEV + visible_index).reshape(-1).astype(jnp.int32)
    tiles_down = PH // TILE
    tiles_across = PW // TILE
    tile_group = ((jnp.arange(TY, dtype=jnp.int32) // tiles_down)[:, None] * N_CELL + (jnp.arange(TX, dtype=jnp.int32) // tiles_across)[None, :]).astype(jnp.int32)
    entry_ids = (tile_group[:, :, None] * VIS + tile_lists).reshape(TY * TX, LIST).astype(jnp.int32)
    live_mask = (jnp.arange(LIST, dtype=jnp.int32)[None, None, :] < tile_len[:, :, None]).astype(jnp.float32).reshape(TY * TX, LIST)
    tile_count = TY * TX
    block_size = math.gcd(tile_count, 64)
    block_total = tile_count // block_size

    def total_loss(attr_all):
        visible_rows = jnp.take(attr_all, global_ids, axis=1)
        features = project_rows(visible_rows, camera)
        tile_feats = jnp.take(features, entry_ids, axis=1)
        grouped = tile_feats.reshape(9, block_total, block_size, LIST).transpose(1, 0, 2, 3)
        masks = live_mask.reshape(block_total, block_size, LIST)
        rendered = lax.map(jax.checkpoint(render_pair), (grouped, masks))
        image = rendered.transpose(1, 0, 2, 3).reshape(3, TY, TX, TILE, TILE).transpose(0, 1, 3, 2, 4).reshape(3, H, W)
        return image_loss(image, target)
    return jax.grad(total_loss)(attributes)
```

```python
import math

import jax
import jax.numpy as jnp
from jax import lax
from jax.experimental import pallas as pl
from jax.experimental.pallas import tpu as pltpu
from jax.sharding import PartitionSpec as P

F32 = jnp.float32
BF16 = jnp.bfloat16
I32 = jnp.int32
MESH = pl.DeviceIdType.MESH

TILE = 16
N_IMG = 8
N_CELL = 16
DEVICES = 128
LIST = 128
TILES = 32
ATTRS = 59
ROWS = 64
FEATS = 9
PAIRS = 5

WEIGHT_SSIM = 0.2
SMOOTHING = 0.01
STAB_ONE = 0.0001
STAB_TWO = 0.0009
BLUR_SIGMA = 1.5
SH_ZERO = 0.28209479177387814
SH_ONE = 0.4886025119029199
SH_TWO = (
    1.0925484305920792,
    -1.0925484305920792,
    0.31539156525252005,
    -1.0925484305920792,
    0.5462742152960396,
)
SH_THREE = (
    -0.5900435899266435,
    2.890611442640554,
    -0.4570457994644658,
    0.3731763325901154,
    -0.4570457994644658,
    1.445305721320277,
    -0.5900435899266435,
)


def blur_taps():
    raw = [math.exp(-((o - 5.0) ** 2) / (2.0 * BLUR_SIGMA * BLUR_SIGMA)) for o in range(11)]
    return [r / sum(raw) for r in raw]


TAPS = blur_taps()


def harmonic_basis(ux, uy, uz):
    xx, yy, zz = ux * ux, uy * uy, uz * uz
    return [
        SH_ZERO,
        -SH_ONE * uy,
        SH_ONE * uz,
        -SH_ONE * ux,
        SH_TWO[0] * ux * uy,
        SH_TWO[1] * uy * uz,
        SH_TWO[2] * (2.0 * zz - xx - yy),
        SH_TWO[3] * ux * uz,
        SH_TWO[4] * (xx - yy),
        SH_THREE[0] * uy * (3.0 * xx - yy),
        SH_THREE[1] * ux * uy * uz,
        SH_THREE[2] * uy * (4.0 * zz - xx - yy),
        SH_THREE[3] * uz * (2.0 * zz - 3.0 * xx - 3.0 * yy),
        SH_THREE[4] * ux * (4.0 * zz - xx - yy),
        SH_THREE[5] * uz * (xx - yy),
        SH_THREE[6] * ux * (xx - 3.0 * yy),
    ]


def project(rows, cam):
    pos = rows[0:3]
    scales = [jnp.exp(r) for r in rows[3:6]]
    qw = 1.5 + jnp.tanh(rows[6])
    qx, qy, qz = rows[7:10]
    inv = 1.0 / jnp.sqrt(qw * qw + qx * qx + qy * qy + qz * qz)
    qw, qx, qy, qz = qw * inv, qx * inv, qy * inv, qz * inv
    rot = [
        [1.0 - 2.0 * (qy * qy + qz * qz), 2.0 * (qx * qy - qw * qz), 2.0 * (qx * qz + qw * qy)],
        [2.0 * (qx * qy + qw * qz), 1.0 - 2.0 * (qx * qx + qz * qz), 2.0 * (qy * qz - qw * qx)],
        [2.0 * (qx * qz - qw * qy), 2.0 * (qy * qz + qw * qx), 1.0 - 2.0 * (qx * qx + qy * qy)],
    ]
    axes = [
        [
            (cam[s][0] * rot[0][k] + cam[s][1] * rot[1][k] + cam[s][2] * rot[2][k]) * scales[k]
            for k in range(3)
        ]
        for s in range(2)
    ]
    cov_a = axes[0][0] * axes[0][0] + axes[0][1] * axes[0][1] + axes[0][2] * axes[0][2] + 0.3
    cov_b = axes[0][0] * axes[1][0] + axes[0][1] * axes[1][1] + axes[0][2] * axes[1][2]
    cov_c = axes[1][0] * axes[1][0] + axes[1][1] * axes[1][1] + axes[1][2] * axes[1][2] + 0.3
    inv_det = 1.0 / (cov_a * cov_c - cov_b * cov_b)
    centers = [
        8.0
        + 7.0 * jnp.sin((cam[s][0] * pos[0] + cam[s][1] * pos[1] + cam[s][2] * pos[2]) / 3.0)
        for s in range(2)
    ]
    off = [pos[k] - cam[2][k] for k in range(3)]
    inv_dist = 1.0 / jnp.sqrt(off[0] * off[0] + off[1] * off[1] + off[2] * off[2])
    basis = harmonic_basis(off[0] * inv_dist, off[1] * inv_dist, off[2] * inv_dist)
    colours = []
    for c in range(3):
        total = 0.5 + basis[0] * rows[11 + 16 * c]
        for m in range(1, 16):
            total = total + basis[m] * rows[11 + 16 * c + m]
        colours.append(total)
    return centers + [cov_c * inv_det, -cov_b * inv_det, cov_a * inv_det] + colours


def read_camera(cam):
    return [[cam[s, k] for k in range(3)] for s in range(3)]


def spread_rows(attr, arows):
    def step(ct, carry):
        lanes = pl.ds(pl.multiple_of(ct * 128, 128), 128)
        for g in range(8):
            n = min(8, ATTRS - 8 * g)
            arows[pl.ds(pl.multiple_of(g * 512 + ct * 8, 8), n), :] = attr[8 * g : 8 * g + n, lanes]
        return carry

    lax.fori_loop(0, 64, step, 0)


def attr_rows(h):
    return [pl.ds((r // 8) * 512 + h * 64 + r % 8, 8, stride=8) for r in range(ATTRS)]


def wrap(value, count):
    return jnp.where(value >= count, value - count, value)


def each_peer(img, cell, act):
    for i in range(N_IMG):
        pi = wrap(img + i, N_IMG) if i else img

        def step(j, carry, pi=pi):
            act(pi, wrap(cell + j, N_CELL))
            return carry

        lax.fori_loop(0 if i else 1, N_CELL, step, 0)


def left_half():
    return lax.broadcasted_iota(I32, (8, 128), 1) < 64


def pack_message(values, msg, low_row, high_row):
    left = left_half()
    for i in range(PAIRS):
        a = values[2 * i]
        b = values[2 * i + 1] if 2 * i + 1 < FEATS else a
        msg[low_row(i), :] = jnp.where(left, a, pltpu.roll(b, 64, 1))
        msg[high_row(i), :] = jnp.where(left, pltpu.roll(a, 64, 1), b)


def unpack_message(msg, low_row, high_row):
    left = left_half()
    values = []
    for i in range(PAIRS):
        low, high = msg[low_row(i), :], msg[high_row(i), :]
        values.append(jnp.where(left, low, pltpu.roll(high, 64, 1)))
        if 2 * i + 1 < FEATS:
            values.append(jnp.where(left, pltpu.roll(low, 64, 1), high))
    return values


def lane_gather(table, ids):
    high = [v // 128 for v in ids]
    low = [v - h * 128 for v, h in zip(ids, high)]
    count = len(ids)

    def step(k8, carry):
        carry = list(carry)
        for kk in range(8):
            k = k8 * 8 + kk
            masks = [h == k for h in high]
            for f in range(FEATS):
                row = jnp.broadcast_to(table[pl.ds(f * ROWS + k, 1), :], (8, 128))
                for c in range(count):
                    got = jnp.take_along_axis(row, low[c], axis=1, mode="promise_in_bounds")
                    carry[c * FEATS + f] = jnp.where(masks[c], got, carry[c * FEATS + f])
        return tuple(carry)

    init = tuple(jnp.zeros((8, 128), F32) for _ in range(count * FEATS))
    out = lax.fori_loop(0, 8, step, init)
    return [list(out[c * FEATS : (c + 1) * FEATS]) for c in range(count)]


def scatter_block(ids, grads, acc):
    high = ids // 256
    low = ids - high * 256
    mask = lax.broadcasted_iota(I32, (32, 256), 0) == high
    upper, lower = [], []
    for g in grads:
        top = g.astype(BF16).astype(F32)
        upper.append(jnp.where(mask, top, 0.0).astype(BF16))
        lower.append(jnp.where(mask, g - top, 0.0).astype(BF16))
    lhs = jnp.concatenate(upper + lower, axis=0)
    hot = jnp.where(lax.broadcasted_iota(I32, (256, 256), 0) == low, 1.0, 0.0).astype(BF16)
    acc[...] += lax.dot_general(
        lhs, hot, (((1,), (1,)), ((), ())), preferred_element_type=F32
    )


def two_parts(v):
    top = v.astype(BF16)
    return top, (v - top.astype(F32)).astype(BF16)


def swap_blocks(z):
    rows = z.shape[0]
    row_at = lax.broadcasted_iota(I32, z.shape, 0)
    lane_at = lax.broadcasted_iota(I32, z.shape, 1)
    for bit in (1, 2, 4, 8):
        row_bit = (row_at // bit) % 2
        lane_bit = (lane_at // (16 * bit)) % 2
        down = pltpu.roll(pltpu.roll(z, rows - bit, 0), 16 * bit, 1)
        up = pltpu.roll(pltpu.roll(z, bit, 0), 256 - 16 * bit, 1)
        z = jnp.where(row_bit == lane_bit, z, jnp.where(row_bit == 0, down, up))
    return z


def border_block(lane_tile, row_block):
    return (lane_tile * 4 + row_block) * 48


def border_copies(ext, img, cell, send, recv):
    west, east = jnp.where(cell == 0, N_CELL - 1, cell - 1), wrap(cell + 1, N_CELL)
    north, south = jnp.where(img == 0, N_IMG - 1, img - 1), wrap(img + 1, N_IMG)
    plan = [
        (border_block(1, 1), border_block(3, 1), 96, img, west),
        (border_block(2, 1), border_block(0, 1), 96, img, east),
    ]
    for lane_tile in (1, 2):
        plan.append((border_block(lane_tile, 1), border_block(lane_tile, 3), 48, north, cell))
        plan.append((border_block(lane_tile, 2), border_block(lane_tile, 0), 48, south, cell))
    plan.append((border_block(1, 1), border_block(3, 3), 48, north, west))
    plan.append((border_block(2, 1), border_block(0, 3), 48, north, east))
    plan.append((border_block(1, 2), border_block(3, 0), 48, south, west))
    plan.append((border_block(2, 2), border_block(0, 0), 48, south, east))
    for source, dest, count, to_img, to_cell in plan:
        pltpu.make_async_remote_copy(
            src_ref=ext.at[pl.ds(source, count)],
            dst_ref=ext.at[pl.ds(dest, count)],
            send_sem=send,
            recv_sem=recv,
            device_id=(to_img, to_cell),
            device_id_type=MESH,
        ).start()


BORDER_ROWS = 2 * 96 + 8 * 48


def wait_rows(ref, count, sem):
    part = ref.at[pl.ds(0, count)]
    pltpu.make_async_copy(part, part, sem).wait()


def window(ext, img, cell, c, row_block):
    left = lax.broadcasted_iota(I32, (16, 128), 1) < 64
    tiles = []
    for lane_tile in range(4):
        v = ext[pl.ds(border_block(lane_tile, row_block) + c * 16, 16), :]
        bad = None
        if lane_tile == 0:
            bad = cell == 0
        if lane_tile == 3:
            bad = cell == N_CELL - 1
        if row_block == 0:
            bad = (img == 0) if bad is None else jnp.logical_or(bad, img == 0)
        if row_block == 3:
            bad = (img == N_IMG - 1) if bad is None else jnp.logical_or(bad, img == N_IMG - 1)
        if bad is not None:
            v = v * jnp.where(bad, 0.0, 1.0)
        tiles.append(pltpu.roll(v, 64, 1))
    return [jnp.where(left, tiles[j], tiles[j + 1]) for j in range(3)]


def blur_down(ref, base, first, count):
    out = []
    for j in range(3):
        start, stride = base
        at = start + j * stride + first
        total = TAPS[5] * ref[pl.ds(at + 5, count), :]
        for o in range(5):
            total = total + TAPS[o] * (
                ref[pl.ds(at + o, count), :] + ref[pl.ds(at + 10 - o, count), :]
            )
        out.append(total)
    return jnp.concatenate(out, axis=1)


def blur_along(v):
    total = TAPS[5] * v
    for o in range(5):
        d = 5 - o
        total = total + TAPS[o] * (pltpu.roll(v, d, 1) + pltpu.roll(v, 384 - d, 1))
    return total


def ssim_value(mean_render, mean_target, square_render, square_target, cross_term):
    spread_render = square_render - mean_render * mean_render
    spread_target = square_target - mean_target * mean_target
    covariance = cross_term - mean_render * mean_target
    upper = (2.0 * mean_render * mean_target + STAB_ONE) * (2.0 * covariance + STAB_TWO)
    lower = (mean_render * mean_render + mean_target * mean_target + STAB_ONE) * (
        spread_render + spread_target + STAB_TWO
    )
    return upper / lower


def map_base(m, c):
    return ((m * 3 + c) * 3 * 64, 64)


def step_kernel(
    cam_ref,
    len_ref,
    vis,
    attr,
    target,
    lists,
    out,
    arows,
    table,
    ids_in,
    ids_own,
    msg,
    inbox,
    msg_back,
    inbox_back,
    ext_render,
    ext_target,
    entry,
    tri_before,
    tri_after,
    weights,
    ratio,
    tile_rows,
    moments,
    maps,
    coefs,
    blurred,
    acc,
    sems,
):
    img = lax.axis_index("img")
    cell = lax.axis_index("cell")
    me = img * N_CELL + cell

    barrier = pltpu.get_barrier_semaphore()
    each_peer(
        img,
        cell,
        lambda pi, pc: pl.semaphore_signal(
            barrier, 1, device_id=(pi, pc), device_id_type=MESH
        ),
    )

    for lane_tile in range(2):
        for t in range(2):
            for c in range(3):
                ext_target[pl.ds(border_block(1 + lane_tile, 1 + t) + c * 16, 16), :] = target[
                    c, 16 * t : 16 * t + 16, 128 * lane_tile : 128 * lane_tile + 128
                ]
    spread_rows(attr, arows)

    pl.semaphore_wait(barrier, DEVICES - 1)

    def send_ids(pi, pc):
        p = pi * N_CELL + pc
        pltpu.make_async_remote_copy(
            src_ref=vis.at[pl.ds(p // 2, 1)],
            dst_ref=ids_in.at[pl.ds(me, 1)],
            send_sem=sems.at[0],
            recv_sem=sems.at[1],
            device_id=(pi, pc),
            device_id_type=MESH,
        ).start()

    each_peer(img, cell, send_ids)
    border_copies(ext_target, img, cell, sems.at[2], sems.at[3])
    ids_in[pl.ds(me, 1), :] = vis[pl.ds(me // 2, 1), :]

    cam = read_camera(cam_ref)

    def project_step(h, carry):
        rows = [arows[at, :] for at in attr_rows(h)]
        feats = project(rows, cam)
        feats.insert(5, jax.nn.sigmoid(rows[10]))
        for f in range(FEATS):
            table[pl.ds(pl.multiple_of(f * ROWS + h * 8, 8), 8), :] = feats[f]
        return carry

    lax.fori_loop(0, 8, project_step, 0)

    row_at = lax.broadcasted_iota(I32, (128, 128), 0)
    lane_at = lax.broadcasted_iota(I32, (128, 128), 1)
    before = jnp.where(row_at < lane_at, 1.0, 0.0).astype(BF16)
    after = jnp.where(row_at > lane_at, 1.0, 0.0).astype(BF16)
    for half in range(2):
        tri_before[128 * half : 128 * half + 128, :] = before
        tri_after[128 * half : 128 * half + 128, :] = after

    wait_rows(ids_in, DEVICES - 1, sems.at[1])
    odd = me - (me // 2) * 2
    left = left_half()

    def gather_step(c2, carry):
        ids = []
        for k in range(2):
            first = ids_in[pl.ds(pl.multiple_of(c2 * 16 + k * 8, 8), 8), :]
            second = ids_in[pl.ds(pl.multiple_of(64 + c2 * 16 + k * 8, 8), 8), :]
            even_form = jnp.where(left, first, pltpu.roll(second, 64, 1))
            odd_form = jnp.where(left, pltpu.roll(first, 64, 1), second)
            v = jnp.where(odd == 0, even_form, odd_form)
            ids_own[pl.ds(pl.multiple_of(c2 * 16 + k * 8, 8), 8), :] = v
            ids.append(v)
        got = lane_gather(table, ids)
        for k in range(2):
            at = (c2 * 2 + k) * 64
            pack_message(
                got[k],
                msg,
                lambda i: pl.ds(at + i, 8, stride=8),
                lambda i: pl.ds(512 + at + i, 8, stride=8),
            )
        return carry

    lax.fori_loop(0, 4, gather_step, 0)

    def send_rows(source, dest, send, recv):
        def act(pi, pc):
            p = pi * N_CELL + pc
            pltpu.make_async_remote_copy(
                src_ref=source.at[pl.ds(pl.multiple_of(p * 8, 8), PAIRS)],
                dst_ref=dest.at[pl.ds(pl.multiple_of(me * 8, 8), PAIRS)],
                send_sem=send,
                recv_sem=recv,
                device_id=(pi, pc),
                device_id_type=MESH,
            ).start()

        each_peer(img, cell, act)
        own = pl.ds(pl.multiple_of(me * 8, 8), PAIRS)
        dest[own, :] = source[own, :]

    send_rows(msg, inbox, sems.at[4], sems.at[5])

    wait_rows(ext_target, BORDER_ROWS, sems.at[3])
    for c in range(3):
        for row_block in range(4):
            parts = window(ext_target, img, cell, c, row_block)
            for j in range(3):
                for m, v in ((3, parts[j]), (4, parts[j] * parts[j])):
                    start, stride = map_base(m, c)
                    maps[pl.ds(start + j * stride + row_block * 16, 16), :] = v
    for m in (3, 4):
        for c in range(3):
            blurred[pl.ds(((m - 3) * 3 + c) * 48, 48), :] = blur_along(
                blur_down(maps, map_base(m, c), 6, 48)
            )

    wait_rows(inbox, (DEVICES - 1) * PAIRS, sems.at[5])

    def table_step(h, carry):
        values = unpack_message(
            inbox,
            lambda i: pl.ds(h * 128 + i, 8, stride=16),
            lambda i: pl.ds(h * 128 + 8 + i, 8, stride=16),
        )
        for f in range(FEATS):
            table[pl.ds(pl.multiple_of(f * ROWS + h * 8, 8), 8), :] = values[f]
        return carry

    lax.fori_loop(0, 8, table_step, 0)

    def list_step(c2, carry):
        at = [pl.multiple_of(c2 * 16 + k * 8, 8) for k in range(2)]
        got = lane_gather(table, [lists[pl.ds(a, 8), :] for a in at])
        for k in range(2):
            for f in range(FEATS):
                entry[pl.ds(pl.multiple_of(f * TILES + at[k], 8), 8), :] = got[k][f]
        return carry

    lax.fori_loop(0, 2, list_step, 0)

    def entry_row(f, t):
        return entry[pl.ds(f * TILES + t, 1), :]

    across = lax.broadcasted_iota(I32, (16, 128), 0).astype(F32) + 0.5
    lane_row = lax.broadcasted_iota(I32, (1, 128), 1)

    def image_row(t, c):
        return (t // 16) * 48 + c * 16 + lax.rem(t, 16)

    def render_step(t, carry):
        alive = lane_row < len_ref[t // 16, lax.rem(t, 16)]
        opacity = jnp.where(alive, entry_row(5, t), 0.0)
        dx = across - entry_row(0, t)
        center_y = entry_row(1, t)
        square_x = (-0.5 * entry_row(2, t)) * dx * dx
        mixed = -entry_row(3, t) * dx
        half_y = -0.5 * entry_row(4, t)
        alpha, logs = [], []
        for y in range(16):
            dy = (y + 0.5) - center_y
            alpha.append(opacity * jnp.exp(square_x + dy * (mixed + half_y * dy)))
            logs.append(jnp.log(1.0 - alpha[y]))
        alpha = jnp.concatenate(alpha, axis=0)
        logs = jnp.concatenate(logs, axis=0)
        before = jnp.dot(
            jnp.concatenate(two_parts(logs), axis=1), tri_before[...], preferred_element_type=F32
        )
        ratio[pl.ds(pl.multiple_of(t * 256, 256), 256), :] = alpha * jnp.exp(-logs)
        weight = jnp.concatenate(two_parts(jnp.exp(before) * alpha), axis=1)
        weights[pl.ds(pl.multiple_of(t * 256, 256), 256), :] = weight
        colour = [two_parts(entry_row(6 + c, t)) for c in range(3)]
        lhs = jnp.concatenate(
            [c[part] for part in range(2) for c in colour] + [jnp.zeros((10, 128), BF16)], axis=0
        )
        pixels = lax.dot_general(
            jnp.concatenate([lhs, lhs], axis=1),
            weight,
            (((1,), (1,)), ((), ())),
            preferred_element_type=F32,
        )
        for c in range(3):
            tile_rows[pl.ds(image_row(t, c), 1), :] = pixels[c : c + 1] + pixels[3 + c : 4 + c]
        return carry

    lax.fori_loop(0, TILES, render_step, 0)

    picture = swap_blocks(tile_rows[...])
    for lane_tile in range(2):
        ext_render[pl.ds(border_block(1 + lane_tile, 1), 96), :] = picture[
            :, 128 * lane_tile : 128 * lane_tile + 128
        ]
    border_copies(ext_render, img, cell, sems.at[6], sems.at[7])
    wait_rows(ext_render, BORDER_ROWS, sems.at[7])

    for c in range(3):
        for row_block in range(4):
            parts = window(ext_render, img, cell, c, row_block)
            start, stride = map_base(3, c)
            for j in range(3):
                rows = pl.ds(start + j * stride + row_block * 16, 16)
                v = parts[j]
                for m, value in ((0, v), (1, v * v), (2, v * maps[rows, :])):
                    first, step = map_base(m, c)
                    maps[pl.ds(first + j * step + row_block * 16, 16), :] = value
    row_at = lax.broadcasted_iota(I32, (48, 384), 0) + (img * 32 - 5)
    lane_at = lax.broadcasted_iota(I32, (48, 384), 1) + (cell * 256 - 64)
    inside = (row_at >= 0) & (row_at < N_IMG * 32) & (lane_at >= 0) & (lane_at < N_CELL * 256)
    for c in range(3):
        mean, square, cross = [
            blur_along(blur_down(maps, map_base(m, c), 6, 48)) for m in range(3)
        ]
        mean_target = blurred[pl.ds(c * 48, 48), :]
        square_target = blurred[pl.ds((3 + c) * 48, 48), :]
        similarity, pullback = jax.vjp(
            lambda a, b, d: ssim_value(a, mean_target, b, square_target, d), mean, square, cross
        )
        for m, v in enumerate(pullback(jnp.full((48, 384), -WEIGHT_SSIM, F32))):
            v = jnp.where(inside, v, 0.0)
            for j in range(3):
                coefs[pl.ds(((m * 3 + c) * 3 + j) * 48, 48), :] = v[:, 128 * j : 128 * j + 128]
    for c in range(3):
        back_mean, back_square, back_cross = [
            blur_along(blur_down(coefs, ((m * 3 + c) * 3 * 48, 48), 0, 32))[:, 64:320]
            for m in range(3)
        ]
        for t in range(2):
            rows = slice(16 * t, 16 * t + 16)
            image = jnp.concatenate(
                [
                    ext_render[pl.ds(border_block(1 + k, 1 + t) + c * 16, 16), :]
                    for k in range(2)
                ],
                axis=1,
            )
            wanted = target[c, rows, :]
            difference = image - wanted
            tile_rows[pl.ds(t * 48 + c * 16, 16), :] = (
                (1.0 - WEIGHT_SSIM)
                * difference
                / jnp.sqrt(difference * difference + SMOOTHING * SMOOTHING)
                + back_mean[rows]
                + 2.0 * image * back_square[rows]
                + wanted * back_cross[rows]
            )
    tile_rows[...] = swap_blocks(tile_rows[...])

    def back_step(t, carry):
        pixel_grad = [two_parts(tile_rows[pl.ds(image_row(t, c), 1), :]) for c in range(3)]
        colour = [two_parts(entry_row(6 + c, t)) for c in range(3)]
        tops, lows = [g[0] for g in pixel_grad], [g[1] for g in pixel_grad]
        grad_rows = jnp.concatenate(tops + lows + tops + [jnp.zeros((7, 256), BF16)], axis=0)
        colour_rows = jnp.concatenate(
            [c[0] for c in colour] * 2 + [c[1] for c in colour] + [jnp.zeros((7, 128), BF16)],
            axis=0,
        )
        value = lax.dot_general(
            grad_rows, colour_rows, (((0,), (0,)), ((), ())), preferred_element_type=F32
        )
        weight = weights[pl.ds(pl.multiple_of(t * 256, 256), 256), :]
        gain = value * (weight[:, :128].astype(F32) + weight[:, 128:].astype(F32))
        later = jnp.dot(
            jnp.concatenate(two_parts(gain), axis=1), tri_after[...], preferred_element_type=F32
        )
        pull = gain - ratio[pl.ds(pl.multiple_of(t * 256, 256), 256), :] * later
        dx = across - entry_row(0, t)
        center_y = entry_row(1, t)
        sum_0 = sum_y = sum_yy = None
        for y in range(16):
            dy = (y + 0.5) - center_y
            part = pull[16 * y : 16 * y + 16]
            part_y = part * dy
            part_yy = part_y * dy
            sum_0 = part if y == 0 else sum_0 + part
            sum_y = part_y if y == 0 else sum_y + part_y
            sum_yy = part_yy if y == 0 else sum_yy + part_yy
        sum_x = sum_0 * dx
        found = [sum_0, sum_x, sum_y, sum_x * dx, sum_y * dx, sum_yy]
        for m in range(6):
            moments[pl.ds(m * TILES + t, 1), :] = jnp.sum(found[m], axis=0, keepdims=True)
        mixed = jnp.dot(grad_rows, weight, preferred_element_type=F32)
        for c in range(3):
            both = mixed[c : c + 1] + mixed[3 + c : 4 + c]
            moments[pl.ds((6 + c) * TILES + t, 1), :] = both[:, :128] + both[:, 128:]
        return carry

    lax.fori_loop(0, TILES, back_step, 0)

    feat = [entry[f * TILES : (f + 1) * TILES, :] for f in range(6)]
    mom = [moments[m * TILES : (m + 1) * TILES, :] for m in range(6)]
    entry[0:TILES, :] = feat[2] * mom[1] + feat[3] * mom[2]
    entry[TILES : 2 * TILES, :] = feat[3] * mom[1] + feat[4] * mom[2]
    entry[2 * TILES : 3 * TILES, :] = -0.5 * mom[3]
    entry[3 * TILES : 4 * TILES, :] = -mom[4]
    entry[4 * TILES : 5 * TILES, :] = -0.5 * mom[5]
    entry[5 * TILES : 6 * TILES, :] = mom[0]
    entry[6 * TILES : 9 * TILES, :] = moments[6 * TILES : 9 * TILES, :]

    acc[...] = jnp.zeros_like(acc)

    def slot_step(b, carry):
        def pair(ref, at):
            both = ref[pl.ds(at, 2), :]
            return jnp.concatenate([both[0:1], both[1:2]], axis=1)

        scatter_block(
            pair(lists, b * 2), [pair(entry, f * TILES + b * 2) for f in range(FEATS)], acc
        )
        return carry

    lax.fori_loop(0, TILES // 2, slot_step, 0)

    def total_rows(f, h):
        a = acc[pl.ds(pl.multiple_of(f * 32 + h * 8, 8), 8), :]
        b = acc[pl.ds(pl.multiple_of(288 + f * 32 + h * 8, 8), 8), :]
        return a + b

    def back_pack(h, carry):
        totals = [total_rows(f, h) for f in range(FEATS)]
        for half in range(2):
            pack_message(
                [v[:, 128 * half : 128 * half + 128] for v in totals],
                msg_back,
                lambda i: pl.ds(h * 256 + (2 * half) * 8 + i, 8, stride=32),
                lambda i: pl.ds(h * 256 + (2 * half + 1) * 8 + i, 8, stride=32),
            )
        return carry

    lax.fori_loop(0, 4, back_pack, 0)
    send_rows(msg_back, inbox_back, sems.at[8], sems.at[9])

    acc[...] = jnp.zeros_like(acc)
    wait_rows(inbox_back, (DEVICES - 1) * PAIRS, sems.at[9])

    def owner_unpack(c, carry):
        values = unpack_message(
            inbox_back,
            lambda i: pl.ds(c * 64 + i, 8, stride=8),
            lambda i: pl.ds(512 + c * 64 + i, 8, stride=8),
        )
        for f in range(FEATS):
            table[pl.ds(pl.multiple_of(f * ROWS + c * 8, 8), 8), :] = values[f]
        return carry

    lax.fori_loop(0, 8, owner_unpack, 0)

    def owner_step(b, carry):
        def pair(ref, at):
            both = ref[pl.ds(at, 2), :]
            return jnp.concatenate([both[0:1], both[1:2]], axis=1)

        scatter_block(
            pair(ids_own, b * 2), [pair(table, f * ROWS + b * 2) for f in range(FEATS)], acc
        )
        return carry

    lax.fori_loop(0, ROWS // 2, owner_step, 0)

    def finish(h, carry):
        for f in range(FEATS):
            v = total_rows(f, h)
            for half in range(2):
                out[pl.ds(f * ROWS + h * 16 + half, 8, stride=2), :] = v[
                    :, 128 * half : 128 * half + 128
                ]
        return carry

    lax.fori_loop(0, 4, finish, 0)

    wait_rows(ids_in, DEVICES - 1, sems.at[0])
    wait_rows(ext_target, BORDER_ROWS, sems.at[2])
    wait_rows(msg, (DEVICES - 1) * PAIRS, sems.at[4])
    wait_rows(ext_render, BORDER_ROWS, sems.at[6])
    wait_rows(msg_back, (DEVICES - 1) * PAIRS, sems.at[8])


def pullback_kernel(cam_ref, attr, feat_grad, out, arows):
    cam = read_camera(cam_ref)
    spread_rows(attr, arows)

    def step(h, carry):
        places = attr_rows(h)
        rows = [arows[at, :] for at in places]
        _, pullback = jax.vjp(lambda r: project(r, cam), rows)
        grads = [
            feat_grad[pl.ds(pl.multiple_of(f * ROWS + h * 8, 8), 8), :] for f in range(FEATS)
        ]
        log_opacity = grads.pop(5)
        (result,) = pullback(grads)
        result[10] = log_opacity * (1.0 - jax.nn.sigmoid(rows[10]))
        for at, v in zip(places, result):
            arows[at, :] = v
        return carry

    lax.fori_loop(0, 8, step, 0)

    def gather_rows(ct, carry):
        lanes = pl.ds(pl.multiple_of(ct * 128, 128), 128)
        for g in range(8):
            n = min(8, ATTRS - 8 * g)
            out[8 * g : 8 * g + n, lanes] = arows[pl.ds(pl.multiple_of(g * 512 + ct * 8, 8), n), :]
        return carry

    lax.fori_loop(0, 64, gather_rows, 0)


def shards(attributes, camera, target, visible_index, tile_lists, tile_len):
    vmem = pl.BlockSpec(memory_space=pltpu.VMEM)
    smem = pl.BlockSpec(memory_space=pltpu.SMEM)
    feat_grad = pl.pallas_call(
        step_kernel,
        out_shape=jax.ShapeDtypeStruct((FEATS * ROWS, 128), F32),
        in_specs=[smem, smem, vmem, vmem, vmem, vmem],
        out_specs=vmem,
        scratch_shapes=[
            pltpu.VMEM((4096, 128), F32),
            pltpu.VMEM((FEATS * ROWS, 128), F32),
            pltpu.VMEM((DEVICES, 128), I32),
            pltpu.VMEM((ROWS, 128), I32),
            pltpu.VMEM((DEVICES * 8, 128), F32),
            pltpu.VMEM((DEVICES * 8, 128), F32),
            pltpu.VMEM((DEVICES * 8, 128), F32),
            pltpu.VMEM((DEVICES * 8, 128), F32),
            pltpu.VMEM((16 * 48, 128), F32),
            pltpu.VMEM((16 * 48, 128), F32),
            pltpu.VMEM((FEATS * TILES, 128), F32),
            pltpu.VMEM((256, 128), BF16),
            pltpu.VMEM((256, 128), BF16),
            pltpu.VMEM((TILES * 256, 256), BF16),
            pltpu.VMEM((TILES * 256, 128), F32),
            pltpu.VMEM((96, 256), F32),
            pltpu.VMEM((FEATS * TILES, 128), F32),
            pltpu.VMEM((5 * 3 * 3 * 64, 128), F32),
            pltpu.VMEM((3 * 3 * 3 * 48, 128), F32),
            pltpu.VMEM((2 * 3 * 48, 384), F32),
            pltpu.VMEM((2 * FEATS * 32, 256), F32),
            pltpu.SemaphoreType.DMA((10,)),
        ],
        compiler_params=pltpu.CompilerParams(
            collective_id=0, has_side_effects=True, vmem_limit_bytes=56 * 1024 * 1024
        ),
        name="splat_step",
    )(
        camera,
        tile_len,
        visible_index.reshape(ROWS, 128),
        attributes,
        target,
        tile_lists.reshape(TILES, LIST),
    )
    return pl.pallas_call(
        pullback_kernel,
        out_shape=jax.ShapeDtypeStruct(attributes.shape, F32),
        in_specs=[smem, vmem, vmem],
        out_specs=vmem,
        scratch_shapes=[pltpu.VMEM((4096, 128), F32)],
        name="splat_pullback",
    )(camera, attributes, feat_grad)


def solution(mesh):
    return jax.shard_map(
        shards,
        mesh=mesh,
        in_specs=(
            P(None, ("img", "cell")),
            P(),
            P(None, "img", "cell"),
            P(("img", "cell"), None),
            P("img", "cell", None),
            P("img", "cell"),
        ),
        out_specs=P(None, ("img", "cell")),
        check_vma=False,
    )
```

```python
import math

import jax
import jax.numpy as jnp
from jax import lax
from jax.experimental import pallas as pl
from jax.experimental.pallas import tpu as pltpu
from jax.sharding import PartitionSpec as P

F32 = jnp.float32
BF16 = jnp.bfloat16
I32 = jnp.int32
MESH = pl.DeviceIdType.MESH

TILE = 16
N_IMG = 8
N_CELL = 16
DEVICES = 128
LIST = 128
TILES = 32
ATTRS = 59
ROWS = 64
FEATS = 9
PAIRS = 5
GROUP = 4

WEIGHT_SSIM = 0.2
SMOOTHING = 0.01
STAB_ONE = 0.0001
STAB_TWO = 0.0009
BLUR_SIGMA = 1.5
SH_ZERO = 0.28209479177387814
SH_ONE = 0.4886025119029199
SH_TWO = (
    1.0925484305920792,
    -1.0925484305920792,
    0.31539156525252005,
    -1.0925484305920792,
    0.5462742152960396,
)
SH_THREE = (
    -0.5900435899266435,
    2.890611442640554,
    -0.4570457994644658,
    0.3731763325901154,
    -0.4570457994644658,
    1.445305721320277,
    -0.5900435899266435,
)


def blur_taps():
    raw = [math.exp(-((o - 5.0) ** 2) / (2.0 * BLUR_SIGMA * BLUR_SIGMA)) for o in range(11)]
    return [r / sum(raw) for r in raw]


TAPS = blur_taps()


def harmonic_basis(ux, uy, uz):
    xx, yy, zz = ux * ux, uy * uy, uz * uz
    return [
        SH_ZERO,
        -SH_ONE * uy,
        SH_ONE * uz,
        -SH_ONE * ux,
        SH_TWO[0] * ux * uy,
        SH_TWO[1] * uy * uz,
        SH_TWO[2] * (2.0 * zz - xx - yy),
        SH_TWO[3] * ux * uz,
        SH_TWO[4] * (xx - yy),
        SH_THREE[0] * uy * (3.0 * xx - yy),
        SH_THREE[1] * ux * uy * uz,
        SH_THREE[2] * uy * (4.0 * zz - xx - yy),
        SH_THREE[3] * uz * (2.0 * zz - 3.0 * xx - 3.0 * yy),
        SH_THREE[4] * ux * (4.0 * zz - xx - yy),
        SH_THREE[5] * uz * (xx - yy),
        SH_THREE[6] * ux * (xx - 3.0 * yy),
    ]


def project(rows, cam):
    pos = rows[0:3]
    scales = [jnp.exp(r) for r in rows[3:6]]
    qw = 1.5 + jnp.tanh(rows[6])
    qx, qy, qz = rows[7:10]
    inv = 1.0 / jnp.sqrt(qw * qw + qx * qx + qy * qy + qz * qz)
    qw, qx, qy, qz = qw * inv, qx * inv, qy * inv, qz * inv
    rot = [
        [1.0 - 2.0 * (qy * qy + qz * qz), 2.0 * (qx * qy - qw * qz), 2.0 * (qx * qz + qw * qy)],
        [2.0 * (qx * qy + qw * qz), 1.0 - 2.0 * (qx * qx + qz * qz), 2.0 * (qy * qz - qw * qx)],
        [2.0 * (qx * qz - qw * qy), 2.0 * (qy * qz + qw * qx), 1.0 - 2.0 * (qx * qx + qy * qy)],
    ]
    axes = [
        [
            (cam[s][0] * rot[0][k] + cam[s][1] * rot[1][k] + cam[s][2] * rot[2][k]) * scales[k]
            for k in range(3)
        ]
        for s in range(2)
    ]
    cov_a = axes[0][0] * axes[0][0] + axes[0][1] * axes[0][1] + axes[0][2] * axes[0][2] + 0.3
    cov_b = axes[0][0] * axes[1][0] + axes[0][1] * axes[1][1] + axes[0][2] * axes[1][2]
    cov_c = axes[1][0] * axes[1][0] + axes[1][1] * axes[1][1] + axes[1][2] * axes[1][2] + 0.3
    inv_det = 1.0 / (cov_a * cov_c - cov_b * cov_b)
    centers = [
        8.0
        + 7.0 * jnp.sin((cam[s][0] * pos[0] + cam[s][1] * pos[1] + cam[s][2] * pos[2]) / 3.0)
        for s in range(2)
    ]
    off = [pos[k] - cam[2][k] for k in range(3)]
    inv_dist = 1.0 / jnp.sqrt(off[0] * off[0] + off[1] * off[1] + off[2] * off[2])
    basis = harmonic_basis(off[0] * inv_dist, off[1] * inv_dist, off[2] * inv_dist)
    colours = []
    for c in range(3):
        total = 0.5 + basis[0] * rows[11 + 16 * c]
        for m in range(1, 16):
            total = total + basis[m] * rows[11 + 16 * c + m]
        colours.append(total)
    return centers + [cov_c * inv_det, -cov_b * inv_det, cov_a * inv_det] + colours


def read_camera(cam):
    return [[cam[s, k] for k in range(3)] for s in range(3)]


def spread_rows(attr, arows):
    def step(ct, carry):
        lanes = pl.ds(pl.multiple_of(ct * 128, 128), 128)
        for g in range(8):
            n = min(8, ATTRS - 8 * g)
            arows[pl.ds(pl.multiple_of(g * 512 + ct * 8, 8), n), :] = attr[8 * g : 8 * g + n, lanes]
        return carry

    lax.fori_loop(0, 64, step, 0)


def attr_rows(h):
    return [pl.ds((r // 8) * 512 + h * 64 + r % 8, 8, stride=8) for r in range(ATTRS)]


def wrap(value, count):
    return jnp.where(value >= count, value - count, value)


def each_peer(img, cell, act):
    for i in range(N_IMG):
        pi = wrap(img + i, N_IMG) if i else img

        def step(j, carry, pi=pi):
            act(pi, wrap(cell + j, N_CELL))
            return carry

        lax.fori_loop(0 if i else 1, N_CELL, step, 0)


def left_half():
    return lax.broadcasted_iota(I32, (8, 128), 1) < 64


def pack_message(values, msg, low_row, high_row):
    left = left_half()
    for i in range(PAIRS):
        a = values[2 * i]
        b = values[2 * i + 1] if 2 * i + 1 < FEATS else a
        msg[low_row(i), :] = jnp.where(left, a, pltpu.roll(b, 64, 1))
        msg[high_row(i), :] = jnp.where(left, pltpu.roll(a, 64, 1), b)


def unpack_message(msg, low_row, high_row):
    left = left_half()
    values = []
    for i in range(PAIRS):
        low, high = msg[low_row(i), :], msg[high_row(i), :]
        values.append(jnp.where(left, low, pltpu.roll(high, 64, 1)))
        if 2 * i + 1 < FEATS:
            values.append(jnp.where(left, pltpu.roll(low, 64, 1), high))
    return values


def one_hot(low):
    return jnp.where(lax.broadcasted_iota(I32, (256, 256), 0) == low, 1.0, 0.0).astype(BF16)


def split_ids(ids):
    high = lax.shift_right_logical(ids, 8)
    return high, ids - lax.shift_left(high, 8)


def row_pair(ref, at):
    both = ref[pl.ds(at, 2), :]
    return jnp.concatenate([both[0:1], both[1:2]], axis=1)


def make_parts(table, parts):
    for f in range(FEATS):
        for half in range(2):
            v = table[pl.ds(f * ROWS + half, 32, stride=2), :]
            for part in range(3):
                top = v.astype(BF16)
                parts[
                    32 * f : 32 * f + 32, 256 * part + 128 * half : 256 * part + 128 * half + 128
                ] = top
                v = v - top.astype(F32)


def gather_blocks(parts, ids, hots):
    found = [
        jnp.dot(
            parts[...], jnp.concatenate([hot] * 3, axis=0), preferred_element_type=F32
        )
        for hot in hots
    ]
    out = []
    for v, block in zip(found, ids):
        mask = lax.broadcasted_iota(I32, (32, 256), 0) == split_ids(block)[0]
        out.append(
            [
                jnp.sum(
                    jnp.where(mask, v[32 * f : 32 * f + 32], 0.0), axis=0, keepdims=True
                )
                for f in range(FEATS)
            ]
        )
    return out


def scatter_blocks(ids, grads, hots, acc):
    lhs = []
    for block, rows in zip(ids, grads):
        mask = lax.broadcasted_iota(I32, (32, 256), 0) == split_ids(block)[0]
        upper, lower = [], []
        for g in rows:
            top = g.astype(BF16).astype(F32)
            upper.append(jnp.where(mask, top, 0.0).astype(BF16))
            lower.append(jnp.where(mask, g - top, 0.0).astype(BF16))
        lhs.append(jnp.concatenate(upper + lower, axis=0))
    acc[...] += lax.dot_general(
        jnp.concatenate(lhs, axis=1),
        hots,
        (((1,), (1,)), ((), ())),
        preferred_element_type=F32,
    )


def two_parts(v):
    top = v.astype(BF16)
    return top, (v - top.astype(F32)).astype(BF16)


def swap_blocks(z):
    rows = z.shape[0]
    row_at = lax.broadcasted_iota(I32, z.shape, 0)
    lane_at = lax.broadcasted_iota(I32, z.shape, 1)
    for bit in (1, 2, 4, 8):
        row_bit = (row_at // bit) % 2
        lane_bit = (lane_at // (16 * bit)) % 2
        down = pltpu.roll(pltpu.roll(z, rows - bit, 0), 16 * bit, 1)
        up = pltpu.roll(pltpu.roll(z, bit, 0), 256 - 16 * bit, 1)
        z = jnp.where(row_bit == lane_bit, z, jnp.where(row_bit == 0, down, up))
    return z


def border_block(lane_tile, row_block):
    return (lane_tile * 4 + row_block) * 48


def border_copies(ext, img, cell, send, recv):
    west, east = jnp.where(cell == 0, N_CELL - 1, cell - 1), wrap(cell + 1, N_CELL)
    north, south = jnp.where(img == 0, N_IMG - 1, img - 1), wrap(img + 1, N_IMG)
    plan = [
        (border_block(1, 1), border_block(3, 1), 96, img, west),
        (border_block(2, 1), border_block(0, 1), 96, img, east),
    ]
    for lane_tile in (1, 2):
        plan.append((border_block(lane_tile, 1), border_block(lane_tile, 3), 48, north, cell))
        plan.append((border_block(lane_tile, 2), border_block(lane_tile, 0), 48, south, cell))
    plan.append((border_block(1, 1), border_block(3, 3), 48, north, west))
    plan.append((border_block(2, 1), border_block(0, 3), 48, north, east))
    plan.append((border_block(1, 2), border_block(3, 0), 48, south, west))
    plan.append((border_block(2, 2), border_block(0, 0), 48, south, east))
    for source, dest, count, to_img, to_cell in plan:
        pltpu.make_async_remote_copy(
            src_ref=ext.at[pl.ds(source, count)],
            dst_ref=ext.at[pl.ds(dest, count)],
            send_sem=send,
            recv_sem=recv,
            device_id=(to_img, to_cell),
            device_id_type=MESH,
        ).start()


BORDER_ROWS = 2 * 96 + 8 * 48


def wait_rows(ref, count, sem):
    part = ref.at[pl.ds(0, count)]
    pltpu.make_async_copy(part, part, sem).wait()


def window(ext, img, cell, c, row_block):
    left = lax.broadcasted_iota(I32, (16, 128), 1) < 64
    tiles = []
    for lane_tile in range(4):
        v = ext[pl.ds(border_block(lane_tile, row_block) + c * 16, 16), :]
        bad = None
        if lane_tile == 0:
            bad = cell == 0
        if lane_tile == 3:
            bad = cell == N_CELL - 1
        if row_block == 0:
            bad = (img == 0) if bad is None else jnp.logical_or(bad, img == 0)
        if row_block == 3:
            bad = (img == N_IMG - 1) if bad is None else jnp.logical_or(bad, img == N_IMG - 1)
        if bad is not None:
            v = v * jnp.where(bad, 0.0, 1.0)
        tiles.append(pltpu.roll(v, 64, 1))
    return [jnp.where(left, tiles[j], tiles[j + 1]) for j in range(3)]


def blur_down(ref, base, first, count):
    out = []
    for j in range(3):
        start, stride = base
        at = start + j * stride + first
        total = TAPS[5] * ref[pl.ds(at + 5, count), :]
        for o in range(5):
            total = total + TAPS[o] * (
                ref[pl.ds(at + o, count), :] + ref[pl.ds(at + 10 - o, count), :]
            )
        out.append(total)
    return jnp.concatenate(out, axis=1)


def blur_along(v):
    total = TAPS[5] * v
    for o in range(5):
        d = 5 - o
        total = total + TAPS[o] * (pltpu.roll(v, d, 1) + pltpu.roll(v, 384 - d, 1))
    return total


def ssim_value(mean_render, mean_target, square_render, square_target, cross_term):
    spread_render = square_render - mean_render * mean_render
    spread_target = square_target - mean_target * mean_target
    covariance = cross_term - mean_render * mean_target
    upper = (2.0 * mean_render * mean_target + STAB_ONE) * (2.0 * covariance + STAB_TWO)
    lower = (mean_render * mean_render + mean_target * mean_target + STAB_ONE) * (
        spread_render + spread_target + STAB_TWO
    )
    return upper / lower


def map_base(m, c):
    return ((m * 3 + c) * 3 * 64, 64)


def step_kernel(
    cam_ref,
    len_ref,
    vis,
    attr_hbm,
    target,
    lists,
    out,
    attr,
    arows,
    table,
    parts,
    hot_list,
    hot_own,
    ids_in,
    ids_own,
    msg,
    inbox,
    msg_back,
    inbox_back,
    ext_render,
    ext_target,
    entry,
    tri_before,
    tri_after,
    weights,
    ratio,
    tile_rows,
    moments,
    maps,
    coefs,
    blurred,
    acc,
    sems,
):
    img = lax.axis_index("img")
    cell = lax.axis_index("cell")
    me = img * N_CELL + cell

    barrier = pltpu.get_barrier_semaphore()
    each_peer(
        img,
        cell,
        lambda pi, pc: pl.semaphore_signal(
            barrier, 1, device_id=(pi, pc), device_id_type=MESH
        ),
    )
    load_attr = pltpu.make_async_copy(attr_hbm, attr, sems.at[10])
    load_attr.start()

    for lane_tile in range(2):
        for t in range(2):
            for c in range(3):
                ext_target[pl.ds(border_block(1 + lane_tile, 1 + t) + c * 16, 16), :] = target[
                    c, 16 * t : 16 * t + 16, 128 * lane_tile : 128 * lane_tile + 128
                ]

    def list_hot(b, carry):
        hot_list[:, pl.ds(pl.multiple_of(b * 256, 256), 256)] = one_hot(
            split_ids(row_pair(lists, b * 2))[1]
        )
        return carry

    lax.fori_loop(0, TILES // 2, list_hot, 0)

    cam = read_camera(cam_ref)
    load_attr.wait()
    spread_rows(attr, arows)

    def project_step(h, carry):
        rows = [arows[at, :] for at in attr_rows(h)]
        feats = project(rows, cam)
        feats.insert(5, jax.nn.sigmoid(rows[10]))
        for f in range(FEATS):
            table[pl.ds(pl.multiple_of(f * ROWS + h * 8, 8), 8), :] = feats[f]
        return carry

    lax.fori_loop(0, 8, project_step, 0)
    make_parts(table, parts)

    row_at = lax.broadcasted_iota(I32, (128, 128), 0)
    lane_at = lax.broadcasted_iota(I32, (128, 128), 1)
    before = jnp.where(row_at < lane_at, 1.0, 0.0).astype(BF16)
    after = jnp.where(row_at > lane_at, 1.0, 0.0).astype(BF16)
    for half in range(2):
        tri_before[128 * half : 128 * half + 128, :] = before
        tri_after[128 * half : 128 * half + 128, :] = after

    pl.semaphore_wait(barrier, DEVICES - 1)

    def send_ids(pi, pc):
        p = pi * N_CELL + pc
        pltpu.make_async_remote_copy(
            src_ref=vis.at[pl.ds(p // 2, 1)],
            dst_ref=ids_in.at[pl.ds(me, 1)],
            send_sem=sems.at[0],
            recv_sem=sems.at[1],
            device_id=(pi, pc),
            device_id_type=MESH,
        ).start()

    each_peer(img, cell, send_ids)
    border_copies(ext_target, img, cell, sems.at[2], sems.at[3])
    ids_in[pl.ds(me, 1), :] = vis[pl.ds(me // 2, 1), :]

    wait_rows(ext_target, BORDER_ROWS, sems.at[3])
    for c in range(3):
        for row_block in range(4):
            strips = window(ext_target, img, cell, c, row_block)
            for j in range(3):
                for m, v in ((3, strips[j]), (4, strips[j] * strips[j])):
                    start, stride = map_base(m, c)
                    maps[pl.ds(start + j * stride + row_block * 16, 16), :] = v
    for m in (3, 4):
        for c in range(3):
            blurred[pl.ds(((m - 3) * 3 + c) * 48, 48), :] = blur_along(
                blur_down(maps, map_base(m, c), 6, 48)
            )

    wait_rows(ids_in, DEVICES - 1, sems.at[1])
    odd = me - (me // 2) * 2
    left = left_half()
    for c in range(8):
        first = ids_in[8 * c : 8 * c + 8, :]
        second = ids_in[64 + 8 * c : 72 + 8 * c, :]
        even_form = jnp.where(left, first, pltpu.roll(second, 64, 1))
        odd_form = jnp.where(left, pltpu.roll(first, 64, 1), second)
        ids_own[8 * c : 8 * c + 8, :] = jnp.where(odd == 0, even_form, odd_form)

    def send_message(source, dest, send, recv, pi, pc):
        pltpu.make_async_remote_copy(
            src_ref=source.at[pl.ds(pl.multiple_of((pi * N_CELL + pc) * 8, 8), PAIRS)],
            dst_ref=dest.at[pl.ds(pl.multiple_of(me * 8, 8), PAIRS)],
            send_sem=send,
            recv_sem=recv,
            device_id=(pi, pc),
            device_id_type=MESH,
        ).start()

    left_row = lax.broadcasted_iota(I32, (1, 128), 1) < 64
    half_img = img - (img // 4) * 4
    own_group = half_img * 2 + cell // 8

    def reply_step(k, carry):
        g = wrap(own_group + 1 + k, 8)
        ids = [row_pair(ids_own, g * 8 + 2 * n) for n in range(4)]
        hots = [one_hot(split_ids(v)[1]) for v in ids]
        for n in range(4):
            hot_own[:, pl.ds(pl.multiple_of(g * 1024 + n * 256, 256), 256)] = hots[n]
        got = gather_blocks(parts, ids, hots)
        for n in range(4):
            for row in range(2):
                d = g * 8 + 2 * n + row
                for i in range(PAIRS):
                    first = got[n][2 * i][:, 128 * row : 128 * row + 128]
                    second = got[n][min(2 * i + 1, FEATS - 1)][:, 128 * row : 128 * row + 128]
                    msg[pl.ds(d * 8 + i, 1), :] = jnp.where(
                        left_row, first, pltpu.roll(second, 64, 1)
                    )
                    msg[pl.ds(512 + d * 8 + i, 1), :] = jnp.where(
                        left_row, pltpu.roll(first, 64, 1), second
                    )
        for side in range(2):
            to_img = 4 * side + g // 2

            def send_step(n, carry):
                to_cell = (g - (g // 2) * 2) * 8 + n

                @pl.when(jnp.logical_or(to_img != img, to_cell != cell))
                def _():
                    send_message(msg, inbox, sems.at[4], sems.at[5], to_img, to_cell)

                return carry

            lax.fori_loop(0, 8, send_step, 0)
        return carry

    lax.fori_loop(0, 8, reply_step, 0)
    own = pl.ds(pl.multiple_of(me * 8, 8), PAIRS)
    inbox[own, :] = msg[own, :]

    wait_rows(inbox, (DEVICES - 1) * PAIRS, sems.at[5])

    def table_step(h, carry):
        values = unpack_message(
            inbox,
            lambda i: pl.ds(h * 128 + i, 8, stride=16),
            lambda i: pl.ds(h * 128 + 8 + i, 8, stride=16),
        )
        for f in range(FEATS):
            table[pl.ds(pl.multiple_of(f * ROWS + h * 8, 8), 8), :] = values[f]
        return carry

    lax.fori_loop(0, 8, table_step, 0)
    make_parts(table, parts)

    def list_step(k, carry):
        got = gather_blocks(
            parts,
            [row_pair(lists, k * 8 + 2 * n) for n in range(4)],
            [
                hot_list[:, pl.ds(pl.multiple_of(k * 1024 + n * 256, 256), 256)]
                for n in range(4)
            ],
        )
        for n in range(4):
            for row in range(2):
                for f in range(FEATS):
                    entry[pl.ds(f * TILES + k * 8 + 2 * n + row, 1), :] = got[n][f][
                        :, 128 * row : 128 * row + 128
                    ]
        return carry

    lax.fori_loop(0, 4, list_step, 0)

    def entry_row(f, t):
        return entry[pl.ds(f * TILES + t, 1), :]

    across = lax.broadcasted_iota(I32, (16, 128), 0).astype(F32) + 0.5
    lane_row = lax.broadcasted_iota(I32, (1, 128), 1)

    def spans(tile_row, k):
        return [tile_row * 16 + k * GROUP + n for n in range(GROUP)]

    def pixels_of(t):
        return pl.ds(pl.multiple_of(t * 256, 256), 256)

    for tile_row in range(2):

        def render_step(k, carry, tile_row=tile_row):
            tiles = spans(tile_row, k)
            alphas, sums = [], []
            for n, t in enumerate(tiles):
                alive = lane_row < len_ref[tile_row, k * GROUP + n]
                opacity = jnp.where(alive, entry_row(5, t), 0.0)
                dx = across - entry_row(0, t)
                center_y = entry_row(1, t)
                square_x = (-0.5 * entry_row(2, t)) * dx * dx
                mixed = -entry_row(3, t) * dx
                half_y = -0.5 * entry_row(4, t)
                alpha = []
                for y in range(16):
                    dy = (y + 0.5) - center_y
                    alpha.append(opacity * jnp.exp(square_x + dy * (mixed + half_y * dy)))
                alpha = jnp.concatenate(alpha, axis=0)
                logs = jnp.log(1.0 - alpha)
                sums.append(
                    jnp.dot(
                        jnp.concatenate(two_parts(logs), axis=1),
                        tri_before[...],
                        preferred_element_type=F32,
                    )
                )
                ratio[pixels_of(t), :] = alpha * jnp.exp(-logs)
                alphas.append(alpha)
            products = []
            for n, t in enumerate(tiles):
                weight = jnp.concatenate(two_parts(jnp.exp(sums[n]) * alphas[n]), axis=1)
                weights[pixels_of(t), :] = weight
                colour = [two_parts(entry_row(6 + c, t)) for c in range(3)]
                lhs = jnp.concatenate(
                    [c[part] for part in range(2) for c in colour] + [jnp.zeros((10, 128), BF16)],
                    axis=0,
                )
                products.append(
                    lax.dot_general(
                        jnp.concatenate([lhs, lhs], axis=1),
                        weight,
                        (((1,), (1,)), ((), ())),
                        preferred_element_type=F32,
                    )
                )
            for n in range(GROUP):
                for c in range(3):
                    tile_rows[pl.ds(tile_row * 48 + c * 16 + k * GROUP + n, 1), :] = (
                        products[n][c : c + 1] + products[n][3 + c : 4 + c]
                    )
            return carry

        lax.fori_loop(0, 16 // GROUP, render_step, 0)

    picture = swap_blocks(tile_rows[...])
    for lane_tile in range(2):
        ext_render[pl.ds(border_block(1 + lane_tile, 1), 96), :] = picture[
            :, 128 * lane_tile : 128 * lane_tile + 128
        ]
    border_copies(ext_render, img, cell, sems.at[6], sems.at[7])
    wait_rows(ext_render, BORDER_ROWS, sems.at[7])

    for c in range(3):
        for row_block in range(4):
            parts = window(ext_render, img, cell, c, row_block)
            start, stride = map_base(3, c)
            for j in range(3):
                rows = pl.ds(start + j * stride + row_block * 16, 16)
                v = parts[j]
                for m, value in ((0, v), (1, v * v), (2, v * maps[rows, :])):
                    first, step = map_base(m, c)
                    maps[pl.ds(first + j * step + row_block * 16, 16), :] = value
    row_at = lax.broadcasted_iota(I32, (48, 384), 0) + (img * 32 - 5)
    lane_at = lax.broadcasted_iota(I32, (48, 384), 1) + (cell * 256 - 64)
    inside = (row_at >= 0) & (row_at < N_IMG * 32) & (lane_at >= 0) & (lane_at < N_CELL * 256)
    for c in range(3):
        mean, square, cross = [
            blur_along(blur_down(maps, map_base(m, c), 6, 48)) for m in range(3)
        ]
        mean_target = blurred[pl.ds(c * 48, 48), :]
        square_target = blurred[pl.ds((3 + c) * 48, 48), :]
        similarity, pullback = jax.vjp(
            lambda a, b, d: ssim_value(a, mean_target, b, square_target, d), mean, square, cross
        )
        for m, v in enumerate(pullback(jnp.full((48, 384), -WEIGHT_SSIM, F32))):
            v = jnp.where(inside, v, 0.0)
            for j in range(3):
                coefs[pl.ds(((m * 3 + c) * 3 + j) * 48, 48), :] = v[:, 128 * j : 128 * j + 128]
    for c in range(3):
        back_mean, back_square, back_cross = [
            blur_along(blur_down(coefs, ((m * 3 + c) * 3 * 48, 48), 0, 32))[:, 64:320]
            for m in range(3)
        ]
        for t in range(2):
            rows = slice(16 * t, 16 * t + 16)
            image = jnp.concatenate(
                [
                    ext_render[pl.ds(border_block(1 + k, 1 + t) + c * 16, 16), :]
                    for k in range(2)
                ],
                axis=1,
            )
            wanted = target[c, rows, :]
            difference = image - wanted
            tile_rows[pl.ds(t * 48 + c * 16, 16), :] = (
                (1.0 - WEIGHT_SSIM)
                * difference
                / jnp.sqrt(difference * difference + SMOOTHING * SMOOTHING)
                + back_mean[rows]
                + 2.0 * image * back_square[rows]
                + wanted * back_cross[rows]
            )
    tile_rows[...] = swap_blocks(tile_rows[...])

    for tile_row in range(2):

        def back_step(k, carry, tile_row=tile_row):
            tiles = spans(tile_row, k)
            grad_rows, values = [], []
            for n, t in enumerate(tiles):
                pixel_grad = [
                    two_parts(tile_rows[pl.ds(tile_row * 48 + c * 16 + k * GROUP + n, 1), :])
                    for c in range(3)
                ]
                colour = [two_parts(entry_row(6 + c, t)) for c in range(3)]
                tops, lows = [g[0] for g in pixel_grad], [g[1] for g in pixel_grad]
                grad_rows.append(
                    jnp.concatenate(tops + lows + tops + [jnp.zeros((7, 256), BF16)], axis=0)
                )
                colour_rows = jnp.concatenate(
                    [c[0] for c in colour] * 2
                    + [c[1] for c in colour]
                    + [jnp.zeros((7, 128), BF16)],
                    axis=0,
                )
                values.append(
                    lax.dot_general(
                        grad_rows[n],
                        colour_rows,
                        (((0,), (0,)), ((), ())),
                        preferred_element_type=F32,
                    )
                )
            gains, laters, mixes = [], [], []
            for n, t in enumerate(tiles):
                weight = weights[pixels_of(t), :]
                mixes.append(jnp.dot(grad_rows[n], weight, preferred_element_type=F32))
                gain = values[n] * (weight[:, :128].astype(F32) + weight[:, 128:].astype(F32))
                laters.append(
                    jnp.dot(
                        jnp.concatenate(two_parts(gain), axis=1),
                        tri_after[...],
                        preferred_element_type=F32,
                    )
                )
                gains.append(gain)
            for n, t in enumerate(tiles):
                pull = gains[n] - ratio[pixels_of(t), :] * laters[n]
                dx = across - entry_row(0, t)
                center_y = entry_row(1, t)
                sum_0 = sum_y = sum_yy = None
                for y in range(16):
                    dy = (y + 0.5) - center_y
                    part = pull[16 * y : 16 * y + 16]
                    part_y = part * dy
                    part_yy = part_y * dy
                    sum_0 = part if y == 0 else sum_0 + part
                    sum_y = part_y if y == 0 else sum_y + part_y
                    sum_yy = part_yy if y == 0 else sum_yy + part_yy
                sum_x = sum_0 * dx
                found = [sum_0, sum_x, sum_y, sum_x * dx, sum_y * dx, sum_yy]
                for m in range(6):
                    moments[pl.ds(m * TILES + t, 1), :] = jnp.sum(
                        found[m], axis=0, keepdims=True
                    )
                for c in range(3):
                    both = mixes[n][c : c + 1] + mixes[n][3 + c : 4 + c]
                    moments[pl.ds((6 + c) * TILES + t, 1), :] = both[:, :128] + both[:, 128:]
            return carry

        lax.fori_loop(0, 16 // GROUP, back_step, 0)

    feat = [entry[f * TILES : (f + 1) * TILES, :] for f in range(6)]
    mom = [moments[m * TILES : (m + 1) * TILES, :] for m in range(6)]
    entry[0:TILES, :] = feat[2] * mom[1] + feat[3] * mom[2]
    entry[TILES : 2 * TILES, :] = feat[3] * mom[1] + feat[4] * mom[2]
    entry[2 * TILES : 3 * TILES, :] = -0.5 * mom[3]
    entry[3 * TILES : 4 * TILES, :] = -mom[4]
    entry[4 * TILES : 5 * TILES, :] = -0.5 * mom[5]
    entry[5 * TILES : 6 * TILES, :] = mom[0]
    entry[6 * TILES : 9 * TILES, :] = moments[6 * TILES : 9 * TILES, :]

    acc[...] = jnp.zeros_like(acc)

    def slot_step(k, carry):
        at = [k * 8 + 2 * n for n in range(4)]
        scatter_blocks(
            [row_pair(lists, a) for a in at],
            [[row_pair(entry, f * TILES + a) for f in range(FEATS)] for a in at],
            hot_list[:, pl.ds(pl.multiple_of(k * 1024, 1024), 1024)],
            acc,
        )
        return carry

    lax.fori_loop(0, TILES // 8, slot_step, 0)

    def total_rows(f, h):
        a = acc[pl.ds(pl.multiple_of(f * 32 + h * 8, 8), 8), :]
        b = acc[pl.ds(pl.multiple_of(288 + f * 32 + h * 8, 8), 8), :]
        return a + b

    def back_pack(h, carry):
        totals = [total_rows(f, h) for f in range(FEATS)]
        for half in range(2):
            pack_message(
                [v[:, 128 * half : 128 * half + 128] for v in totals],
                msg_back,
                lambda i: pl.ds(h * 256 + (2 * half) * 8 + i, 8, stride=32),
                lambda i: pl.ds(h * 256 + (2 * half + 1) * 8 + i, 8, stride=32),
            )
        return carry

    lax.fori_loop(0, 4, back_pack, 0)
    each_peer(
        img,
        cell,
        lambda pi, pc: send_message(msg_back, inbox_back, sems.at[8], sems.at[9], pi, pc),
    )
    inbox_back[own, :] = msg_back[own, :]

    acc[...] = jnp.zeros_like(acc)
    wait_rows(inbox_back, (DEVICES - 1) * PAIRS, sems.at[9])

    def owner_unpack(c, carry):
        values = unpack_message(
            inbox_back,
            lambda i: pl.ds(c * 64 + i, 8, stride=8),
            lambda i: pl.ds(512 + c * 64 + i, 8, stride=8),
        )
        for f in range(FEATS):
            table[pl.ds(pl.multiple_of(f * ROWS + c * 8, 8), 8), :] = values[f]
        return carry

    lax.fori_loop(0, 8, owner_unpack, 0)

    def owner_step(k, carry):
        at = [k * 8 + 2 * n for n in range(4)]
        scatter_blocks(
            [row_pair(ids_own, a) for a in at],
            [[row_pair(table, f * ROWS + a) for f in range(FEATS)] for a in at],
            hot_own[:, pl.ds(pl.multiple_of(k * 1024, 1024), 1024)],
            acc,
        )
        return carry

    lax.fori_loop(0, ROWS // 8, owner_step, 0)

    def finish(h, carry):
        for f in range(FEATS):
            v = total_rows(f, h)
            for half in range(2):
                out[pl.ds(f * ROWS + h * 16 + half, 8, stride=2), :] = v[
                    :, 128 * half : 128 * half + 128
                ]
        return carry

    lax.fori_loop(0, 4, finish, 0)

    wait_rows(ids_in, DEVICES - 1, sems.at[0])
    wait_rows(ext_target, BORDER_ROWS, sems.at[2])
    wait_rows(msg, (DEVICES - 1) * PAIRS, sems.at[4])
    wait_rows(ext_render, BORDER_ROWS, sems.at[6])
    wait_rows(msg_back, (DEVICES - 1) * PAIRS, sems.at[8])


def pullback_kernel(cam_ref, attr_hbm, feat_grad, out_hbm, attr, arows, result, load_sems, save_sem):
    cam = read_camera(cam_ref)

    def block(h):
        return pl.ds(pl.multiple_of(h * 1024, 1024), 1024)

    def load(h):
        return pltpu.make_async_copy(
            attr_hbm.at[:, block(h)], attr.at[:, block(h)], load_sems.at[h]
        )

    for h in range(8):
        load(h).start()

    def step(h, carry):
        load(h).wait()
        for k in range(8):
            lanes = pl.ds(pl.multiple_of(h * 1024 + k * 128, 128), 128)
            for g in range(8):
                n = min(8, ATTRS - 8 * g)
                arows[g * 64 + 8 * k : g * 64 + 8 * k + n, :] = attr[8 * g : 8 * g + n, lanes]
        places = [pl.ds((r // 8) * 64 + r % 8, 8, stride=8) for r in range(ATTRS)]
        rows = [arows[at, :] for at in places]
        _, pullback = jax.vjp(lambda r: project(r, cam), rows)
        grads = [
            feat_grad[pl.ds(pl.multiple_of(f * ROWS + h * 8, 8), 8), :] for f in range(FEATS)
        ]
        log_opacity = grads.pop(5)
        (found,) = pullback(grads)
        found[10] = log_opacity * (1.0 - jax.nn.sigmoid(rows[10]))
        for at, v in zip(places, found):
            arows[at, :] = v
        for k in range(8):
            lanes = pl.ds(pl.multiple_of(h * 1024 + k * 128, 128), 128)
            for g in range(8):
                n = min(8, ATTRS - 8 * g)
                result[8 * g : 8 * g + n, lanes] = arows[g * 64 + 8 * k : g * 64 + 8 * k + n, :]
        pltpu.make_async_copy(result.at[:, block(h)], out_hbm.at[:, block(h)], save_sem).start()
        return carry

    lax.fori_loop(0, 8, step, 0)
    pltpu.make_async_copy(result, out_hbm, save_sem).wait()


def shards(attributes, camera, target, visible_index, tile_lists, tile_len):
    vmem = pl.BlockSpec(memory_space=pltpu.VMEM)
    smem = pl.BlockSpec(memory_space=pltpu.SMEM)
    feat_grad = pl.pallas_call(
        step_kernel,
        out_shape=jax.ShapeDtypeStruct((FEATS * ROWS, 128), F32),
        in_specs=[smem, smem, vmem, pl.BlockSpec(memory_space=pl.ANY), vmem, vmem],
        out_specs=vmem,
        scratch_shapes=[
            pltpu.VMEM((ATTRS, 8192), F32),
            pltpu.VMEM((4096, 128), F32),
            pltpu.VMEM((FEATS * ROWS, 128), F32),
            pltpu.VMEM((FEATS * 32, 768), BF16),
            pltpu.VMEM((256, TILES * LIST), BF16),
            pltpu.VMEM((256, ROWS * 128), BF16),
            pltpu.VMEM((DEVICES, 128), I32),
            pltpu.VMEM((ROWS, 128), I32),
            pltpu.VMEM((DEVICES * 8, 128), F32),
            pltpu.VMEM((DEVICES * 8, 128), F32),
            pltpu.VMEM((DEVICES * 8, 128), F32),
            pltpu.VMEM((DEVICES * 8, 128), F32),
            pltpu.VMEM((16 * 48, 128), F32),
            pltpu.VMEM((16 * 48, 128), F32),
            pltpu.VMEM((FEATS * TILES, 128), F32),
            pltpu.VMEM((256, 128), BF16),
            pltpu.VMEM((256, 128), BF16),
            pltpu.VMEM((TILES * 256, 256), BF16),
            pltpu.VMEM((TILES * 256, 128), F32),
            pltpu.VMEM((96, 256), F32),
            pltpu.VMEM((FEATS * TILES, 128), F32),
            pltpu.VMEM((5 * 3 * 3 * 64, 128), F32),
            pltpu.VMEM((3 * 3 * 3 * 48, 128), F32),
            pltpu.VMEM((2 * 3 * 48, 384), F32),
            pltpu.VMEM((2 * FEATS * 32, 256), F32),
            pltpu.SemaphoreType.DMA((11,)),
        ],
        compiler_params=pltpu.CompilerParams(
            collective_id=0, has_side_effects=True, vmem_limit_bytes=56 * 1024 * 1024
        ),
        name="splat_step",
    )(
        camera,
        tile_len,
        visible_index.reshape(ROWS, 128),
        attributes,
        target,
        tile_lists.reshape(TILES, LIST),
    )
    return pl.pallas_call(
        pullback_kernel,
        out_shape=jax.ShapeDtypeStruct(attributes.shape, F32),
        in_specs=[smem, pl.BlockSpec(memory_space=pl.ANY), vmem],
        out_specs=pl.BlockSpec(memory_space=pl.ANY),
        scratch_shapes=[
            pltpu.VMEM((ATTRS, 8192), F32),
            pltpu.VMEM((512, 128), F32),
            pltpu.VMEM((ATTRS, 8192), F32),
            pltpu.SemaphoreType.DMA((8,)),
            pltpu.SemaphoreType.DMA,
        ],
        name="splat_pullback",
    )(camera, attributes, feat_grad)


def solution(mesh):
    return jax.shard_map(
        shards,
        mesh=mesh,
        in_specs=(
            P(None, ("img", "cell")),
            P(),
            P(None, "img", "cell"),
            P(("img", "cell"), None),
            P("img", "cell", None),
            P("img", "cell"),
        ),
        out_specs=P(None, ("img", "cell")),
        check_vma=False,
    )
```

```python
import math

import jax
import jax.numpy as jnp
from jax import lax
from jax.experimental import pallas as pl
from jax.experimental.pallas import tpu as pltpu
from jax.sharding import PartitionSpec as P

F32 = jnp.float32
BF16 = jnp.bfloat16
I32 = jnp.int32
MESH = pl.DeviceIdType.MESH

TILE = 16
N_IMG = 8
N_CELL = 16
DEVICES = 128
LIST = 128
TILES = 32
ATTRS = 59
ROWS = 64
FEATS = 9
PAIRS = 5
EXACT = 5
BLOCKS = 8
GROUP = 4

WEIGHT_SSIM = 0.2
SMOOTHING = 0.01
STAB_ONE = 0.0001
STAB_TWO = 0.0009
BLUR_SIGMA = 1.5
SH_ZERO = 0.28209479177387814
SH_ONE = 0.4886025119029199
SH_TWO = (
    1.0925484305920792,
    -1.0925484305920792,
    0.31539156525252005,
    -1.0925484305920792,
    0.5462742152960396,
)
SH_THREE = (
    -0.5900435899266435,
    2.890611442640554,
    -0.4570457994644658,
    0.3731763325901154,
    -0.4570457994644658,
    1.445305721320277,
    -0.5900435899266435,
)


def blur_taps():
    raw = [math.exp(-((o - 5.0) ** 2) / (2.0 * BLUR_SIGMA * BLUR_SIGMA)) for o in range(11)]
    return [r / sum(raw) for r in raw]


TAPS = blur_taps()


def harmonic_basis(ux, uy, uz):
    xx, yy, zz = ux * ux, uy * uy, uz * uz
    return [
        SH_ZERO,
        -SH_ONE * uy,
        SH_ONE * uz,
        -SH_ONE * ux,
        SH_TWO[0] * ux * uy,
        SH_TWO[1] * uy * uz,
        SH_TWO[2] * (2.0 * zz - xx - yy),
        SH_TWO[3] * ux * uz,
        SH_TWO[4] * (xx - yy),
        SH_THREE[0] * uy * (3.0 * xx - yy),
        SH_THREE[1] * ux * uy * uz,
        SH_THREE[2] * uy * (4.0 * zz - xx - yy),
        SH_THREE[3] * uz * (2.0 * zz - 3.0 * xx - 3.0 * yy),
        SH_THREE[4] * ux * (4.0 * zz - xx - yy),
        SH_THREE[5] * uz * (xx - yy),
        SH_THREE[6] * ux * (xx - 3.0 * yy),
    ]


def project(rows, cam):
    pos = rows[0:3]
    scales = [jnp.exp(r) for r in rows[3:6]]
    qw = 1.5 + jnp.tanh(rows[6])
    qx, qy, qz = rows[7:10]
    inv = 1.0 / jnp.sqrt(qw * qw + qx * qx + qy * qy + qz * qz)
    qw, qx, qy, qz = qw * inv, qx * inv, qy * inv, qz * inv
    rot = [
        [1.0 - 2.0 * (qy * qy + qz * qz), 2.0 * (qx * qy - qw * qz), 2.0 * (qx * qz + qw * qy)],
        [2.0 * (qx * qy + qw * qz), 1.0 - 2.0 * (qx * qx + qz * qz), 2.0 * (qy * qz - qw * qx)],
        [2.0 * (qx * qz - qw * qy), 2.0 * (qy * qz + qw * qx), 1.0 - 2.0 * (qx * qx + qy * qy)],
    ]
    axes = [
        [
            (cam[s][0] * rot[0][k] + cam[s][1] * rot[1][k] + cam[s][2] * rot[2][k]) * scales[k]
            for k in range(3)
        ]
        for s in range(2)
    ]
    cov_a = axes[0][0] * axes[0][0] + axes[0][1] * axes[0][1] + axes[0][2] * axes[0][2] + 0.3
    cov_b = axes[0][0] * axes[1][0] + axes[0][1] * axes[1][1] + axes[0][2] * axes[1][2]
    cov_c = axes[1][0] * axes[1][0] + axes[1][1] * axes[1][1] + axes[1][2] * axes[1][2] + 0.3
    inv_det = 1.0 / (cov_a * cov_c - cov_b * cov_b)
    centers = [
        8.0
        + 7.0 * jnp.sin((cam[s][0] * pos[0] + cam[s][1] * pos[1] + cam[s][2] * pos[2]) / 3.0)
        for s in range(2)
    ]
    off = [pos[k] - cam[2][k] for k in range(3)]
    inv_dist = 1.0 / jnp.sqrt(off[0] * off[0] + off[1] * off[1] + off[2] * off[2])
    basis = harmonic_basis(off[0] * inv_dist, off[1] * inv_dist, off[2] * inv_dist)
    colours = []
    for c in range(3):
        total = 0.5 + basis[0] * rows[11 + 16 * c]
        for m in range(1, 16):
            total = total + basis[m] * rows[11 + 16 * c + m]
        colours.append(total)
    return centers + [cov_c * inv_det, -cov_b * inv_det, cov_a * inv_det] + colours


def read_camera(cam):
    return [[cam[s, k] for k in range(3)] for s in range(3)]


def spread_rows(attr, arows):
    def step(ct, carry):
        lanes = pl.ds(pl.multiple_of(ct * 128, 128), 128)
        for g in range(8):
            n = min(8, ATTRS - 8 * g)
            arows[pl.ds(pl.multiple_of(g * 512 + ct * 8, 8), n), :] = attr[8 * g : 8 * g + n, lanes]
        return carry

    lax.fori_loop(0, 64, step, 0)


def attr_rows(h):
    return [pl.ds((r // 8) * 512 + h * 64 + r % 8, 8, stride=8) for r in range(ATTRS)]


def wrap(value, count):
    return jnp.where(value >= count, value - count, value)


def each_peer(img, cell, act):
    base = wrap(cell + 8, N_CELL)
    for i in (4, 5, 3, 2, 6, 1, 7, 0):
        pi = wrap(img + i, N_IMG) if i else img

        def step(j, carry, pi=pi):
            act(pi, wrap(base + j, N_CELL))
            return carry

        if i:
            lax.fori_loop(0, N_CELL, step, 0)
        else:
            lax.fori_loop(0, 8, step, 0)
            lax.fori_loop(9, N_CELL, step, 0)


def left_half():
    return lax.broadcasted_iota(I32, (8, 128), 1) < 64


def pack_message(values, msg, low_row, high_row):
    left = left_half()
    for i in range(PAIRS):
        a = values[2 * i]
        b = values[2 * i + 1] if 2 * i + 1 < FEATS else a
        msg[low_row(i), :] = jnp.where(left, a, pltpu.roll(b, 64, 1))
        msg[high_row(i), :] = jnp.where(left, pltpu.roll(a, 64, 1), b)


def unpack_message(msg, low_row, high_row):
    left = left_half()
    values = []
    for i in range(PAIRS):
        low, high = msg[low_row(i), :], msg[high_row(i), :]
        values.append(jnp.where(left, low, pltpu.roll(high, 64, 1)))
        if 2 * i + 1 < FEATS:
            values.append(jnp.where(left, pltpu.roll(low, 64, 1), high))
    return values


def one_hot(low):
    return jnp.where(lax.broadcasted_iota(I32, (256, 256), 0) == low, 1.0, 0.0).astype(BF16)


def split_ids(ids):
    high = lax.shift_right_logical(ids, 8)
    return high, ids - lax.shift_left(high, 8)


def row_pair(ref, at):
    both = ref[pl.ds(at, 2), :]
    return jnp.concatenate([both[0:1], both[1:2]], axis=1)


def make_parts(table, parts, thirds):
    for f in range(FEATS):
        rows = slice(32 * f, 32 * f + 32)
        for half in range(2):
            v = table[pl.ds(f * ROWS + half, 32, stride=2), :]
            top = v.astype(BF16)
            v = v - top.astype(F32)
            middle = v.astype(BF16)
            parts[rows, 128 * half : 128 * half + 128] = top
            parts[rows, 256 + 128 * half : 384 + 128 * half] = middle
            if f < EXACT:
                low = (v - middle.astype(F32)).astype(BF16)
                thirds[rows, 128 * half : 128 * half + 128] = low


def gather_blocks(parts, thirds, ids, hots):
    found, fine = [], []
    for hot in hots:
        found.append(
            jnp.dot(
                parts[...], jnp.concatenate([hot] * 2, axis=0), preferred_element_type=F32
            )
        )
        fine.append(jnp.dot(thirds[...], hot, preferred_element_type=F32))
    out = []
    for v, low, block in zip(found, fine, ids):
        mask = lax.broadcasted_iota(I32, (32, 256), 0) == split_ids(block)[0]
        rows = []
        for f in range(FEATS):
            value = v[32 * f : 32 * f + 32]
            if f < EXACT:
                value = value + low[32 * f : 32 * f + 32]
            rows.append(jnp.sum(jnp.where(mask, value, 0.0), axis=0, keepdims=True))
        out.append(rows)
    return out


def scatter_blocks(ids, grads, hots, acc):
    lhs = []
    for block, rows in zip(ids, grads):
        mask = lax.broadcasted_iota(I32, (32, 256), 0) == split_ids(block)[0]
        upper, lower = [], []
        for g in rows:
            top = g.astype(BF16).astype(F32)
            upper.append(jnp.where(mask, top, 0.0).astype(BF16))
            lower.append(jnp.where(mask, g - top, 0.0).astype(BF16))
        lhs.append(jnp.concatenate(upper + lower, axis=0))
    acc[...] += lax.dot_general(
        jnp.concatenate(lhs, axis=1),
        hots,
        (((1,), (1,)), ((), ())),
        preferred_element_type=F32,
    )


def two_parts(v):
    top = v.astype(BF16)
    return top, (v - top.astype(F32)).astype(BF16)


def swap_blocks(z):
    rows = z.shape[0]
    row_at = lax.broadcasted_iota(I32, z.shape, 0)
    lane_at = lax.broadcasted_iota(I32, z.shape, 1)
    for bit in (1, 2, 4, 8):
        row_bit = (row_at // bit) % 2
        lane_bit = (lane_at // (16 * bit)) % 2
        down = pltpu.roll(pltpu.roll(z, rows - bit, 0), 16 * bit, 1)
        up = pltpu.roll(pltpu.roll(z, bit, 0), 256 - 16 * bit, 1)
        z = jnp.where(row_bit == lane_bit, z, jnp.where(row_bit == 0, down, up))
    return z


NORTH, SOUTH, PACK_WEST, PACK_EAST, FROM_WEST, FROM_EAST = 192, 288, 384, 400, 416, 432
FROM_NW, FROM_NE, FROM_SW, FROM_SE, EXT_ROWS = 448, 456, 464, 472, 480
BORDER_ROWS = 256


def pack_columns(ext):
    lane = lax.broadcasted_iota(I32, (8, 128), 1)
    for t in range(2):
        west = jnp.zeros((8, 128), F32)
        east = west
        for k in range(6):
            here = (lane >= 16 * k) & (lane < 16 * k + 16)
            at = t * 48 + 8 * k
            first, last = ext[at : at + 8, :], ext[96 + at : 104 + at, :]
            west = jnp.where(here, pltpu.roll(first, 16 * k, 1) if k else first, west)
            east = jnp.where(here, pltpu.roll(last, 16 * k + 16, 1), east)
        ext[PACK_WEST + 8 * t : PACK_WEST + 8 * t + 8, :] = west
        ext[PACK_EAST + 8 * t : PACK_EAST + 8 * t + 8, :] = east


def border_copies(ext, img, cell, send, recv):
    west, east = jnp.where(cell == 0, N_CELL - 1, cell - 1), wrap(cell + 1, N_CELL)
    north, south = jnp.where(img == 0, N_IMG - 1, img - 1), wrap(img + 1, N_IMG)
    plan = [
        (PACK_WEST, FROM_SE, 8, north, west),
        (PACK_EAST, FROM_SW, 8, north, east),
        (PACK_WEST + 8, FROM_NE, 8, south, west),
        (PACK_EAST + 8, FROM_NW, 8, south, east),
        (PACK_WEST, FROM_EAST, 16, img, west),
        (PACK_EAST, FROM_WEST, 16, img, east),
    ]
    for k in range(2):
        plan.append((96 * k, SOUTH + 48 * k, 48, north, cell))
        plan.append((96 * k + 48, NORTH + 48 * k, 48, south, cell))
    for source, dest, count, to_img, to_cell in plan:
        pltpu.make_async_remote_copy(
            src_ref=ext.at[pl.ds(source, count)],
            dst_ref=ext.at[pl.ds(dest, count)],
            send_sem=send,
            recv_sem=recv,
            device_id=(to_img, to_cell),
            device_id_type=MESH,
        ).start()


def wait_rows(ref, count, sem):
    part = ref.at[pl.ds(0, count)]
    pltpu.make_async_copy(part, part, sem).wait()


def window(ext, img, cell, c, row_block, half):
    lane = lax.broadcasted_iota(I32, (8, 128), 1)
    at = 16 * c + 8 * half
    bases = [NORTH, 0, 48, SOUTH][row_block]
    step = 48 if row_block in (0, 3) else 96
    sides = [
        (FROM_NW, FROM_NE),
        (FROM_WEST, FROM_EAST),
        (FROM_WEST + 8, FROM_EAST + 8),
        (FROM_SW, FROM_SE),
    ][row_block]
    first = pltpu.roll(ext[bases + at : bases + at + 8, :], 64, 1)
    second = pltpu.roll(ext[bases + step + at : bases + step + at + 8, :], 64, 1)
    block = 16 * (2 * c + half)
    left = pltpu.roll(ext[sides[0] : sides[0] + 8, :], (48 - block) % 128, 1)
    right = pltpu.roll(ext[sides[1] : sides[1] + 8, :], (64 - block) % 128, 1)
    keep_left = jnp.where(cell == 0, 64, 48)
    keep_right = jnp.where(cell == N_CELL - 1, 64, 80)
    tiles = [
        jnp.where(lane < 64, jnp.where(lane >= keep_left, left, 0.0), first),
        jnp.where(lane < 64, first, second),
        jnp.where(lane < 64, second, jnp.where(lane < keep_right, right, 0.0)),
    ]
    if row_block == 0:
        tiles = [v * jnp.where(img == 0, 0.0, 1.0) for v in tiles]
    if row_block == 3:
        tiles = [v * jnp.where(img == N_IMG - 1, 0.0, 1.0) for v in tiles]
    return tiles


def blur(ref, start, stride):
    down = []
    for j in range(3):
        at = start + j * stride
        total = TAPS[5] * ref[pl.ds(at + 5, 8), :]
        for o in range(5):
            total = total + TAPS[o] * (ref[pl.ds(at + o, 8), :] + ref[pl.ds(at + 10 - o, 8), :])
        down.append(total)
    v = jnp.concatenate(down, axis=1)
    total = TAPS[5] * v
    for o in range(5):
        d = 5 - o
        total = total + TAPS[o] * (pltpu.roll(v, d, 1) + pltpu.roll(v, 384 - d, 1))
    return total


def ssim_value(mean_render, mean_target, square_render, square_target, cross_term):
    spread_render = square_render - mean_render * mean_render
    spread_target = square_target - mean_target * mean_target
    covariance = cross_term - mean_render * mean_target
    upper = (2.0 * mean_render * mean_target + STAB_ONE) * (2.0 * covariance + STAB_TWO)
    lower = (mean_render * mean_render + mean_target * mean_target + STAB_ONE) * (
        spread_render + spread_target + STAB_TWO
    )
    return upper / lower


def map_row(m, c):
    return (m * 3 + c) * 3 * 64


def step_kernel(
    cam_ref,
    len_ref,
    vis,
    attr_hbm,
    target,
    lists,
    out,
    attr,
    arows,
    table,
    parts,
    thirds,
    hot_list,
    hot_own,
    ids_in,
    ids_own,
    msg,
    inbox,
    msg_back,
    inbox_back,
    ext_render,
    ext_target,
    entry,
    tri_before,
    tri_after,
    weights,
    ratio,
    tile_rows,
    moments,
    maps,
    coefs,
    blurred,
    acc,
    sems,
):
    img = lax.axis_index("img")
    cell = lax.axis_index("cell")
    me = img * N_CELL + cell

    barrier = pltpu.get_barrier_semaphore()
    each_peer(
        img,
        cell,
        lambda pi, pc: pl.semaphore_signal(
            barrier, 1, device_id=(pi, pc), device_id_type=MESH
        ),
    )
    load_attr = pltpu.make_async_copy(attr_hbm, attr, sems.at[10])
    load_attr.start()

    for k in range(2):
        for t in range(2):
            for c in range(3):
                at = 96 * k + 48 * t + 16 * c
                ext_target[at : at + 16, :] = target[
                    c, 16 * t : 16 * t + 16, 128 * k : 128 * k + 128
                ]
    pack_columns(ext_target)

    def list_hot(b, carry):
        hot_list[:, pl.ds(pl.multiple_of(b * 256, 256), 256)] = one_hot(
            split_ids(row_pair(lists, b * 2))[1]
        )
        return carry

    lax.fori_loop(0, TILES // 2, list_hot, 0)

    cam = read_camera(cam_ref)
    load_attr.wait()
    spread_rows(attr, arows)

    def project_step(h, carry):
        rows = [arows[at, :] for at in attr_rows(h)]
        feats = project(rows, cam)
        feats.insert(5, jax.nn.sigmoid(rows[10]))
        for f in range(FEATS):
            table[pl.ds(pl.multiple_of(f * ROWS + h * 8, 8), 8), :] = feats[f]
        return carry

    lax.fori_loop(0, 8, project_step, 0)
    make_parts(table, parts, thirds)

    row_at = lax.broadcasted_iota(I32, (128, 128), 0)
    lane_at = lax.broadcasted_iota(I32, (128, 128), 1)
    before = jnp.where(row_at < lane_at, 1.0, 0.0).astype(BF16)
    after = jnp.where(row_at > lane_at, 1.0, 0.0).astype(BF16)
    for half in range(2):
        tri_before[128 * half : 128 * half + 128, :] = before
        tri_after[128 * half : 128 * half + 128, :] = after

    pl.semaphore_wait(barrier, DEVICES - 1)

    def send_ids(pi, pc):
        p = pi * N_CELL + pc
        pltpu.make_async_remote_copy(
            src_ref=vis.at[pl.ds(p // 2, 1)],
            dst_ref=ids_in.at[pl.ds(me, 1)],
            send_sem=sems.at[0],
            recv_sem=sems.at[1],
            device_id=(pi, pc),
            device_id_type=MESH,
        ).start()

    each_peer(img, cell, send_ids)
    border_copies(ext_target, img, cell, sems.at[2], sems.at[3])
    ids_in[pl.ds(me, 1), :] = vis[pl.ds(me // 2, 1), :]

    wait_rows(ext_target, BORDER_ROWS, sems.at[3])
    for c in range(3):
        for row_block in range(4):
            for half in range(2):
                strips = window(ext_target, img, cell, c, row_block, half)
                for j in range(3):
                    for m, v in ((3, strips[j]), (4, strips[j] * strips[j])):
                        at = map_row(m, c) + 64 * j + 16 * row_block + 8 * half
                        maps[at : at + 8, :] = v

    def target_blur(c, carry):
        for m in range(2):
            for r in range(6):
                at = pl.multiple_of((m * 3 + c) * 48 + 8 * r, 8)
                blurred[pl.ds(at, 8), :] = blur(maps, map_row(3 + m, c) + 6 + 8 * r, 64)
        return carry

    lax.fori_loop(0, 3, target_blur, 0)

    wait_rows(ids_in, DEVICES - 1, sems.at[1])
    odd = me - (me // 2) * 2
    left = left_half()
    for c in range(8):
        first = ids_in[8 * c : 8 * c + 8, :]
        second = ids_in[64 + 8 * c : 72 + 8 * c, :]
        even_form = jnp.where(left, first, pltpu.roll(second, 64, 1))
        odd_form = jnp.where(left, pltpu.roll(first, 64, 1), second)
        ids_own[8 * c : 8 * c + 8, :] = jnp.where(odd == 0, even_form, odd_form)

    def send_message(source, dest, send, recv, pi, pc):
        pltpu.make_async_remote_copy(
            src_ref=source.at[pl.ds(pl.multiple_of((pi * N_CELL + pc) * 8, 8), PAIRS)],
            dst_ref=dest.at[pl.ds(pl.multiple_of(me * 8, 8), PAIRS)],
            send_sem=send,
            recv_sem=recv,
            device_id=(pi, pc),
            device_id_type=MESH,
        ).start()

    left_row = lax.broadcasted_iota(I32, (1, 128), 1) < 64
    half_img = img - (img // 4) * 4
    own_group = half_img * 2 + cell // 8

    def reply_step(k, carry):
        g = wrap(own_group + 1 + k, 8)
        ids = [row_pair(ids_own, g * 8 + 2 * n) for n in range(4)]
        hots = [one_hot(split_ids(v)[1]) for v in ids]
        for n in range(4):
            hot_own[:, pl.ds(pl.multiple_of(g * 1024 + n * 256, 256), 256)] = hots[n]
        got = gather_blocks(parts, thirds, ids, hots)
        for n in range(4):
            for row in range(2):
                d = g * 8 + 2 * n + row
                for i in range(PAIRS):
                    first = got[n][2 * i][:, 128 * row : 128 * row + 128]
                    second = got[n][min(2 * i + 1, FEATS - 1)][:, 128 * row : 128 * row + 128]
                    msg[pl.ds(d * 8 + i, 1), :] = jnp.where(
                        left_row, first, pltpu.roll(second, 64, 1)
                    )
                    msg[pl.ds(512 + d * 8 + i, 1), :] = jnp.where(
                        left_row, pltpu.roll(first, 64, 1), second
                    )
        for side in range(2):
            to_img = 4 * side + g // 2

            def send_step(n, carry):
                to_cell = (g - (g // 2) * 2) * 8 + n

                @pl.when(jnp.logical_or(to_img != img, to_cell != cell))
                def _():
                    send_message(msg, inbox, sems.at[4], sems.at[5], to_img, to_cell)

                return carry

            lax.fori_loop(0, 8, send_step, 0)
        return carry

    lax.fori_loop(0, 8, reply_step, 0)
    own = pl.ds(pl.multiple_of(me * 8, 8), PAIRS)
    inbox[own, :] = msg[own, :]

    wait_rows(inbox, (DEVICES - 1) * PAIRS, sems.at[5])

    def table_step(h, carry):
        values = unpack_message(
            inbox,
            lambda i: pl.ds(h * 128 + i, 8, stride=16),
            lambda i: pl.ds(h * 128 + 8 + i, 8, stride=16),
        )
        for f in range(FEATS):
            table[pl.ds(pl.multiple_of(f * ROWS + h * 8, 8), 8), :] = values[f]
        return carry

    lax.fori_loop(0, 8, table_step, 0)
    make_parts(table, parts, thirds)

    def list_step(k, carry):
        got = gather_blocks(
            parts,
            thirds,
            [row_pair(lists, k * 8 + 2 * n) for n in range(4)],
            [
                hot_list[:, pl.ds(pl.multiple_of(k * 1024 + n * 256, 256), 256)]
                for n in range(4)
            ],
        )
        for n in range(4):
            for row in range(2):
                for f in range(FEATS):
                    entry[pl.ds(f * TILES + k * 8 + 2 * n + row, 1), :] = got[n][f][
                        :, 128 * row : 128 * row + 128
                    ]
        return carry

    lax.fori_loop(0, 4, list_step, 0)

    def entry_row(f, t):
        return entry[pl.ds(f * TILES + t, 1), :]

    across = lax.broadcasted_iota(I32, (16, 128), 0).astype(F32) + 0.5
    lane_row = lax.broadcasted_iota(I32, (1, 128), 1)

    def spans(tile_row, k):
        return [tile_row * 16 + k * GROUP + n for n in range(GROUP)]

    def pixels_of(t):
        return pl.ds(pl.multiple_of(t * 256, 256), 256)

    for tile_row in range(2):

        def render_step(k, carry, tile_row=tile_row):
            tiles = spans(tile_row, k)
            alphas, sums = [], []
            for n, t in enumerate(tiles):
                alive = lane_row < len_ref[tile_row, k * GROUP + n]
                opacity = jnp.where(alive, entry_row(5, t), 0.0)
                dx = across - entry_row(0, t)
                center_y = entry_row(1, t)
                square_x = (-0.5 * entry_row(2, t)) * dx * dx
                mixed = -entry_row(3, t) * dx
                half_y = -0.5 * entry_row(4, t)
                alpha = []
                for y in range(16):
                    dy = (y + 0.5) - center_y
                    alpha.append(opacity * jnp.exp(square_x + dy * (mixed + half_y * dy)))
                alpha = jnp.concatenate(alpha, axis=0)
                logs = jnp.log(1.0 - alpha)
                sums.append(
                    jnp.dot(
                        jnp.concatenate(two_parts(logs), axis=1),
                        tri_before[...],
                        preferred_element_type=F32,
                    )
                )
                ratio[pixels_of(t), :] = alpha * jnp.exp(-logs)
                alphas.append(alpha)
            products = []
            for n, t in enumerate(tiles):
                weight = jnp.concatenate(two_parts(jnp.exp(sums[n]) * alphas[n]), axis=1)
                weights[pixels_of(t), :] = weight
                colour = [two_parts(entry_row(6 + c, t)) for c in range(3)]
                lhs = jnp.concatenate(
                    [c[part] for part in range(2) for c in colour] + [jnp.zeros((10, 128), BF16)],
                    axis=0,
                )
                products.append(
                    lax.dot_general(
                        jnp.concatenate([lhs, lhs], axis=1),
                        weight,
                        (((1,), (1,)), ((), ())),
                        preferred_element_type=F32,
                    )
                )
            for n in range(GROUP):
                for c in range(3):
                    tile_rows[pl.ds(tile_row * 48 + c * 16 + k * GROUP + n, 1), :] = (
                        products[n][c : c + 1] + products[n][3 + c : 4 + c]
                    )
            return carry

        lax.fori_loop(0, 16 // GROUP, render_step, 0)

    picture = swap_blocks(tile_rows[...])
    for k in range(2):
        ext_render[96 * k : 96 * k + 96, :] = picture[:, 128 * k : 128 * k + 128]
    pack_columns(ext_render)
    border_copies(ext_render, img, cell, sems.at[6], sems.at[7])
    wait_rows(ext_render, BORDER_ROWS, sems.at[7])

    for c in range(3):
        for row_block in range(4):
            for half in range(2):
                strips = window(ext_render, img, cell, c, row_block, half)
                for j in range(3):
                    at = 64 * j + 16 * row_block + 8 * half
                    v = strips[j]
                    wanted = maps[map_row(3, c) + at : map_row(3, c) + at + 8, :]
                    for m, value in ((0, v), (1, v * v), (2, v * wanted)):
                        maps[map_row(m, c) + at : map_row(m, c) + at + 8, :] = value
    row_at = lax.broadcasted_iota(I32, (8, 384), 0) + (img * 32 - 5)
    lane_at = lax.broadcasted_iota(I32, (8, 384), 1) + (cell * 256 - 64)
    inside = (lane_at >= 0) & (lane_at < N_CELL * 256)

    def similarity_step(c, carry):
        for r in range(6):
            mean, square, cross = [blur(maps, map_row(m, c) + 6 + 8 * r, 64) for m in range(3)]
            mean_target, square_target = [
                blurred[pl.ds(pl.multiple_of((m * 3 + c) * 48 + 8 * r, 8), 8), :]
                for m in range(2)
            ]
            _, pullback = jax.vjp(
                lambda x, y, z, mt=mean_target, st=square_target: ssim_value(x, mt, y, st, z),
                mean,
                square,
                cross,
            )
            keep = inside & (row_at + 8 * r >= 0) & (row_at + 8 * r < N_IMG * 32)
            for m, v in enumerate(pullback(jnp.full((8, 384), -WEIGHT_SSIM, F32))):
                v = jnp.where(keep, v, 0.0)
                for j in range(3):
                    at = pl.multiple_of(((m * 3 + c) * 3 + j) * 48 + 8 * r, 8)
                    coefs[pl.ds(at, 8), :] = v[:, 128 * j : 128 * j + 128]
        return carry

    lax.fori_loop(0, 3, similarity_step, 0)
    left = left_half()

    def image_step(c, carry):
        for r in range(4):
            back_mean, back_square, back_cross = [
                blur(coefs, (m * 3 + c) * 3 * 48 + 8 * r, 48) for m in range(3)
            ]
            found = []
            for j in range(3):
                lanes = slice(128 * j, 128 * j + 128)
                at = 64 * j + 16 + 8 * r
                image = maps[pl.ds(pl.multiple_of(map_row(0, c) + at, 8), 8), :]
                wanted = maps[pl.ds(pl.multiple_of(map_row(3, c) + at, 8), 8), :]
                difference = image - wanted
                slope = (
                    (1.0 - WEIGHT_SSIM)
                    * difference
                    / jnp.sqrt(difference * difference + SMOOTHING * SMOOTHING)
                )
                found.append(
                    pltpu.roll(
                        slope
                        + back_mean[:, lanes]
                        + 2.0 * image * back_square[:, lanes]
                        + wanted * back_cross[:, lanes],
                        64,
                        1,
                    )
                )
            at = pl.multiple_of((r // 2) * 48 + c * 16 + (r % 2) * 8, 8)
            tile_rows[pl.ds(at, 8), :] = jnp.concatenate(
                [jnp.where(left, found[0], found[1]), jnp.where(left, found[1], found[2])],
                axis=1,
            )
        return carry

    lax.fori_loop(0, 3, image_step, 0)
    tile_rows[...] = swap_blocks(tile_rows[...])

    for tile_row in range(2):

        def back_step(k, carry, tile_row=tile_row):
            tiles = spans(tile_row, k)
            grad_rows, values = [], []
            for n, t in enumerate(tiles):
                pixel_grad = [
                    two_parts(tile_rows[pl.ds(tile_row * 48 + c * 16 + k * GROUP + n, 1), :])
                    for c in range(3)
                ]
                colour = [two_parts(entry_row(6 + c, t)) for c in range(3)]
                tops, lows = [g[0] for g in pixel_grad], [g[1] for g in pixel_grad]
                grad_rows.append(
                    jnp.concatenate(tops + lows + tops + [jnp.zeros((7, 256), BF16)], axis=0)
                )
                colour_rows = jnp.concatenate(
                    [c[0] for c in colour] * 2
                    + [c[1] for c in colour]
                    + [jnp.zeros((7, 128), BF16)],
                    axis=0,
                )
                values.append(
                    lax.dot_general(
                        grad_rows[n],
                        colour_rows,
                        (((0,), (0,)), ((), ())),
                        preferred_element_type=F32,
                    )
                )
            gains, laters, mixes = [], [], []
            for n, t in enumerate(tiles):
                weight = weights[pixels_of(t), :]
                mixes.append(jnp.dot(grad_rows[n], weight, preferred_element_type=F32))
                gain = values[n] * (weight[:, :128].astype(F32) + weight[:, 128:].astype(F32))
                laters.append(
                    jnp.dot(
                        jnp.concatenate(two_parts(gain), axis=1),
                        tri_after[...],
                        preferred_element_type=F32,
                    )
                )
                gains.append(gain)
            for n, t in enumerate(tiles):
                pull = gains[n] - ratio[pixels_of(t), :] * laters[n]
                dx = across - entry_row(0, t)
                center_y = entry_row(1, t)
                sum_0 = sum_y = sum_yy = None
                for y in range(16):
                    dy = (y + 0.5) - center_y
                    part = pull[16 * y : 16 * y + 16]
                    part_y = part * dy
                    part_yy = part_y * dy
                    sum_0 = part if y == 0 else sum_0 + part
                    sum_y = part_y if y == 0 else sum_y + part_y
                    sum_yy = part_yy if y == 0 else sum_yy + part_yy
                sum_x = sum_0 * dx
                found = [sum_0, sum_x, sum_y, sum_x * dx, sum_y * dx, sum_yy]
                for m in range(6):
                    moments[pl.ds(m * TILES + t, 1), :] = jnp.sum(
                        found[m], axis=0, keepdims=True
                    )
                for c in range(3):
                    both = mixes[n][c : c + 1] + mixes[n][3 + c : 4 + c]
                    moments[pl.ds((6 + c) * TILES + t, 1), :] = both[:, :128] + both[:, 128:]
            return carry

        lax.fori_loop(0, 16 // GROUP, back_step, 0)

    feat = [entry[f * TILES : (f + 1) * TILES, :] for f in range(6)]
    mom = [moments[m * TILES : (m + 1) * TILES, :] for m in range(6)]
    entry[0:TILES, :] = feat[2] * mom[1] + feat[3] * mom[2]
    entry[TILES : 2 * TILES, :] = feat[3] * mom[1] + feat[4] * mom[2]
    entry[2 * TILES : 3 * TILES, :] = -0.5 * mom[3]
    entry[3 * TILES : 4 * TILES, :] = -mom[4]
    entry[4 * TILES : 5 * TILES, :] = -0.5 * mom[5]
    entry[5 * TILES : 6 * TILES, :] = mom[0]
    entry[6 * TILES : 9 * TILES, :] = moments[6 * TILES : 9 * TILES, :]

    acc[...] = jnp.zeros_like(acc)

    def slot_step(k, carry):
        at = [k * 2 * BLOCKS + 2 * n for n in range(BLOCKS)]
        scatter_blocks(
            [row_pair(lists, a) for a in at],
            [[row_pair(entry, f * TILES + a) for f in range(FEATS)] for a in at],
            hot_list[:, pl.ds(pl.multiple_of(k * 256 * BLOCKS, 256), 256 * BLOCKS)],
            acc,
        )
        return carry

    lax.fori_loop(0, TILES // (2 * BLOCKS), slot_step, 0)

    def total_rows(f, h):
        a = acc[pl.ds(pl.multiple_of(f * 32 + h * 8, 8), 8), :]
        b = acc[pl.ds(pl.multiple_of(288 + f * 32 + h * 8, 8), 8), :]
        return a + b

    def back_pack(h, carry):
        totals = [total_rows(f, h) for f in range(FEATS)]
        for half in range(2):
            pack_message(
                [v[:, 128 * half : 128 * half + 128] for v in totals],
                msg_back,
                lambda i: pl.ds(h * 256 + (2 * half) * 8 + i, 8, stride=32),
                lambda i: pl.ds(h * 256 + (2 * half + 1) * 8 + i, 8, stride=32),
            )
        return carry

    lax.fori_loop(0, 4, back_pack, 0)
    each_peer(
        img,
        cell,
        lambda pi, pc: send_message(msg_back, inbox_back, sems.at[8], sems.at[9], pi, pc),
    )
    inbox_back[own, :] = msg_back[own, :]

    acc[...] = jnp.zeros_like(acc)
    wait_rows(inbox_back, (DEVICES - 1) * PAIRS, sems.at[9])

    def owner_unpack(c, carry):
        values = unpack_message(
            inbox_back,
            lambda i: pl.ds(c * 64 + i, 8, stride=8),
            lambda i: pl.ds(512 + c * 64 + i, 8, stride=8),
        )
        for f in range(FEATS):
            table[pl.ds(pl.multiple_of(f * ROWS + c * 8, 8), 8), :] = values[f]
        return carry

    lax.fori_loop(0, 8, owner_unpack, 0)

    def owner_step(k, carry):
        at = [k * 2 * BLOCKS + 2 * n for n in range(BLOCKS)]
        scatter_blocks(
            [row_pair(ids_own, a) for a in at],
            [[row_pair(table, f * ROWS + a) for f in range(FEATS)] for a in at],
            hot_own[:, pl.ds(pl.multiple_of(k * 256 * BLOCKS, 256), 256 * BLOCKS)],
            acc,
        )
        return carry

    lax.fori_loop(0, ROWS // (2 * BLOCKS), owner_step, 0)

    def finish(h, carry):
        for f in range(FEATS):
            v = total_rows(f, h)
            for half in range(2):
                out[pl.ds(f * ROWS + h * 16 + half, 8, stride=2), :] = v[
                    :, 128 * half : 128 * half + 128
                ]
        return carry

    lax.fori_loop(0, 4, finish, 0)

    wait_rows(ids_in, DEVICES - 1, sems.at[0])
    wait_rows(ext_target, BORDER_ROWS, sems.at[2])
    wait_rows(msg, (DEVICES - 1) * PAIRS, sems.at[4])
    wait_rows(ext_render, BORDER_ROWS, sems.at[6])
    wait_rows(msg_back, (DEVICES - 1) * PAIRS, sems.at[8])


def pullback_kernel(cam_ref, attr_hbm, feat_grad, out_hbm, attr, arows, result, load_sems, save_sem):
    cam = read_camera(cam_ref)

    def block(h):
        return pl.ds(pl.multiple_of(h * 1024, 1024), 1024)

    def load(h):
        return pltpu.make_async_copy(
            attr_hbm.at[:, block(h)], attr.at[:, block(h)], load_sems.at[h]
        )

    for h in range(8):
        load(h).start()

    def step(h, carry):
        load(h).wait()
        for k in range(8):
            lanes = pl.ds(pl.multiple_of(h * 1024 + k * 128, 128), 128)
            for g in range(8):
                n = min(8, ATTRS - 8 * g)
                arows[g * 64 + 8 * k : g * 64 + 8 * k + n, :] = attr[8 * g : 8 * g + n, lanes]
        places = [pl.ds((r // 8) * 64 + r % 8, 8, stride=8) for r in range(ATTRS)]
        rows = [arows[at, :] for at in places]
        _, pullback = jax.vjp(lambda r: project(r, cam), rows)
        grads = [
            feat_grad[pl.ds(pl.multiple_of(f * ROWS + h * 8, 8), 8), :] for f in range(FEATS)
        ]
        log_opacity = grads.pop(5)
        (found,) = pullback(grads)
        found[10] = log_opacity * (1.0 - jax.nn.sigmoid(rows[10]))
        for at, v in zip(places, found):
            arows[at, :] = v
        for k in range(8):
            lanes = pl.ds(pl.multiple_of(h * 1024 + k * 128, 128), 128)
            for g in range(8):
                n = min(8, ATTRS - 8 * g)
                result[8 * g : 8 * g + n, lanes] = arows[g * 64 + 8 * k : g * 64 + 8 * k + n, :]
        pltpu.make_async_copy(result.at[:, block(h)], out_hbm.at[:, block(h)], save_sem).start()
        return carry

    lax.fori_loop(0, 8, step, 0)
    pltpu.make_async_copy(result, out_hbm, save_sem).wait()


def shards(attributes, camera, target, visible_index, tile_lists, tile_len):
    vmem = pl.BlockSpec(memory_space=pltpu.VMEM)
    smem = pl.BlockSpec(memory_space=pltpu.SMEM)
    feat_grad = pl.pallas_call(
        step_kernel,
        out_shape=jax.ShapeDtypeStruct((FEATS * ROWS, 128), F32),
        in_specs=[smem, smem, vmem, pl.BlockSpec(memory_space=pl.ANY), vmem, vmem],
        out_specs=vmem,
        scratch_shapes=[
            pltpu.VMEM((ATTRS, 8192), F32),
            pltpu.VMEM((4096, 128), F32),
            pltpu.VMEM((FEATS * ROWS, 128), F32),
            pltpu.VMEM((FEATS * 32, 512), BF16),
            pltpu.VMEM((EXACT * 32, 256), BF16),
            pltpu.VMEM((256, TILES * LIST), BF16),
            pltpu.VMEM((256, ROWS * 128), BF16),
            pltpu.VMEM((DEVICES, 128), I32),
            pltpu.VMEM((ROWS, 128), I32),
            pltpu.VMEM((DEVICES * 8, 128), F32),
            pltpu.VMEM((DEVICES * 8, 128), F32),
            pltpu.VMEM((DEVICES * 8, 128), F32),
            pltpu.VMEM((DEVICES * 8, 128), F32),
            pltpu.VMEM((EXT_ROWS, 128), F32),
            pltpu.VMEM((EXT_ROWS, 128), F32),
            pltpu.VMEM((FEATS * TILES, 128), F32),
            pltpu.VMEM((256, 128), BF16),
            pltpu.VMEM((256, 128), BF16),
            pltpu.VMEM((TILES * 256, 256), BF16),
            pltpu.VMEM((TILES * 256, 128), F32),
            pltpu.VMEM((96, 256), F32),
            pltpu.VMEM((FEATS * TILES, 128), F32),
            pltpu.VMEM((5 * 3 * 3 * 64, 128), F32),
            pltpu.VMEM((3 * 3 * 3 * 48, 128), F32),
            pltpu.VMEM((2 * 3 * 48, 384), F32),
            pltpu.VMEM((2 * FEATS * 32, 256), F32),
            pltpu.SemaphoreType.DMA((11,)),
        ],
        compiler_params=pltpu.CompilerParams(
            collective_id=0, has_side_effects=True, vmem_limit_bytes=56 * 1024 * 1024
        ),
        name="splat_step",
    )(
        camera,
        tile_len,
        visible_index.reshape(ROWS, 128),
        attributes,
        target,
        tile_lists.reshape(TILES, LIST),
    )
    return pl.pallas_call(
        pullback_kernel,
        out_shape=jax.ShapeDtypeStruct(attributes.shape, F32),
        in_specs=[smem, pl.BlockSpec(memory_space=pl.ANY), vmem],
        out_specs=pl.BlockSpec(memory_space=pl.ANY),
        scratch_shapes=[
            pltpu.VMEM((ATTRS, 8192), F32),
            pltpu.VMEM((512, 128), F32),
            pltpu.VMEM((ATTRS, 8192), F32),
            pltpu.SemaphoreType.DMA((8,)),
            pltpu.SemaphoreType.DMA,
        ],
        name="splat_pullback",
    )(camera, attributes, feat_grad)


def solution(mesh):
    return jax.shard_map(
        shards,
        mesh=mesh,
        in_specs=(
            P(None, ("img", "cell")),
            P(),
            P(None, "img", "cell"),
            P(("img", "cell"), None),
            P("img", "cell", None),
            P("img", "cell"),
        ),
        out_specs=P(None, ("img", "cell")),
        check_vma=False,
    )
```

```python
import math

import jax
import jax.numpy as jnp
from jax import lax
from jax.experimental import pallas as pl
from jax.experimental.pallas import tpu as pltpu
from jax.sharding import PartitionSpec as P

F32 = jnp.float32
BF16 = jnp.bfloat16
I32 = jnp.int32
MESH = pl.DeviceIdType.MESH

TILE = 16
N_IMG = 8
N_CELL = 16
DEVICES = 128
LIST = 128
TILES = 32
ATTRS = 59
ROWS = 64
FEATS = 9
PAIRS = 5
EXACT = 5
BLOCKS = 8
GROUP = 4

WEIGHT_SSIM = 0.2
SMOOTHING = 0.01
STAB_ONE = 0.0001
STAB_TWO = 0.0009
BLUR_SIGMA = 1.5
SH_ZERO = 0.28209479177387814
SH_ONE = 0.4886025119029199
SH_TWO = (
    1.0925484305920792,
    -1.0925484305920792,
    0.31539156525252005,
    -1.0925484305920792,
    0.5462742152960396,
)
SH_THREE = (
    -0.5900435899266435,
    2.890611442640554,
    -0.4570457994644658,
    0.3731763325901154,
    -0.4570457994644658,
    1.445305721320277,
    -0.5900435899266435,
)


def blur_taps():
    raw = [math.exp(-((o - 5.0) ** 2) / (2.0 * BLUR_SIGMA * BLUR_SIGMA)) for o in range(11)]
    return [r / sum(raw) for r in raw]


TAPS = blur_taps()


def harmonic_basis(ux, uy, uz):
    xx, yy, zz = ux * ux, uy * uy, uz * uz
    return [
        SH_ZERO,
        -SH_ONE * uy,
        SH_ONE * uz,
        -SH_ONE * ux,
        SH_TWO[0] * ux * uy,
        SH_TWO[1] * uy * uz,
        SH_TWO[2] * (2.0 * zz - xx - yy),
        SH_TWO[3] * ux * uz,
        SH_TWO[4] * (xx - yy),
        SH_THREE[0] * uy * (3.0 * xx - yy),
        SH_THREE[1] * ux * uy * uz,
        SH_THREE[2] * uy * (4.0 * zz - xx - yy),
        SH_THREE[3] * uz * (2.0 * zz - 3.0 * xx - 3.0 * yy),
        SH_THREE[4] * ux * (4.0 * zz - xx - yy),
        SH_THREE[5] * uz * (xx - yy),
        SH_THREE[6] * ux * (xx - 3.0 * yy),
    ]


def project(rows, cam):
    pos = rows[0:3]
    scales = [jnp.exp(r) for r in rows[3:6]]
    qw = 1.5 + jnp.tanh(rows[6])
    qx, qy, qz = rows[7:10]
    inv = 1.0 / jnp.sqrt(qw * qw + qx * qx + qy * qy + qz * qz)
    qw, qx, qy, qz = qw * inv, qx * inv, qy * inv, qz * inv
    rot = [
        [1.0 - 2.0 * (qy * qy + qz * qz), 2.0 * (qx * qy - qw * qz), 2.0 * (qx * qz + qw * qy)],
        [2.0 * (qx * qy + qw * qz), 1.0 - 2.0 * (qx * qx + qz * qz), 2.0 * (qy * qz - qw * qx)],
        [2.0 * (qx * qz - qw * qy), 2.0 * (qy * qz + qw * qx), 1.0 - 2.0 * (qx * qx + qy * qy)],
    ]
    axes = [
        [
            (cam[s][0] * rot[0][k] + cam[s][1] * rot[1][k] + cam[s][2] * rot[2][k]) * scales[k]
            for k in range(3)
        ]
        for s in range(2)
    ]
    cov_a = axes[0][0] * axes[0][0] + axes[0][1] * axes[0][1] + axes[0][2] * axes[0][2] + 0.3
    cov_b = axes[0][0] * axes[1][0] + axes[0][1] * axes[1][1] + axes[0][2] * axes[1][2]
    cov_c = axes[1][0] * axes[1][0] + axes[1][1] * axes[1][1] + axes[1][2] * axes[1][2] + 0.3
    inv_det = 1.0 / (cov_a * cov_c - cov_b * cov_b)
    centers = [
        8.0
        + 7.0 * jnp.sin((cam[s][0] * pos[0] + cam[s][1] * pos[1] + cam[s][2] * pos[2]) / 3.0)
        for s in range(2)
    ]
    off = [pos[k] - cam[2][k] for k in range(3)]
    inv_dist = 1.0 / jnp.sqrt(off[0] * off[0] + off[1] * off[1] + off[2] * off[2])
    basis = harmonic_basis(off[0] * inv_dist, off[1] * inv_dist, off[2] * inv_dist)
    colours = []
    for c in range(3):
        total = 0.5 + basis[0] * rows[11 + 16 * c]
        for m in range(1, 16):
            total = total + basis[m] * rows[11 + 16 * c + m]
        colours.append(total)
    return centers + [cov_c * inv_det, -cov_b * inv_det, cov_a * inv_det] + colours


def read_camera(cam):
    return [[cam[s, k] for k in range(3)] for s in range(3)]


def spread_rows(attr, arows):
    def step(ct, carry):
        lanes = pl.ds(pl.multiple_of(ct * 128, 128), 128)
        for g in range(8):
            n = min(8, ATTRS - 8 * g)
            arows[pl.ds(pl.multiple_of(g * 512 + ct * 8, 8), n), :] = attr[8 * g : 8 * g + n, lanes]
        return carry

    lax.fori_loop(0, 64, step, 0)


def attr_rows(h):
    return [pl.ds((r // 8) * 512 + h * 64 + r % 8, 8, stride=8) for r in range(ATTRS)]


def wrap(value, count):
    return jnp.where(value >= count, value - count, value)


def ring_distance(d):
    return min(d, 4 - d)


STEPS = sorted(
    ((dy, dz) for dy in range(4) for dz in range(4)),
    key=lambda s: ring_distance(s[0]) + ring_distance(s[1]),
)


def pick(index, values):
    found = values[0]
    for n in range(1, len(values)):
        found = jnp.where(index == n, values[n], found)
    return found


class Place:
    def __init__(self, img, cell):
        self.y, self.z = lax.div(img, 2), lax.div(cell, 4)
        core, x = img - self.y * 2, cell - self.z * 4
        self.cores = [core, 1 - core]
        self.xs = [wrap(x + dx, 4) if dx else x for dx in range(4)]
        self.x_halves = [lax.div(v, 2) for v in self.xs]

    def devices(self, dy, dz):
        row, column = wrap(self.y + dy, 4) * 2, wrap(self.z + dz, 4)
        found = []
        for q in range(8):
            pi = row + self.cores[q % 2]
            found.append((pi, column * 4 + self.xs[q // 2], pi * 8 + column * 2 + self.x_halves[q // 2]))
        return found


def opposite(q):
    return (4 - q // 2) % 4 * 2 + q % 2


def each_step(place, act):
    for dy, dz in reversed(STEPS):
        seen = STEPS.index(((4 - dy) % 4, (4 - dz) % 4))
        for q, (pi, pc, half) in enumerate(place.devices(dy, dz)):
            if (dy, dz, q) != (0, 0, 0):
                act(pi, pc, half, seen * 8 + opposite(q), seen // 2)


def left_half():
    return lax.broadcasted_iota(I32, (8, 128), 1) < 64


def pack_message(values, msg, low_row, high_row):
    left = left_half()
    for i in range(PAIRS):
        a = values[2 * i]
        b = values[2 * i + 1] if 2 * i + 1 < FEATS else a
        msg[low_row(i), :] = jnp.where(left, a, pltpu.roll(b, 64, 1))
        msg[high_row(i), :] = jnp.where(left, pltpu.roll(a, 64, 1), b)


def unpack_message(msg, low_row, high_row):
    left = left_half()
    values = []
    for i in range(PAIRS):
        low, high = msg[low_row(i), :], msg[high_row(i), :]
        values.append(jnp.where(left, low, pltpu.roll(high, 64, 1)))
        if 2 * i + 1 < FEATS:
            values.append(jnp.where(left, pltpu.roll(low, 64, 1), high))
    return values


def one_hot(low):
    return jnp.where(lax.broadcasted_iota(I32, (256, 256), 0) == low, 1.0, 0.0).astype(BF16)


def split_ids(ids):
    high = lax.shift_right_logical(ids, 8)
    return high, ids - lax.shift_left(high, 8)


def row_pair(ref, at):
    both = ref[pl.ds(at, 2), :]
    return jnp.concatenate([both[0:1], both[1:2]], axis=1)


def make_parts(table, parts, thirds):
    for f in range(FEATS):
        rows = slice(32 * f, 32 * f + 32)
        for half in range(2):
            v = table[pl.ds(f * ROWS + half, 32, stride=2), :]
            top = v.astype(BF16)
            v = v - top.astype(F32)
            middle = v.astype(BF16)
            parts[rows, 128 * half : 128 * half + 128] = top
            parts[rows, 256 + 128 * half : 384 + 128 * half] = middle
            if f < EXACT:
                low = (v - middle.astype(F32)).astype(BF16)
                thirds[rows, 128 * half : 128 * half + 128] = low


def gather_blocks(parts, thirds, ids, hots):
    found, fine = [], []
    for hot in hots:
        found.append(
            jnp.dot(
                parts[...], jnp.concatenate([hot] * 2, axis=0), preferred_element_type=F32
            )
        )
        fine.append(jnp.dot(thirds[...], hot, preferred_element_type=F32))
    out = []
    for v, low, block in zip(found, fine, ids):
        mask = lax.broadcasted_iota(I32, (32, 256), 0) == split_ids(block)[0]
        rows = []
        for f in range(FEATS):
            value = v[32 * f : 32 * f + 32]
            if f < EXACT:
                value = value + low[32 * f : 32 * f + 32]
            rows.append(jnp.sum(jnp.where(mask, value, 0.0), axis=0, keepdims=True))
        out.append(rows)
    return out


def scatter_blocks(ids, grads, hots, acc):
    lhs = []
    for block, rows in zip(ids, grads):
        mask = lax.broadcasted_iota(I32, (32, 256), 0) == split_ids(block)[0]
        upper, lower = [], []
        for g in rows:
            top = g.astype(BF16).astype(F32)
            upper.append(jnp.where(mask, top, 0.0).astype(BF16))
            lower.append(jnp.where(mask, g - top, 0.0).astype(BF16))
        lhs.append(jnp.concatenate(upper + lower, axis=0))
    acc[...] += lax.dot_general(
        jnp.concatenate(lhs, axis=1),
        hots,
        (((1,), (1,)), ((), ())),
        preferred_element_type=F32,
    )


def two_parts(v):
    top = v.astype(BF16)
    return top, (v - top.astype(F32)).astype(BF16)


def swap_blocks(z):
    rows = z.shape[0]
    row_at = lax.broadcasted_iota(I32, z.shape, 0)
    lane_at = lax.broadcasted_iota(I32, z.shape, 1)
    for bit in (1, 2, 4, 8):
        row_bit = (row_at // bit) % 2
        lane_bit = (lane_at // (16 * bit)) % 2
        down = pltpu.roll(pltpu.roll(z, rows - bit, 0), 16 * bit, 1)
        up = pltpu.roll(pltpu.roll(z, bit, 0), 256 - 16 * bit, 1)
        z = jnp.where(row_bit == lane_bit, z, jnp.where(row_bit == 0, down, up))
    return z


NORTH, SOUTH, PACK_WEST, PACK_EAST, FROM_WEST, FROM_EAST = 192, 288, 384, 400, 416, 432
FROM_NW, FROM_NE, FROM_SW, FROM_SE, EXT_ROWS = 448, 456, 464, 472, 480
BORDER_ROWS = 256


def pack_columns(ext):
    lane = lax.broadcasted_iota(I32, (8, 128), 1)
    for t in range(2):
        west = jnp.zeros((8, 128), F32)
        east = west
        for k in range(6):
            here = (lane >= 16 * k) & (lane < 16 * k + 16)
            at = t * 48 + 8 * k
            first, last = ext[at : at + 8, :], ext[96 + at : 104 + at, :]
            west = jnp.where(here, pltpu.roll(first, 16 * k, 1) if k else first, west)
            east = jnp.where(here, pltpu.roll(last, 16 * k + 16, 1), east)
        ext[PACK_WEST + 8 * t : PACK_WEST + 8 * t + 8, :] = west
        ext[PACK_EAST + 8 * t : PACK_EAST + 8 * t + 8, :] = east


def border_copies(ext, img, cell, send, recv):
    west, east = jnp.where(cell == 0, N_CELL - 1, cell - 1), wrap(cell + 1, N_CELL)
    north, south = jnp.where(img == 0, N_IMG - 1, img - 1), wrap(img + 1, N_IMG)
    plan = [
        (PACK_WEST, FROM_SE, 8, north, west),
        (PACK_EAST, FROM_SW, 8, north, east),
        (PACK_WEST + 8, FROM_NE, 8, south, west),
        (PACK_EAST + 8, FROM_NW, 8, south, east),
        (PACK_WEST, FROM_EAST, 16, img, west),
        (PACK_EAST, FROM_WEST, 16, img, east),
    ]
    for k in range(2):
        plan.append((96 * k, SOUTH + 48 * k, 48, north, cell))
        plan.append((96 * k + 48, NORTH + 48 * k, 48, south, cell))
    for source, dest, count, to_img, to_cell in plan:
        pltpu.make_async_remote_copy(
            src_ref=ext.at[pl.ds(source, count)],
            dst_ref=ext.at[pl.ds(dest, count)],
            send_sem=send,
            recv_sem=recv,
            device_id=(to_img, to_cell),
            device_id_type=MESH,
        ).start()


def wait_rows(ref, count, sem):
    part = ref.at[pl.ds(0, count)]
    pltpu.make_async_copy(part, part, sem).wait()


def window(ext, img, cell, c, row_block, half):
    lane = lax.broadcasted_iota(I32, (8, 128), 1)
    at = 16 * c + 8 * half
    bases = [NORTH, 0, 48, SOUTH][row_block]
    step = 48 if row_block in (0, 3) else 96
    sides = [
        (FROM_NW, FROM_NE),
        (FROM_WEST, FROM_EAST),
        (FROM_WEST + 8, FROM_EAST + 8),
        (FROM_SW, FROM_SE),
    ][row_block]
    first = pltpu.roll(ext[bases + at : bases + at + 8, :], 64, 1)
    second = pltpu.roll(ext[bases + step + at : bases + step + at + 8, :], 64, 1)
    block = 16 * (2 * c + half)
    left = pltpu.roll(ext[sides[0] : sides[0] + 8, :], (48 - block) % 128, 1)
    right = pltpu.roll(ext[sides[1] : sides[1] + 8, :], (64 - block) % 128, 1)
    keep_left = jnp.where(cell == 0, 64, 48)
    keep_right = jnp.where(cell == N_CELL - 1, 64, 80)
    tiles = [
        jnp.where(lane < 64, jnp.where(lane >= keep_left, left, 0.0), first),
        jnp.where(lane < 64, first, second),
        jnp.where(lane < 64, second, jnp.where(lane < keep_right, right, 0.0)),
    ]
    if row_block == 0:
        tiles = [v * jnp.where(img == 0, 0.0, 1.0) for v in tiles]
    if row_block == 3:
        tiles = [v * jnp.where(img == N_IMG - 1, 0.0, 1.0) for v in tiles]
    return tiles


def blur(ref, start, stride):
    down = []
    for j in range(3):
        at = start + j * stride
        total = TAPS[5] * ref[pl.ds(at + 5, 8), :]
        for o in range(5):
            total = total + TAPS[o] * (ref[pl.ds(at + o, 8), :] + ref[pl.ds(at + 10 - o, 8), :])
        down.append(total)
    v = jnp.concatenate(down, axis=1)
    total = TAPS[5] * v
    for o in range(5):
        d = 5 - o
        total = total + TAPS[o] * (pltpu.roll(v, d, 1) + pltpu.roll(v, 384 - d, 1))
    return total


def ssim_value(mean_render, mean_target, square_render, square_target, cross_term):
    spread_render = square_render - mean_render * mean_render
    spread_target = square_target - mean_target * mean_target
    covariance = cross_term - mean_render * mean_target
    upper = (2.0 * mean_render * mean_target + STAB_ONE) * (2.0 * covariance + STAB_TWO)
    lower = (mean_render * mean_render + mean_target * mean_target + STAB_ONE) * (
        spread_render + spread_target + STAB_TWO
    )
    return upper / lower


def map_row(m, c):
    return (m * 3 + c) * 3 * 64


def step_kernel(
    cam_ref,
    len_ref,
    vis,
    attr_hbm,
    target,
    lists,
    out,
    attr,
    arows,
    table,
    parts,
    thirds,
    hot_list,
    hot_own,
    ids_in,
    ids_own,
    msg,
    inbox,
    msg_back,
    inbox_back,
    ext_render,
    ext_target,
    entry,
    tri_before,
    tri_after,
    weights,
    ratio,
    tile_rows,
    moments,
    maps,
    coefs,
    blurred,
    acc,
    sems,
    id_sems,
    back_sems,
):
    img = lax.axis_index("img")
    cell = lax.axis_index("cell")
    me = img * N_CELL + cell

    barrier = pltpu.get_barrier_semaphore()
    place = Place(img, cell)
    each_step(
        place,
        lambda pi, pc, *_: pl.semaphore_signal(
            barrier, 1, device_id=(pi, pc), device_id_type=MESH
        ),
    )
    load_attr = pltpu.make_async_copy(attr_hbm, attr, sems.at[10])
    load_attr.start()

    for k in range(2):
        for t in range(2):
            for c in range(3):
                at = 96 * k + 48 * t + 16 * c
                ext_target[at : at + 16, :] = target[
                    c, 16 * t : 16 * t + 16, 128 * k : 128 * k + 128
                ]
    pack_columns(ext_target)

    def list_hot(b, carry):
        hot_list[:, pl.ds(pl.multiple_of(b * 256, 256), 256)] = one_hot(
            split_ids(row_pair(lists, b * 2))[1]
        )
        return carry

    lax.fori_loop(0, TILES // 2, list_hot, 0)

    cam = read_camera(cam_ref)
    load_attr.wait()
    spread_rows(attr, arows)

    def project_step(h, carry):
        rows = [arows[at, :] for at in attr_rows(h)]
        feats = project(rows, cam)
        feats.insert(5, jax.nn.sigmoid(rows[10]))
        for f in range(FEATS):
            table[pl.ds(pl.multiple_of(f * ROWS + h * 8, 8), 8), :] = feats[f]
        return carry

    lax.fori_loop(0, 8, project_step, 0)
    make_parts(table, parts, thirds)

    row_at = lax.broadcasted_iota(I32, (128, 128), 0)
    lane_at = lax.broadcasted_iota(I32, (128, 128), 1)
    before = jnp.where(row_at < lane_at, 1.0, 0.0).astype(BF16)
    after = jnp.where(row_at > lane_at, 1.0, 0.0).astype(BF16)
    for half in range(2):
        tri_before[128 * half : 128 * half + 128, :] = before
        tri_after[128 * half : 128 * half + 128, :] = after

    pl.semaphore_wait(barrier, DEVICES - 1)

    def send_ids(pi, pc, half, rank, group):
        pltpu.make_async_remote_copy(
            src_ref=vis.at[pl.ds(half, 1)],
            dst_ref=ids_in.at[pl.ds(rank, 1)],
            send_sem=sems.at[0],
            recv_sem=id_sems.at[group],
            device_id=(pi, pc),
            device_id_type=MESH,
        ).start()

    each_step(place, send_ids)
    pltpu.make_async_copy(
        vis.at[pl.ds(me // 2, 1)], ids_in.at[pl.ds(0, 1)], id_sems.at[0]
    ).start()
    border_copies(ext_target, img, cell, sems.at[2], sems.at[3])

    wait_rows(ext_target, BORDER_ROWS, sems.at[3])
    for c in range(3):
        for row_block in range(4):
            for half in range(2):
                strips = window(ext_target, img, cell, c, row_block, half)
                for j in range(3):
                    for m, v in ((3, strips[j]), (4, strips[j] * strips[j])):
                        at = map_row(m, c) + 64 * j + 16 * row_block + 8 * half
                        maps[at : at + 8, :] = v

    def target_blur(c, carry):
        for m in range(2):
            for r in range(6):
                at = pl.multiple_of((m * 3 + c) * 48 + 8 * r, 8)
                blurred[pl.ds(at, 8), :] = blur(maps, map_row(3 + m, c) + 6 + 8 * r, 64)
        return carry

    lax.fori_loop(0, 3, target_blur, 0)

    odd = me - (me // 2) * 2
    left = left_half()
    left_row = lax.broadcasted_iota(I32, (1, 128), 1) < 64

    def reply_step(g, carry):
        wait_rows(ids_in, 16, id_sems.at[g])
        at = pl.multiple_of(g * 16, 8)
        first, second = ids_in[pl.ds(at, 8), :], ids_in[pl.ds(at + 8, 8), :]
        even_form = jnp.where(left, first, pltpu.roll(second, 64, 1))
        odd_form = jnp.where(left, pltpu.roll(first, 64, 1), second)
        both = jnp.where(odd == 0, even_form, odd_form)
        ids_own[pl.ds(pl.multiple_of(g * 8, 8), 8), :] = both
        ids = [
            jnp.concatenate([both[2 * n : 2 * n + 1], both[2 * n + 1 : 2 * n + 2]], axis=1)
            for n in range(4)
        ]
        hots = [one_hot(split_ids(v)[1]) for v in ids]
        for n in range(4):
            hot_own[:, pl.ds(pl.multiple_of(g * 1024 + n * 256, 256), 256)] = hots[n]
        got = gather_blocks(parts, thirds, ids, hots)
        for n in range(4):
            for row in range(2):
                d = g * 128 + (2 * n + row) * 8
                for i in range(PAIRS):
                    low = got[n][2 * i][:, 128 * row : 128 * row + 128]
                    high = got[n][min(2 * i + 1, FEATS - 1)][:, 128 * row : 128 * row + 128]
                    msg[pl.ds(d + i, 1), :] = jnp.where(left_row, low, pltpu.roll(high, 64, 1))
                    msg[pl.ds(d + 64 + i, 1), :] = jnp.where(
                        left_row, pltpu.roll(low, 64, 1), high
                    )
        for side in range(2):
            dy = pick(g, [STEPS[2 * n + side][0] for n in range(8)])
            dz = pick(g, [STEPS[2 * n + side][1] for n in range(8)])

            for q, (pi, pc, _) in enumerate(place.devices(dy, dz)):
                copy = pltpu.make_async_remote_copy(
                    src_ref=msg.at[pl.ds(pl.multiple_of(g * 128 + side * 64 + q * 8, 8), PAIRS)],
                    dst_ref=inbox.at[pl.ds(pl.multiple_of(me * 8, 8), PAIRS)],
                    send_sem=sems.at[4],
                    recv_sem=sems.at[5],
                    device_id=(pi, pc),
                    device_id_type=MESH,
                )
                if side == 0 and q == 0:
                    pl.when(g > 0)(copy.start)
                else:
                    copy.start()
        return carry

    lax.fori_loop(0, 8, reply_step, 0)
    own = pl.ds(pl.multiple_of(me * 8, 8), PAIRS)
    inbox[own, :] = msg[0:PAIRS, :]

    wait_rows(inbox, (DEVICES - 1) * PAIRS, sems.at[5])

    def table_step(h, carry):
        values = unpack_message(
            inbox,
            lambda i: pl.ds(h * 128 + i, 8, stride=16),
            lambda i: pl.ds(h * 128 + 8 + i, 8, stride=16),
        )
        for f in range(FEATS):
            table[pl.ds(pl.multiple_of(f * ROWS + h * 8, 8), 8), :] = values[f]
        return carry

    lax.fori_loop(0, 8, table_step, 0)
    make_parts(table, parts, thirds)

    def list_step(k, carry):
        got = gather_blocks(
            parts,
            thirds,
            [row_pair(lists, k * 8 + 2 * n) for n in range(4)],
            [
                hot_list[:, pl.ds(pl.multiple_of(k * 1024 + n * 256, 256), 256)]
                for n in range(4)
            ],
        )
        for n in range(4):
            for row in range(2):
                for f in range(FEATS):
                    entry[pl.ds(f * TILES + k * 8 + 2 * n + row, 1), :] = got[n][f][
                        :, 128 * row : 128 * row + 128
                    ]
        return carry

    lax.fori_loop(0, 4, list_step, 0)

    def entry_row(f, t):
        return entry[pl.ds(f * TILES + t, 1), :]

    across = lax.broadcasted_iota(I32, (16, 128), 0).astype(F32) + 0.5
    lane_row = lax.broadcasted_iota(I32, (1, 128), 1)

    def spans(tile_row, k):
        return [tile_row * 16 + k * GROUP + n for n in range(GROUP)]

    def pixels_of(t):
        return pl.ds(pl.multiple_of(t * 256, 256), 256)

    for tile_row in range(2):

        def render_step(k, carry, tile_row=tile_row):
            tiles = spans(tile_row, k)
            alphas, sums = [], []
            for n, t in enumerate(tiles):
                alive = lane_row < len_ref[tile_row, k * GROUP + n]
                opacity = jnp.where(alive, entry_row(5, t), 0.0)
                dx = across - entry_row(0, t)
                center_y = entry_row(1, t)
                square_x = (-0.5 * entry_row(2, t)) * dx * dx
                mixed = -entry_row(3, t) * dx
                half_y = -0.5 * entry_row(4, t)
                alpha = []
                for y in range(16):
                    dy = (y + 0.5) - center_y
                    alpha.append(opacity * jnp.exp(square_x + dy * (mixed + half_y * dy)))
                alpha = jnp.concatenate(alpha, axis=0)
                logs = jnp.log(1.0 - alpha)
                sums.append(
                    jnp.dot(
                        jnp.concatenate(two_parts(logs), axis=1),
                        tri_before[...],
                        preferred_element_type=F32,
                    )
                )
                ratio[pixels_of(t), :] = alpha * jnp.exp(-logs)
                alphas.append(alpha)
            products = []
            for n, t in enumerate(tiles):
                weight = jnp.concatenate(two_parts(jnp.exp(sums[n]) * alphas[n]), axis=1)
                weights[pixels_of(t), :] = weight
                colour = [two_parts(entry_row(6 + c, t)) for c in range(3)]
                lhs = jnp.concatenate(
                    [c[part] for part in range(2) for c in colour] + [jnp.zeros((10, 128), BF16)],
                    axis=0,
                )
                products.append(
                    lax.dot_general(
                        jnp.concatenate([lhs, lhs], axis=1),
                        weight,
                        (((1,), (1,)), ((), ())),
                        preferred_element_type=F32,
                    )
                )
            for n in range(GROUP):
                for c in range(3):
                    tile_rows[pl.ds(tile_row * 48 + c * 16 + k * GROUP + n, 1), :] = (
                        products[n][c : c + 1] + products[n][3 + c : 4 + c]
                    )
            return carry

        lax.fori_loop(0, 16 // GROUP, render_step, 0)

    picture = swap_blocks(tile_rows[...])
    for k in range(2):
        ext_render[96 * k : 96 * k + 96, :] = picture[:, 128 * k : 128 * k + 128]
    pack_columns(ext_render)
    border_copies(ext_render, img, cell, sems.at[6], sems.at[7])
    wait_rows(ext_render, BORDER_ROWS, sems.at[7])

    for c in range(3):
        for row_block in range(4):
            for half in range(2):
                strips = window(ext_render, img, cell, c, row_block, half)
                for j in range(3):
                    at = 64 * j + 16 * row_block + 8 * half
                    v = strips[j]
                    wanted = maps[map_row(3, c) + at : map_row(3, c) + at + 8, :]
                    for m, value in ((0, v), (1, v * v), (2, v * wanted)):
                        maps[map_row(m, c) + at : map_row(m, c) + at + 8, :] = value
    row_at = lax.broadcasted_iota(I32, (8, 384), 0) + (img * 32 - 5)
    lane_at = lax.broadcasted_iota(I32, (8, 384), 1) + (cell * 256 - 64)
    inside = (lane_at >= 0) & (lane_at < N_CELL * 256)

    def similarity_step(c, carry):
        for r in range(6):
            mean, square, cross = [blur(maps, map_row(m, c) + 6 + 8 * r, 64) for m in range(3)]
            mean_target, square_target = [
                blurred[pl.ds(pl.multiple_of((m * 3 + c) * 48 + 8 * r, 8), 8), :]
                for m in range(2)
            ]
            _, pullback = jax.vjp(
                lambda x, y, z, mt=mean_target, st=square_target: ssim_value(x, mt, y, st, z),
                mean,
                square,
                cross,
            )
            keep = inside & (row_at + 8 * r >= 0) & (row_at + 8 * r < N_IMG * 32)
            for m, v in enumerate(pullback(jnp.full((8, 384), -WEIGHT_SSIM, F32))):
                v = jnp.where(keep, v, 0.0)
                for j in range(3):
                    at = pl.multiple_of(((m * 3 + c) * 3 + j) * 48 + 8 * r, 8)
                    coefs[pl.ds(at, 8), :] = v[:, 128 * j : 128 * j + 128]
        return carry

    lax.fori_loop(0, 3, similarity_step, 0)
    left = left_half()

    def image_step(c, carry):
        for r in range(4):
            back_mean, back_square, back_cross = [
                blur(coefs, (m * 3 + c) * 3 * 48 + 8 * r, 48) for m in range(3)
            ]
            found = []
            for j in range(3):
                lanes = slice(128 * j, 128 * j + 128)
                at = 64 * j + 16 + 8 * r
                image = maps[pl.ds(pl.multiple_of(map_row(0, c) + at, 8), 8), :]
                wanted = maps[pl.ds(pl.multiple_of(map_row(3, c) + at, 8), 8), :]
                difference = image - wanted
                slope = (
                    (1.0 - WEIGHT_SSIM)
                    * difference
                    / jnp.sqrt(difference * difference + SMOOTHING * SMOOTHING)
                )
                found.append(
                    pltpu.roll(
                        slope
                        + back_mean[:, lanes]
                        + 2.0 * image * back_square[:, lanes]
                        + wanted * back_cross[:, lanes],
                        64,
                        1,
                    )
                )
            at = pl.multiple_of((r // 2) * 48 + c * 16 + (r % 2) * 8, 8)
            tile_rows[pl.ds(at, 8), :] = jnp.concatenate(
                [jnp.where(left, found[0], found[1]), jnp.where(left, found[1], found[2])],
                axis=1,
            )
        return carry

    lax.fori_loop(0, 3, image_step, 0)
    tile_rows[...] = swap_blocks(tile_rows[...])

    for tile_row in range(2):

        def back_step(k, carry, tile_row=tile_row):
            tiles = spans(tile_row, k)
            grad_rows, values = [], []
            for n, t in enumerate(tiles):
                pixel_grad = [
                    two_parts(tile_rows[pl.ds(tile_row * 48 + c * 16 + k * GROUP + n, 1), :])
                    for c in range(3)
                ]
                colour = [two_parts(entry_row(6 + c, t)) for c in range(3)]
                tops, lows = [g[0] for g in pixel_grad], [g[1] for g in pixel_grad]
                grad_rows.append(
                    jnp.concatenate(tops + lows + tops + [jnp.zeros((7, 256), BF16)], axis=0)
                )
                colour_rows = jnp.concatenate(
                    [c[0] for c in colour] * 2
                    + [c[1] for c in colour]
                    + [jnp.zeros((7, 128), BF16)],
                    axis=0,
                )
                values.append(
                    lax.dot_general(
                        grad_rows[n],
                        colour_rows,
                        (((0,), (0,)), ((), ())),
                        preferred_element_type=F32,
                    )
                )
            gains, laters, mixes = [], [], []
            for n, t in enumerate(tiles):
                weight = weights[pixels_of(t), :]
                mixes.append(jnp.dot(grad_rows[n], weight, preferred_element_type=F32))
                gain = values[n] * (weight[:, :128].astype(F32) + weight[:, 128:].astype(F32))
                laters.append(
                    jnp.dot(
                        jnp.concatenate(two_parts(gain), axis=1),
                        tri_after[...],
                        preferred_element_type=F32,
                    )
                )
                gains.append(gain)
            for n, t in enumerate(tiles):
                pull = gains[n] - ratio[pixels_of(t), :] * laters[n]
                dx = across - entry_row(0, t)
                center_y = entry_row(1, t)
                sum_0 = sum_y = sum_yy = None
                for y in range(16):
                    dy = (y + 0.5) - center_y
                    part = pull[16 * y : 16 * y + 16]
                    part_y = part * dy
                    part_yy = part_y * dy
                    sum_0 = part if y == 0 else sum_0 + part
                    sum_y = part_y if y == 0 else sum_y + part_y
                    sum_yy = part_yy if y == 0 else sum_yy + part_yy
                sum_x = sum_0 * dx
                found = [sum_0, sum_x, sum_y, sum_x * dx, sum_y * dx, sum_yy]
                for m in range(6):
                    moments[pl.ds(m * TILES + t, 1), :] = jnp.sum(
                        found[m], axis=0, keepdims=True
                    )
                for c in range(3):
                    both = mixes[n][c : c + 1] + mixes[n][3 + c : 4 + c]
                    moments[pl.ds((6 + c) * TILES + t, 1), :] = both[:, :128] + both[:, 128:]
            return carry

        lax.fori_loop(0, 16 // GROUP, back_step, 0)

    feat = [entry[f * TILES : (f + 1) * TILES, :] for f in range(6)]
    mom = [moments[m * TILES : (m + 1) * TILES, :] for m in range(6)]
    entry[0:TILES, :] = feat[2] * mom[1] + feat[3] * mom[2]
    entry[TILES : 2 * TILES, :] = feat[3] * mom[1] + feat[4] * mom[2]
    entry[2 * TILES : 3 * TILES, :] = -0.5 * mom[3]
    entry[3 * TILES : 4 * TILES, :] = -mom[4]
    entry[4 * TILES : 5 * TILES, :] = -0.5 * mom[5]
    entry[5 * TILES : 6 * TILES, :] = mom[0]
    entry[6 * TILES : 9 * TILES, :] = moments[6 * TILES : 9 * TILES, :]

    acc[...] = jnp.zeros_like(acc)

    def slot_step(k, carry):
        at = [k * 2 * BLOCKS + 2 * n for n in range(BLOCKS)]
        scatter_blocks(
            [row_pair(lists, a) for a in at],
            [[row_pair(entry, f * TILES + a) for f in range(FEATS)] for a in at],
            hot_list[:, pl.ds(pl.multiple_of(k * 256 * BLOCKS, 256), 256 * BLOCKS)],
            acc,
        )
        return carry

    lax.fori_loop(0, TILES // (2 * BLOCKS), slot_step, 0)

    def total_rows(f, h):
        a = acc[pl.ds(pl.multiple_of(f * 32 + h * 8, 8), 8), :]
        b = acc[pl.ds(pl.multiple_of(288 + f * 32 + h * 8, 8), 8), :]
        return a + b

    def back_pack(h, carry):
        totals = [total_rows(f, h) for f in range(FEATS)]
        for half in range(2):
            pack_message(
                [v[:, 128 * half : 128 * half + 128] for v in totals],
                msg_back,
                lambda i: pl.ds(h * 256 + (2 * half) * 8 + i, 8, stride=32),
                lambda i: pl.ds(h * 256 + (2 * half + 1) * 8 + i, 8, stride=32),
            )
        return carry

    lax.fori_loop(0, 4, back_pack, 0)

    def send_back(pi, pc, half, rank, group):
        pltpu.make_async_remote_copy(
            src_ref=msg_back.at[pl.ds(pl.multiple_of((pi * N_CELL + pc) * 8, 8), PAIRS)],
            dst_ref=inbox_back.at[pl.ds(pl.multiple_of(rank * 8, 8), PAIRS)],
            send_sem=sems.at[8],
            recv_sem=back_sems.at[group],
            device_id=(pi, pc),
            device_id_type=MESH,
        ).start()

    each_step(place, send_back)
    pltpu.make_async_copy(
        msg_back.at[own], inbox_back.at[pl.ds(0, PAIRS)], back_sems.at[0]
    ).start()

    acc[...] = jnp.zeros_like(acc)

    def owner_step(k, carry):
        for side in range(BLOCKS // 4):
            g = k * (BLOCKS // 4) + side
            wait_rows(inbox_back, 16 * PAIRS, back_sems.at[g])
            values = unpack_message(
                inbox_back,
                lambda i: pl.ds(g * 128 + i, 8, stride=8),
                lambda i: pl.ds(g * 128 + 64 + i, 8, stride=8),
            )
            for f in range(FEATS):
                table[pl.ds(pl.multiple_of(f * ROWS + g * 8, 8), 8), :] = values[f]
        at = [k * 2 * BLOCKS + 2 * n for n in range(BLOCKS)]
        scatter_blocks(
            [row_pair(ids_own, a) for a in at],
            [[row_pair(table, f * ROWS + a) for f in range(FEATS)] for a in at],
            hot_own[:, pl.ds(pl.multiple_of(k * 256 * BLOCKS, 256), 256 * BLOCKS)],
            acc,
        )
        return carry

    lax.fori_loop(0, ROWS // (2 * BLOCKS), owner_step, 0)

    def finish(h, carry):
        for f in range(FEATS):
            v = total_rows(f, h)
            for half in range(2):
                out[pl.ds(f * ROWS + h * 16 + half, 8, stride=2), :] = v[
                    :, 128 * half : 128 * half + 128
                ]
        return carry

    lax.fori_loop(0, 4, finish, 0)

    wait_rows(ids_in, DEVICES - 1, sems.at[0])
    wait_rows(ext_target, BORDER_ROWS, sems.at[2])
    wait_rows(msg, (DEVICES - 1) * PAIRS, sems.at[4])
    wait_rows(ext_render, BORDER_ROWS, sems.at[6])
    wait_rows(msg_back, (DEVICES - 1) * PAIRS, sems.at[8])


def pullback_kernel(cam_ref, attr_hbm, feat_grad, out_hbm, attr, arows, result, load_sems, save_sem):
    cam = read_camera(cam_ref)

    def block(h):
        return pl.ds(pl.multiple_of(h * 1024, 1024), 1024)

    def load(h):
        return pltpu.make_async_copy(
            attr_hbm.at[:, block(h)], attr.at[:, block(h)], load_sems.at[h]
        )

    for h in range(8):
        load(h).start()

    def step(h, carry):
        load(h).wait()
        for k in range(8):
            lanes = pl.ds(pl.multiple_of(h * 1024 + k * 128, 128), 128)
            for g in range(8):
                n = min(8, ATTRS - 8 * g)
                arows[g * 64 + 8 * k : g * 64 + 8 * k + n, :] = attr[8 * g : 8 * g + n, lanes]
        places = [pl.ds((r // 8) * 64 + r % 8, 8, stride=8) for r in range(ATTRS)]
        rows = [arows[at, :] for at in places]
        _, pullback = jax.vjp(lambda r: project(r, cam), rows)
        grads = [
            feat_grad[pl.ds(pl.multiple_of(f * ROWS + h * 8, 8), 8), :] for f in range(FEATS)
        ]
        log_opacity = grads.pop(5)
        (found,) = pullback(grads)
        found[10] = log_opacity * (1.0 - jax.nn.sigmoid(rows[10]))
        for at, v in zip(places, found):
            arows[at, :] = v
        for k in range(8):
            lanes = pl.ds(pl.multiple_of(h * 1024 + k * 128, 128), 128)
            for g in range(8):
                n = min(8, ATTRS - 8 * g)
                result[8 * g : 8 * g + n, lanes] = arows[g * 64 + 8 * k : g * 64 + 8 * k + n, :]
        pltpu.make_async_copy(result.at[:, block(h)], out_hbm.at[:, block(h)], save_sem).start()
        return carry

    lax.fori_loop(0, 8, step, 0)
    pltpu.make_async_copy(result, out_hbm, save_sem).wait()


def shards(attributes, camera, target, visible_index, tile_lists, tile_len):
    vmem = pl.BlockSpec(memory_space=pltpu.VMEM)
    smem = pl.BlockSpec(memory_space=pltpu.SMEM)
    feat_grad = pl.pallas_call(
        step_kernel,
        out_shape=jax.ShapeDtypeStruct((FEATS * ROWS, 128), F32),
        in_specs=[smem, smem, vmem, pl.BlockSpec(memory_space=pl.ANY), vmem, vmem],
        out_specs=vmem,
        scratch_shapes=[
            pltpu.VMEM((ATTRS, 8192), F32),
            pltpu.VMEM((4096, 128), F32),
            pltpu.VMEM((FEATS * ROWS, 128), F32),
            pltpu.VMEM((FEATS * 32, 512), BF16),
            pltpu.VMEM((EXACT * 32, 256), BF16),
            pltpu.VMEM((256, TILES * LIST), BF16),
            pltpu.VMEM((256, ROWS * 128), BF16),
            pltpu.VMEM((DEVICES, 128), I32),
            pltpu.VMEM((ROWS, 128), I32),
            pltpu.VMEM((DEVICES * 8, 128), F32),
            pltpu.VMEM((DEVICES * 8, 128), F32),
            pltpu.VMEM((DEVICES * 8, 128), F32),
            pltpu.VMEM((DEVICES * 8, 128), F32),
            pltpu.VMEM((EXT_ROWS, 128), F32),
            pltpu.VMEM((EXT_ROWS, 128), F32),
            pltpu.VMEM((FEATS * TILES, 128), F32),
            pltpu.VMEM((256, 128), BF16),
            pltpu.VMEM((256, 128), BF16),
            pltpu.VMEM((TILES * 256, 256), BF16),
            pltpu.VMEM((TILES * 256, 128), F32),
            pltpu.VMEM((96, 256), F32),
            pltpu.VMEM((FEATS * TILES, 128), F32),
            pltpu.VMEM((5 * 3 * 3 * 64, 128), F32),
            pltpu.VMEM((3 * 3 * 3 * 48, 128), F32),
            pltpu.VMEM((2 * 3 * 48, 384), F32),
            pltpu.VMEM((2 * FEATS * 32, 256), F32),
            pltpu.SemaphoreType.DMA((11,)),
            pltpu.SemaphoreType.DMA((8,)),
            pltpu.SemaphoreType.DMA((8,)),
        ],
        compiler_params=pltpu.CompilerParams(
            collective_id=0, has_side_effects=True, vmem_limit_bytes=58 * 1024 * 1024
        ),
        name="splat_step",
    )(
        camera,
        tile_len,
        visible_index.reshape(ROWS, 128),
        attributes,
        target,
        tile_lists.reshape(TILES, LIST),
    )
    return pl.pallas_call(
        pullback_kernel,
        out_shape=jax.ShapeDtypeStruct(attributes.shape, F32),
        in_specs=[smem, pl.BlockSpec(memory_space=pl.ANY), vmem],
        out_specs=pl.BlockSpec(memory_space=pl.ANY),
        scratch_shapes=[
            pltpu.VMEM((ATTRS, 8192), F32),
            pltpu.VMEM((512, 128), F32),
            pltpu.VMEM((ATTRS, 8192), F32),
            pltpu.SemaphoreType.DMA((8,)),
            pltpu.SemaphoreType.DMA,
        ],
        name="splat_pullback",
    )(camera, attributes, feat_grad)


def solution(mesh):
    return jax.shard_map(
        shards,
        mesh=mesh,
        in_specs=(
            P(None, ("img", "cell")),
            P(),
            P(None, "img", "cell"),
            P(("img", "cell"), None),
            P("img", "cell", None),
            P("img", "cell"),
        ),
        out_specs=P(None, ("img", "cell")),
        check_vma=False,
    )
```

```python
import math

import jax
import jax.numpy as jnp
from jax import lax
from jax.experimental import pallas as pl
from jax.experimental.pallas import tpu as pltpu
from jax.sharding import PartitionSpec as P

F32 = jnp.float32
BF16 = jnp.bfloat16
I32 = jnp.int32
MESH = pl.DeviceIdType.MESH

TILE = 16
N_IMG = 8
N_CELL = 16
DEVICES = 128
LIST = 128
TILES = 32
ATTRS = 59
ROWS = 64
FEATS = 9
PAIRS = 5
EXACT = 5
BLOCKS = 8
GROUP = 4

WEIGHT_SSIM = 0.2
SMOOTHING = 0.01
STAB_ONE = 0.0001
STAB_TWO = 0.0009
BLUR_SIGMA = 1.5
SH_ZERO = 0.28209479177387814
SH_ONE = 0.4886025119029199
SH_TWO = (
    1.0925484305920792,
    -1.0925484305920792,
    0.31539156525252005,
    -1.0925484305920792,
    0.5462742152960396,
)
SH_THREE = (
    -0.5900435899266435,
    2.890611442640554,
    -0.4570457994644658,
    0.3731763325901154,
    -0.4570457994644658,
    1.445305721320277,
    -0.5900435899266435,
)


def blur_taps():
    raw = [math.exp(-((o - 5.0) ** 2) / (2.0 * BLUR_SIGMA * BLUR_SIGMA)) for o in range(11)]
    return [r / sum(raw) for r in raw]


TAPS = blur_taps()


def harmonic_basis(ux, uy, uz):
    xx, yy, zz = ux * ux, uy * uy, uz * uz
    return [
        SH_ZERO,
        -SH_ONE * uy,
        SH_ONE * uz,
        -SH_ONE * ux,
        SH_TWO[0] * ux * uy,
        SH_TWO[1] * uy * uz,
        SH_TWO[2] * (2.0 * zz - xx - yy),
        SH_TWO[3] * ux * uz,
        SH_TWO[4] * (xx - yy),
        SH_THREE[0] * uy * (3.0 * xx - yy),
        SH_THREE[1] * ux * uy * uz,
        SH_THREE[2] * uy * (4.0 * zz - xx - yy),
        SH_THREE[3] * uz * (2.0 * zz - 3.0 * xx - 3.0 * yy),
        SH_THREE[4] * ux * (4.0 * zz - xx - yy),
        SH_THREE[5] * uz * (xx - yy),
        SH_THREE[6] * ux * (xx - 3.0 * yy),
    ]


def project(rows, cam):
    pos = rows[0:3]
    scales = [jnp.exp(r) for r in rows[3:6]]
    qw = 1.5 + jnp.tanh(rows[6])
    qx, qy, qz = rows[7:10]
    inv = 1.0 / jnp.sqrt(qw * qw + qx * qx + qy * qy + qz * qz)
    qw, qx, qy, qz = qw * inv, qx * inv, qy * inv, qz * inv
    rot = [
        [1.0 - 2.0 * (qy * qy + qz * qz), 2.0 * (qx * qy - qw * qz), 2.0 * (qx * qz + qw * qy)],
        [2.0 * (qx * qy + qw * qz), 1.0 - 2.0 * (qx * qx + qz * qz), 2.0 * (qy * qz - qw * qx)],
        [2.0 * (qx * qz - qw * qy), 2.0 * (qy * qz + qw * qx), 1.0 - 2.0 * (qx * qx + qy * qy)],
    ]
    axes = [
        [
            (cam[s][0] * rot[0][k] + cam[s][1] * rot[1][k] + cam[s][2] * rot[2][k]) * scales[k]
            for k in range(3)
        ]
        for s in range(2)
    ]
    cov_a = axes[0][0] * axes[0][0] + axes[0][1] * axes[0][1] + axes[0][2] * axes[0][2] + 0.3
    cov_b = axes[0][0] * axes[1][0] + axes[0][1] * axes[1][1] + axes[0][2] * axes[1][2]
    cov_c = axes[1][0] * axes[1][0] + axes[1][1] * axes[1][1] + axes[1][2] * axes[1][2] + 0.3
    inv_det = 1.0 / (cov_a * cov_c - cov_b * cov_b)
    centers = [
        8.0
        + 7.0 * jnp.sin((cam[s][0] * pos[0] + cam[s][1] * pos[1] + cam[s][2] * pos[2]) / 3.0)
        for s in range(2)
    ]
    off = [pos[k] - cam[2][k] for k in range(3)]
    inv_dist = 1.0 / jnp.sqrt(off[0] * off[0] + off[1] * off[1] + off[2] * off[2])
    basis = harmonic_basis(off[0] * inv_dist, off[1] * inv_dist, off[2] * inv_dist)
    colours = []
    for c in range(3):
        total = 0.5 + basis[0] * rows[11 + 16 * c]
        for m in range(1, 16):
            total = total + basis[m] * rows[11 + 16 * c + m]
        colours.append(total)
    return centers + [cov_c * inv_det, -cov_b * inv_det, cov_a * inv_det] + colours


def read_camera(cam):
    return [[cam[s, k] for k in range(3)] for s in range(3)]


def spread_rows(attr, arows):
    def step(ct, carry):
        lanes = pl.ds(pl.multiple_of(ct * 128, 128), 128)
        for g in range(8):
            n = min(8, ATTRS - 8 * g)
            arows[pl.ds(pl.multiple_of(g * 512 + ct * 8, 8), n), :] = attr[8 * g : 8 * g + n, lanes]
        return carry

    lax.fori_loop(0, 64, step, 0)


def attr_rows(h):
    return [pl.ds((r // 8) * 512 + h * 64 + r % 8, 8, stride=8) for r in range(ATTRS)]


def wrap(value, count):
    return jnp.where(value >= count, value - count, value)


def ring_distance(d):
    return min(d, 4 - d)


STEPS = sorted(
    ((dy, dz) for dy in range(4) for dz in range(4)),
    key=lambda s: ring_distance(s[0]) + ring_distance(s[1]),
)


def pick(index, values):
    found = values[0]
    for n in range(1, len(values)):
        found = jnp.where(index == n, values[n], found)
    return found


class Place:
    def __init__(self, img, cell):
        self.y, self.z = lax.div(img, 2), lax.div(cell, 4)
        core, x = img - self.y * 2, cell - self.z * 4
        self.cores = [core, 1 - core]
        self.xs = [wrap(x + dx, 4) if dx else x for dx in range(4)]
        self.x_halves = [lax.div(v, 2) for v in self.xs]

    def devices(self, dy, dz):
        row, column = wrap(self.y + dy, 4) * 2, wrap(self.z + dz, 4)
        found = []
        for q in range(8):
            pi = row + self.cores[q % 2]
            found.append((pi, column * 4 + self.xs[q // 2], pi * 8 + column * 2 + self.x_halves[q // 2]))
        return found


def opposite(q):
    return (4 - q // 2) % 4 * 2 + q % 2


def each_step(place, act):
    for dy, dz in reversed(STEPS):
        seen = STEPS.index(((4 - dy) % 4, (4 - dz) % 4))
        for q, (pi, pc, half) in enumerate(place.devices(dy, dz)):
            if (dy, dz, q) != (0, 0, 0):
                act(pi, pc, half, seen * 8 + opposite(q), seen // 2)


def left_half():
    return lax.broadcasted_iota(I32, (8, 128), 1) < 64


def pack_message(values, msg, low_row, high_row):
    left = left_half()
    for i in range(PAIRS):
        a = values[2 * i]
        b = values[2 * i + 1] if 2 * i + 1 < FEATS else a
        msg[low_row(i), :] = jnp.where(left, a, pltpu.roll(b, 64, 1))
        msg[high_row(i), :] = jnp.where(left, pltpu.roll(a, 64, 1), b)


def unpack_message(msg, low_row, high_row):
    left = left_half()
    values = []
    for i in range(PAIRS):
        low, high = msg[low_row(i), :], msg[high_row(i), :]
        values.append(jnp.where(left, low, pltpu.roll(high, 64, 1)))
        if 2 * i + 1 < FEATS:
            values.append(jnp.where(left, pltpu.roll(low, 64, 1), high))
    return values


def one_hot(low):
    return jnp.where(lax.broadcasted_iota(I32, (256, 256), 0) == low, 1.0, 0.0).astype(BF16)


def split_ids(ids):
    high = lax.shift_right_logical(ids, 8)
    return high, ids - lax.shift_left(high, 8)


def row_pair(ref, at):
    both = ref[pl.ds(at, 2), :]
    return jnp.concatenate([both[0:1], both[1:2]], axis=1)


def make_parts(table, parts, thirds):
    for f in range(FEATS):
        rows = slice(32 * f, 32 * f + 32)
        for half in range(2):
            v = table[pl.ds(f * ROWS + half, 32, stride=2), :]
            top = v.astype(BF16)
            v = v - top.astype(F32)
            middle = v.astype(BF16)
            parts[rows, 128 * half : 128 * half + 128] = top
            parts[rows, 256 + 128 * half : 384 + 128 * half] = middle
            if f < EXACT:
                low = (v - middle.astype(F32)).astype(BF16)
                thirds[rows, 128 * half : 128 * half + 128] = low


def gather_blocks(parts, thirds, ids, hots):
    found, fine = [], []
    for hot in hots:
        found.append(
            jnp.dot(
                parts[...], jnp.concatenate([hot] * 2, axis=0), preferred_element_type=F32
            )
        )
        fine.append(jnp.dot(thirds[...], hot, preferred_element_type=F32))
    out = []
    for v, low, block in zip(found, fine, ids):
        mask = lax.broadcasted_iota(I32, (32, 256), 0) == split_ids(block)[0]
        rows = []
        for f in range(FEATS):
            value = v[32 * f : 32 * f + 32]
            if f < EXACT:
                value = value + low[32 * f : 32 * f + 32]
            rows.append(jnp.sum(jnp.where(mask, value, 0.0), axis=0, keepdims=True))
        out.append(rows)
    return out


def scatter_blocks(ids, grads, hots, acc):
    lhs = []
    for block, rows in zip(ids, grads):
        mask = lax.broadcasted_iota(I32, (32, 256), 0) == split_ids(block)[0]
        upper, lower = [], []
        for g in rows:
            top = g.astype(BF16).astype(F32)
            upper.append(jnp.where(mask, top, 0.0).astype(BF16))
            lower.append(jnp.where(mask, g - top, 0.0).astype(BF16))
        lhs.append(jnp.concatenate(upper + lower, axis=0))
    acc[...] += lax.dot_general(
        jnp.concatenate(lhs, axis=1),
        hots,
        (((1,), (1,)), ((), ())),
        preferred_element_type=F32,
    )


def two_parts(v):
    top = v.astype(BF16)
    return top, (v - top.astype(F32)).astype(BF16)


def swap_blocks(z):
    rows = z.shape[0]
    row_at = lax.broadcasted_iota(I32, z.shape, 0)
    lane_at = lax.broadcasted_iota(I32, z.shape, 1)
    for bit in (1, 2, 4, 8):
        row_bit = (row_at // bit) % 2
        lane_bit = (lane_at // (16 * bit)) % 2
        down = pltpu.roll(pltpu.roll(z, rows - bit, 0), 16 * bit, 1)
        up = pltpu.roll(pltpu.roll(z, bit, 0), 256 - 16 * bit, 1)
        z = jnp.where(row_bit == lane_bit, z, jnp.where(row_bit == 0, down, up))
    return z


NORTH, SOUTH, PACK_WEST, PACK_EAST, FROM_WEST, FROM_EAST = 192, 288, 384, 400, 416, 432
FROM_NW, FROM_NE, FROM_SW, FROM_SE, EXT_ROWS = 448, 456, 464, 472, 480
BORDER_ROWS = 256


def pack_columns(ext):
    lane = lax.broadcasted_iota(I32, (8, 128), 1)
    for t in range(2):
        west = jnp.zeros((8, 128), F32)
        east = west
        for k in range(6):
            here = (lane >= 16 * k) & (lane < 16 * k + 16)
            at = t * 48 + 8 * k
            first, last = ext[at : at + 8, :], ext[96 + at : 104 + at, :]
            west = jnp.where(here, pltpu.roll(first, 16 * k, 1) if k else first, west)
            east = jnp.where(here, pltpu.roll(last, 16 * k + 16, 1), east)
        ext[PACK_WEST + 8 * t : PACK_WEST + 8 * t + 8, :] = west
        ext[PACK_EAST + 8 * t : PACK_EAST + 8 * t + 8, :] = east


def border_copies(ext, img, cell, send, recv):
    west, east = jnp.where(cell == 0, N_CELL - 1, cell - 1), wrap(cell + 1, N_CELL)
    north, south = jnp.where(img == 0, N_IMG - 1, img - 1), wrap(img + 1, N_IMG)
    plan = [
        (PACK_WEST, FROM_SE, 8, north, west),
        (PACK_EAST, FROM_SW, 8, north, east),
        (PACK_WEST + 8, FROM_NE, 8, south, west),
        (PACK_EAST + 8, FROM_NW, 8, south, east),
        (PACK_WEST, FROM_EAST, 16, img, west),
        (PACK_EAST, FROM_WEST, 16, img, east),
    ]
    for k in range(2):
        plan.append((96 * k, SOUTH + 48 * k, 48, north, cell))
        plan.append((96 * k + 48, NORTH + 48 * k, 48, south, cell))
    for source, dest, count, to_img, to_cell in plan:
        pltpu.make_async_remote_copy(
            src_ref=ext.at[pl.ds(source, count)],
            dst_ref=ext.at[pl.ds(dest, count)],
            send_sem=send,
            recv_sem=recv,
            device_id=(to_img, to_cell),
            device_id_type=MESH,
        ).start()


def wait_rows(ref, count, sem):
    part = ref.at[pl.ds(0, count)]
    pltpu.make_async_copy(part, part, sem).wait()


def window(ext, img, cell, c, row_block, half):
    lane = lax.broadcasted_iota(I32, (8, 128), 1)
    at = 16 * c + 8 * half
    bases = [NORTH, 0, 48, SOUTH][row_block]
    step = 48 if row_block in (0, 3) else 96
    sides = [
        (FROM_NW, FROM_NE),
        (FROM_WEST, FROM_EAST),
        (FROM_WEST + 8, FROM_EAST + 8),
        (FROM_SW, FROM_SE),
    ][row_block]
    first = pltpu.roll(ext[bases + at : bases + at + 8, :], 64, 1)
    second = pltpu.roll(ext[bases + step + at : bases + step + at + 8, :], 64, 1)
    block = 16 * (2 * c + half)
    left = pltpu.roll(ext[sides[0] : sides[0] + 8, :], (48 - block) % 128, 1)
    right = pltpu.roll(ext[sides[1] : sides[1] + 8, :], (64 - block) % 128, 1)
    keep_left = jnp.where(cell == 0, 64, 48)
    keep_right = jnp.where(cell == N_CELL - 1, 64, 80)
    tiles = [
        jnp.where(lane < 64, jnp.where(lane >= keep_left, left, 0.0), first),
        jnp.where(lane < 64, first, second),
        jnp.where(lane < 64, second, jnp.where(lane < keep_right, right, 0.0)),
    ]
    if row_block == 0:
        tiles = [v * jnp.where(img == 0, 0.0, 1.0) for v in tiles]
    if row_block == 3:
        tiles = [v * jnp.where(img == N_IMG - 1, 0.0, 1.0) for v in tiles]
    return tiles


def blur(ref, start, stride):
    down = []
    for j in range(3):
        at = start + j * stride
        total = TAPS[5] * ref[pl.ds(at + 5, 8), :]
        for o in range(5):
            total = total + TAPS[o] * (ref[pl.ds(at + o, 8), :] + ref[pl.ds(at + 10 - o, 8), :])
        down.append(total)
    v = jnp.concatenate(down, axis=1)
    total = TAPS[5] * v
    for o in range(5):
        d = 5 - o
        total = total + TAPS[o] * (pltpu.roll(v, d, 1) + pltpu.roll(v, 384 - d, 1))
    return total


def ssim_value(mean_render, mean_target, square_render, square_target, cross_term):
    spread_render = square_render - mean_render * mean_render
    spread_target = square_target - mean_target * mean_target
    covariance = cross_term - mean_render * mean_target
    upper = (2.0 * mean_render * mean_target + STAB_ONE) * (2.0 * covariance + STAB_TWO)
    lower = (mean_render * mean_render + mean_target * mean_target + STAB_ONE) * (
        spread_render + spread_target + STAB_TWO
    )
    return upper / lower


def map_row(m, c):
    return (m * 3 + c) * 3 * 64


def step_kernel(
    cam_ref,
    len_ref,
    vis,
    attr_hbm,
    target,
    lists,
    out,
    attr,
    arows,
    table,
    parts,
    thirds,
    hot_list,
    hot_own,
    ids_in,
    ids_own,
    msg,
    inbox,
    msg_back,
    inbox_back,
    ext_render,
    ext_target,
    entry,
    tri_before,
    tri_after,
    weights,
    ratio,
    tile_rows,
    moments,
    maps,
    coefs,
    blurred,
    acc,
    sems,
    id_sems,
    back_sems,
):
    img = lax.axis_index("img")
    cell = lax.axis_index("cell")
    me = img * N_CELL + cell

    barrier = pltpu.get_barrier_semaphore()
    place = Place(img, cell)
    each_step(
        place,
        lambda pi, pc, *_: pl.semaphore_signal(
            barrier, 1, device_id=(pi, pc), device_id_type=MESH
        ),
    )
    load_attr = pltpu.make_async_copy(attr_hbm, attr, sems.at[10])
    load_attr.start()

    for k in range(2):
        for t in range(2):
            for c in range(3):
                at = 96 * k + 48 * t + 16 * c
                ext_target[at : at + 16, :] = target[
                    c, 16 * t : 16 * t + 16, 128 * k : 128 * k + 128
                ]
    pack_columns(ext_target)

    def list_hot(b, carry):
        hot_list[:, pl.ds(pl.multiple_of(b * 256, 256), 256)] = one_hot(
            split_ids(row_pair(lists, b * 2))[1]
        )
        return carry

    lax.fori_loop(0, TILES // 2, list_hot, 0)

    cam = read_camera(cam_ref)
    load_attr.wait()
    spread_rows(attr, arows)

    def project_step(h, carry):
        rows = [arows[at, :] for at in attr_rows(h)]
        feats = project(rows, cam)
        feats.insert(5, jax.nn.sigmoid(rows[10]))
        for f in range(FEATS):
            table[pl.ds(pl.multiple_of(f * ROWS + h * 8, 8), 8), :] = feats[f]
        return carry

    lax.fori_loop(0, 8, project_step, 0)
    make_parts(table, parts, thirds)

    row_at = lax.broadcasted_iota(I32, (128, 128), 0)
    lane_at = lax.broadcasted_iota(I32, (128, 128), 1)
    before = jnp.where(row_at < lane_at, 1.0, 0.0).astype(BF16)
    after = jnp.where(row_at > lane_at, 1.0, 0.0).astype(BF16)
    for half in range(2):
        tri_before[128 * half : 128 * half + 128, :] = before
        tri_after[128 * half : 128 * half + 128, :] = after

    pl.semaphore_wait(barrier, DEVICES - 1)

    def send_ids(pi, pc, half, rank, group):
        pltpu.make_async_remote_copy(
            src_ref=vis.at[pl.ds(half, 1)],
            dst_ref=ids_in.at[pl.ds(rank, 1)],
            send_sem=sems.at[0],
            recv_sem=id_sems.at[group],
            device_id=(pi, pc),
            device_id_type=MESH,
        ).start()

    each_step(place, send_ids)
    pltpu.make_async_copy(
        vis.at[pl.ds(me // 2, 1)], ids_in.at[pl.ds(0, 1)], id_sems.at[0]
    ).start()
    border_copies(ext_target, img, cell, sems.at[2], sems.at[3])

    odd = me - (me // 2) * 2
    left = left_half()
    left_row = lax.broadcasted_iota(I32, (1, 128), 1) < 64

    def reply_step(g, carry):
        wait_rows(ids_in, 16, id_sems.at[g])
        at = pl.multiple_of(g * 16, 8)
        first, second = ids_in[pl.ds(at, 8), :], ids_in[pl.ds(at + 8, 8), :]
        even_form = jnp.where(left, first, pltpu.roll(second, 64, 1))
        odd_form = jnp.where(left, pltpu.roll(first, 64, 1), second)
        both = jnp.where(odd == 0, even_form, odd_form)
        ids_own[pl.ds(pl.multiple_of(g * 8, 8), 8), :] = both
        ids = [
            jnp.concatenate([both[2 * n : 2 * n + 1], both[2 * n + 1 : 2 * n + 2]], axis=1)
            for n in range(4)
        ]
        hots = [one_hot(split_ids(v)[1]) for v in ids]
        for n in range(4):
            hot_own[:, pl.ds(pl.multiple_of(g * 1024 + n * 256, 256), 256)] = hots[n]
        got = gather_blocks(parts, thirds, ids, hots)
        for n in range(4):
            for row in range(2):
                d = g * 128 + (2 * n + row) * 8
                for i in range(PAIRS):
                    low = got[n][2 * i][:, 128 * row : 128 * row + 128]
                    high = got[n][min(2 * i + 1, FEATS - 1)][:, 128 * row : 128 * row + 128]
                    msg[pl.ds(d + i, 1), :] = jnp.where(left_row, low, pltpu.roll(high, 64, 1))
                    msg[pl.ds(d + 64 + i, 1), :] = jnp.where(
                        left_row, pltpu.roll(low, 64, 1), high
                    )
        for side in range(2):
            dy = pick(g, [STEPS[2 * n + side][0] for n in range(8)])
            dz = pick(g, [STEPS[2 * n + side][1] for n in range(8)])

            for q, (pi, pc, _) in enumerate(place.devices(dy, dz)):
                copy = pltpu.make_async_remote_copy(
                    src_ref=msg.at[pl.ds(pl.multiple_of(g * 128 + side * 64 + q * 8, 8), PAIRS)],
                    dst_ref=inbox.at[pl.ds(pl.multiple_of(me * 8, 8), PAIRS)],
                    send_sem=sems.at[4],
                    recv_sem=sems.at[5],
                    device_id=(pi, pc),
                    device_id_type=MESH,
                )
                if side == 0 and q == 0:
                    pl.when(g > 0)(copy.start)
                else:
                    copy.start()
        return carry

    lax.fori_loop(0, 8, reply_step, 0)
    own = pl.ds(pl.multiple_of(me * 8, 8), PAIRS)
    inbox[own, :] = msg[0:PAIRS, :]

    wait_rows(ext_target, BORDER_ROWS, sems.at[3])
    for c in range(3):
        for row_block in range(4):
            for half in range(2):
                strips = window(ext_target, img, cell, c, row_block, half)
                for j in range(3):
                    for m, v in ((3, strips[j]), (4, strips[j] * strips[j])):
                        at = map_row(m, c) + 64 * j + 16 * row_block + 8 * half
                        maps[at : at + 8, :] = v

    def target_blur(c, carry):
        for m in range(2):
            for r in range(6):
                at = pl.multiple_of((m * 3 + c) * 48 + 8 * r, 8)
                blurred[pl.ds(at, 8), :] = blur(maps, map_row(3 + m, c) + 6 + 8 * r, 64)
        return carry

    lax.fori_loop(0, 3, target_blur, 0)

    wait_rows(inbox, (DEVICES - 1) * PAIRS, sems.at[5])

    def table_step(h, carry):
        values = unpack_message(
            inbox,
            lambda i: pl.ds(h * 128 + i, 8, stride=16),
            lambda i: pl.ds(h * 128 + 8 + i, 8, stride=16),
        )
        for f in range(FEATS):
            table[pl.ds(pl.multiple_of(f * ROWS + h * 8, 8), 8), :] = values[f]
        return carry

    lax.fori_loop(0, 8, table_step, 0)
    make_parts(table, parts, thirds)

    def list_step(k, carry):
        got = gather_blocks(
            parts,
            thirds,
            [row_pair(lists, k * 16 + 2 * n) for n in range(8)],
            [
                hot_list[:, pl.ds(pl.multiple_of(k * 2048 + n * 256, 256), 256)]
                for n in range(8)
            ],
        )
        for n in range(8):
            for row in range(2):
                for f in range(FEATS):
                    entry[pl.ds(f * TILES + k * 16 + 2 * n + row, 1), :] = got[n][f][
                        :, 128 * row : 128 * row + 128
                    ]
        return carry

    lax.fori_loop(0, 2, list_step, 0)

    def entry_row(f, t):
        return entry[pl.ds(f * TILES + t, 1), :]

    across = lax.broadcasted_iota(I32, (16, 128), 0).astype(F32) + 0.5
    lane_row = lax.broadcasted_iota(I32, (1, 128), 1)

    def spans(tile_row, k):
        return [tile_row * 16 + k * GROUP + n for n in range(GROUP)]

    def pixels_of(t):
        return pl.ds(pl.multiple_of(t * 256, 256), 256)

    for tile_row in range(2):

        def render_step(k, carry, tile_row=tile_row):
            tiles = spans(tile_row, k)
            alphas, sums = [], []
            for n, t in enumerate(tiles):
                alive = lane_row < len_ref[tile_row, k * GROUP + n]
                opacity = jnp.where(alive, entry_row(5, t), 0.0)
                dx = across - entry_row(0, t)
                center_y = entry_row(1, t)
                square_x = (-0.5 * entry_row(2, t)) * dx * dx
                mixed = -entry_row(3, t) * dx
                half_y = -0.5 * entry_row(4, t)
                alpha = []
                for y in range(16):
                    dy = (y + 0.5) - center_y
                    alpha.append(opacity * jnp.exp(square_x + dy * (mixed + half_y * dy)))
                alpha = jnp.concatenate(alpha, axis=0)
                logs = jnp.log(1.0 - alpha)
                sums.append(
                    jnp.dot(
                        jnp.concatenate(two_parts(logs), axis=1),
                        tri_before[...],
                        preferred_element_type=F32,
                    )
                )
                ratio[pixels_of(t), :] = alpha
                alphas.append(alpha)
            products = []
            for n, t in enumerate(tiles):
                weight = jnp.concatenate(two_parts(jnp.exp(sums[n]) * alphas[n]), axis=1)
                weights[pixels_of(t), :] = weight
                colour = [two_parts(entry_row(6 + c, t)) for c in range(3)]
                lhs = jnp.concatenate(
                    [c[part] for part in range(2) for c in colour] + [jnp.zeros((10, 128), BF16)],
                    axis=0,
                )
                products.append(
                    lax.dot_general(
                        jnp.concatenate([lhs, lhs], axis=1),
                        weight,
                        (((1,), (1,)), ((), ())),
                        preferred_element_type=F32,
                    )
                )
            for n in range(GROUP):
                for c in range(3):
                    tile_rows[pl.ds(tile_row * 48 + c * 16 + k * GROUP + n, 1), :] = (
                        products[n][c : c + 1] + products[n][3 + c : 4 + c]
                    )
            return carry

        lax.fori_loop(0, 16 // GROUP, render_step, 0)

    picture = swap_blocks(tile_rows[...])
    for k in range(2):
        ext_render[96 * k : 96 * k + 96, :] = picture[:, 128 * k : 128 * k + 128]
    pack_columns(ext_render)
    border_copies(ext_render, img, cell, sems.at[6], sems.at[7])

    def ratio_step(t, carry):
        alpha = ratio[pixels_of(t), :]
        ratio[pixels_of(t), :] = alpha / (1.0 - alpha)
        return carry

    lax.fori_loop(0, TILES, ratio_step, 0)
    wait_rows(ext_render, BORDER_ROWS, sems.at[7])

    for c in range(3):
        for row_block in range(4):
            for half in range(2):
                strips = window(ext_render, img, cell, c, row_block, half)
                for j in range(3):
                    at = 64 * j + 16 * row_block + 8 * half
                    v = strips[j]
                    wanted = maps[map_row(3, c) + at : map_row(3, c) + at + 8, :]
                    for m, value in ((0, v), (1, v * v), (2, v * wanted)):
                        maps[map_row(m, c) + at : map_row(m, c) + at + 8, :] = value
    row_at = lax.broadcasted_iota(I32, (8, 384), 0) + (img * 32 - 5)
    lane_at = lax.broadcasted_iota(I32, (8, 384), 1) + (cell * 256 - 64)
    inside = (lane_at >= 0) & (lane_at < N_CELL * 256)

    def similarity_step(c, carry):
        for r in range(6):
            mean, square, cross = [blur(maps, map_row(m, c) + 6 + 8 * r, 64) for m in range(3)]
            mean_target, square_target = [
                blurred[pl.ds(pl.multiple_of((m * 3 + c) * 48 + 8 * r, 8), 8), :]
                for m in range(2)
            ]
            _, pullback = jax.vjp(
                lambda x, y, z, mt=mean_target, st=square_target: ssim_value(x, mt, y, st, z),
                mean,
                square,
                cross,
            )
            keep = inside & (row_at + 8 * r >= 0) & (row_at + 8 * r < N_IMG * 32)
            for m, v in enumerate(pullback(jnp.full((8, 384), -WEIGHT_SSIM, F32))):
                v = jnp.where(keep, v, 0.0)
                for j in range(3):
                    at = pl.multiple_of(((m * 3 + c) * 3 + j) * 48 + 8 * r, 8)
                    coefs[pl.ds(at, 8), :] = v[:, 128 * j : 128 * j + 128]
        return carry

    lax.fori_loop(0, 3, similarity_step, 0)
    left = left_half()

    def image_step(c, carry):
        for r in range(4):
            back_mean, back_square, back_cross = [
                blur(coefs, (m * 3 + c) * 3 * 48 + 8 * r, 48) for m in range(3)
            ]
            found = []
            for j in range(3):
                lanes = slice(128 * j, 128 * j + 128)
                at = 64 * j + 16 + 8 * r
                image = maps[pl.ds(pl.multiple_of(map_row(0, c) + at, 8), 8), :]
                wanted = maps[pl.ds(pl.multiple_of(map_row(3, c) + at, 8), 8), :]
                difference = image - wanted
                slope = (
                    (1.0 - WEIGHT_SSIM)
                    * difference
                    / jnp.sqrt(difference * difference + SMOOTHING * SMOOTHING)
                )
                found.append(
                    pltpu.roll(
                        slope
                        + back_mean[:, lanes]
                        + 2.0 * image * back_square[:, lanes]
                        + wanted * back_cross[:, lanes],
                        64,
                        1,
                    )
                )
            at = pl.multiple_of((r // 2) * 48 + c * 16 + (r % 2) * 8, 8)
            tile_rows[pl.ds(at, 8), :] = jnp.concatenate(
                [jnp.where(left, found[0], found[1]), jnp.where(left, found[1], found[2])],
                axis=1,
            )
        return carry

    lax.fori_loop(0, 3, image_step, 0)
    tile_rows[...] = swap_blocks(tile_rows[...])

    for tile_row in range(2):

        def back_step(k, carry, tile_row=tile_row):
            tiles = spans(tile_row, k)
            grad_rows, values = [], []
            for n, t in enumerate(tiles):
                pixel_grad = [
                    two_parts(tile_rows[pl.ds(tile_row * 48 + c * 16 + k * GROUP + n, 1), :])
                    for c in range(3)
                ]
                colour = [two_parts(entry_row(6 + c, t)) for c in range(3)]
                tops, lows = [g[0] for g in pixel_grad], [g[1] for g in pixel_grad]
                grad_rows.append(
                    jnp.concatenate(tops + lows + tops + [jnp.zeros((7, 256), BF16)], axis=0)
                )
                colour_rows = jnp.concatenate(
                    [c[0] for c in colour] * 2
                    + [c[1] for c in colour]
                    + [jnp.zeros((7, 128), BF16)],
                    axis=0,
                )
                values.append(
                    lax.dot_general(
                        grad_rows[n],
                        colour_rows,
                        (((0,), (0,)), ((), ())),
                        preferred_element_type=F32,
                    )
                )
            gains, laters, mixes = [], [], []
            for n, t in enumerate(tiles):
                weight = weights[pixels_of(t), :]
                mixes.append(jnp.dot(grad_rows[n], weight, preferred_element_type=F32))
                gain = values[n] * (weight[:, :128].astype(F32) + weight[:, 128:].astype(F32))
                laters.append(
                    jnp.dot(
                        jnp.concatenate(two_parts(gain), axis=1),
                        tri_after[...],
                        preferred_element_type=F32,
                    )
                )
                gains.append(gain)
            for n, t in enumerate(tiles):
                pull = gains[n] - ratio[pixels_of(t), :] * laters[n]
                dx = across - entry_row(0, t)
                center_y = entry_row(1, t)
                sum_0 = sum_y = sum_yy = None
                for y in range(16):
                    dy = (y + 0.5) - center_y
                    part = pull[16 * y : 16 * y + 16]
                    part_y = part * dy
                    part_yy = part_y * dy
                    sum_0 = part if y == 0 else sum_0 + part
                    sum_y = part_y if y == 0 else sum_y + part_y
                    sum_yy = part_yy if y == 0 else sum_yy + part_yy
                sum_x = sum_0 * dx
                found = [sum_0, sum_x, sum_y, sum_x * dx, sum_y * dx, sum_yy]
                for m in range(6):
                    moments[pl.ds(m * TILES + t, 1), :] = jnp.sum(
                        found[m], axis=0, keepdims=True
                    )
                for c in range(3):
                    both = mixes[n][c : c + 1] + mixes[n][3 + c : 4 + c]
                    moments[pl.ds((6 + c) * TILES + t, 1), :] = both[:, :128] + both[:, 128:]
            return carry

        lax.fori_loop(0, 16 // GROUP, back_step, 0)

    feat = [entry[f * TILES : (f + 1) * TILES, :] for f in range(6)]
    mom = [moments[m * TILES : (m + 1) * TILES, :] for m in range(6)]
    entry[0:TILES, :] = feat[2] * mom[1] + feat[3] * mom[2]
    entry[TILES : 2 * TILES, :] = feat[3] * mom[1] + feat[4] * mom[2]
    entry[2 * TILES : 3 * TILES, :] = -0.5 * mom[3]
    entry[3 * TILES : 4 * TILES, :] = -mom[4]
    entry[4 * TILES : 5 * TILES, :] = -0.5 * mom[5]
    entry[5 * TILES : 6 * TILES, :] = mom[0]
    entry[6 * TILES : 9 * TILES, :] = moments[6 * TILES : 9 * TILES, :]

    acc[...] = jnp.zeros_like(acc)

    def slot_step(k, carry):
        at = [k * 2 * BLOCKS + 2 * n for n in range(BLOCKS)]
        scatter_blocks(
            [row_pair(lists, a) for a in at],
            [[row_pair(entry, f * TILES + a) for f in range(FEATS)] for a in at],
            hot_list[:, pl.ds(pl.multiple_of(k * 256 * BLOCKS, 256), 256 * BLOCKS)],
            acc,
        )
        return carry

    lax.fori_loop(0, TILES // (2 * BLOCKS), slot_step, 0)

    def total_rows(f, h):
        a = acc[pl.ds(pl.multiple_of(f * 32 + h * 8, 8), 8), :]
        b = acc[pl.ds(pl.multiple_of(288 + f * 32 + h * 8, 8), 8), :]
        return a + b

    def back_pack(h, carry):
        totals = [total_rows(f, h) for f in range(FEATS)]
        for half in range(2):
            pack_message(
                [v[:, 128 * half : 128 * half + 128] for v in totals],
                msg_back,
                lambda i: pl.ds(h * 256 + (2 * half) * 8 + i, 8, stride=32),
                lambda i: pl.ds(h * 256 + (2 * half + 1) * 8 + i, 8, stride=32),
            )
        return carry

    lax.fori_loop(0, 4, back_pack, 0)

    def send_back(pi, pc, half, rank, group):
        pltpu.make_async_remote_copy(
            src_ref=msg_back.at[pl.ds(pl.multiple_of((pi * N_CELL + pc) * 8, 8), PAIRS)],
            dst_ref=inbox_back.at[pl.ds(pl.multiple_of(rank * 8, 8), PAIRS)],
            send_sem=sems.at[8],
            recv_sem=back_sems.at[group],
            device_id=(pi, pc),
            device_id_type=MESH,
        ).start()

    each_step(place, send_back)
    pltpu.make_async_copy(
        msg_back.at[own], inbox_back.at[pl.ds(0, PAIRS)], back_sems.at[0]
    ).start()

    acc[...] = jnp.zeros_like(acc)

    def owner_step(k, carry):
        for side in range(BLOCKS // 4):
            g = k * (BLOCKS // 4) + side
            wait_rows(inbox_back, 16 * PAIRS, back_sems.at[g])
            values = unpack_message(
                inbox_back,
                lambda i: pl.ds(g * 128 + i, 8, stride=8),
                lambda i: pl.ds(g * 128 + 64 + i, 8, stride=8),
            )
            for f in range(FEATS):
                table[pl.ds(pl.multiple_of(f * ROWS + g * 8, 8), 8), :] = values[f]
        at = [k * 2 * BLOCKS + 2 * n for n in range(BLOCKS)]
        scatter_blocks(
            [row_pair(ids_own, a) for a in at],
            [[row_pair(table, f * ROWS + a) for f in range(FEATS)] for a in at],
            hot_own[:, pl.ds(pl.multiple_of(k * 256 * BLOCKS, 256), 256 * BLOCKS)],
            acc,
        )
        return carry

    lax.fori_loop(0, ROWS // (2 * BLOCKS), owner_step, 0)

    def finish(h, carry):
        for f in range(FEATS):
            v = total_rows(f, h)
            for half in range(2):
                out[pl.ds(f * ROWS + h * 16 + half, 8, stride=2), :] = v[
                    :, 128 * half : 128 * half + 128
                ]
        return carry

    lax.fori_loop(0, 4, finish, 0)

    wait_rows(ids_in, DEVICES - 1, sems.at[0])
    wait_rows(ext_target, BORDER_ROWS, sems.at[2])
    wait_rows(msg, (DEVICES - 1) * PAIRS, sems.at[4])
    wait_rows(ext_render, BORDER_ROWS, sems.at[6])
    wait_rows(msg_back, (DEVICES - 1) * PAIRS, sems.at[8])


def pullback_kernel(cam_ref, attr_hbm, feat_grad, out_hbm, attr, arows, result, load_sems, save_sem):
    cam = read_camera(cam_ref)

    def block(h):
        return pl.ds(pl.multiple_of(h * 1024, 1024), 1024)

    def load(h):
        return pltpu.make_async_copy(
            attr_hbm.at[:, block(h)], attr.at[:, block(h)], load_sems.at[h]
        )

    for h in range(8):
        load(h).start()

    def step(h, carry):
        load(h).wait()
        for k in range(8):
            lanes = pl.ds(pl.multiple_of(h * 1024 + k * 128, 128), 128)
            for g in range(8):
                n = min(8, ATTRS - 8 * g)
                arows[g * 64 + 8 * k : g * 64 + 8 * k + n, :] = attr[8 * g : 8 * g + n, lanes]
        places = [pl.ds((r // 8) * 64 + r % 8, 8, stride=8) for r in range(ATTRS)]
        rows = [arows[at, :] for at in places]
        _, pullback = jax.vjp(lambda r: project(r, cam), rows)
        grads = [
            feat_grad[pl.ds(pl.multiple_of(f * ROWS + h * 8, 8), 8), :] for f in range(FEATS)
        ]
        log_opacity = grads.pop(5)
        (found,) = pullback(grads)
        found[10] = log_opacity * (1.0 - jax.nn.sigmoid(rows[10]))
        for at, v in zip(places, found):
            arows[at, :] = v
        for k in range(8):
            lanes = pl.ds(pl.multiple_of(h * 1024 + k * 128, 128), 128)
            for g in range(8):
                n = min(8, ATTRS - 8 * g)
                result[8 * g : 8 * g + n, lanes] = arows[g * 64 + 8 * k : g * 64 + 8 * k + n, :]
        pltpu.make_async_copy(result.at[:, block(h)], out_hbm.at[:, block(h)], save_sem).start()
        return carry

    lax.fori_loop(0, 8, step, 0)
    pltpu.make_async_copy(result, out_hbm, save_sem).wait()


def shards(attributes, camera, target, visible_index, tile_lists, tile_len):
    vmem = pl.BlockSpec(memory_space=pltpu.VMEM)
    smem = pl.BlockSpec(memory_space=pltpu.SMEM)
    feat_grad = pl.pallas_call(
        step_kernel,
        out_shape=jax.ShapeDtypeStruct((FEATS * ROWS, 128), F32),
        in_specs=[smem, smem, vmem, pl.BlockSpec(memory_space=pl.ANY), vmem, vmem],
        out_specs=vmem,
        scratch_shapes=[
            pltpu.VMEM((ATTRS, 8192), F32),
            pltpu.VMEM((4096, 128), F32),
            pltpu.VMEM((FEATS * ROWS, 128), F32),
            pltpu.VMEM((FEATS * 32, 512), BF16),
            pltpu.VMEM((EXACT * 32, 256), BF16),
            pltpu.VMEM((256, TILES * LIST), BF16),
            pltpu.VMEM((256, ROWS * 128), BF16),
            pltpu.VMEM((DEVICES, 128), I32),
            pltpu.VMEM((ROWS, 128), I32),
            pltpu.VMEM((DEVICES * 8, 128), F32),
            pltpu.VMEM((DEVICES * 8, 128), F32),
            pltpu.VMEM((DEVICES * 8, 128), F32),
            pltpu.VMEM((DEVICES * 8, 128), F32),
            pltpu.VMEM((EXT_ROWS, 128), F32),
            pltpu.VMEM((EXT_ROWS, 128), F32),
            pltpu.VMEM((FEATS * TILES, 128), F32),
            pltpu.VMEM((256, 128), BF16),
            pltpu.VMEM((256, 128), BF16),
            pltpu.VMEM((TILES * 256, 256), BF16),
            pltpu.VMEM((TILES * 256, 128), F32),
            pltpu.VMEM((96, 256), F32),
            pltpu.VMEM((FEATS * TILES, 128), F32),
            pltpu.VMEM((5 * 3 * 3 * 64, 128), F32),
            pltpu.VMEM((3 * 3 * 3 * 48, 128), F32),
            pltpu.VMEM((2 * 3 * 48, 384), F32),
            pltpu.VMEM((2 * FEATS * 32, 256), F32),
            pltpu.SemaphoreType.DMA((11,)),
            pltpu.SemaphoreType.DMA((8,)),
            pltpu.SemaphoreType.DMA((8,)),
        ],
        compiler_params=pltpu.CompilerParams(
            collective_id=0, has_side_effects=True, vmem_limit_bytes=58 * 1024 * 1024
        ),
        name="splat_step",
    )(
        camera,
        tile_len,
        visible_index.reshape(ROWS, 128),
        attributes,
        target,
        tile_lists.reshape(TILES, LIST),
    )
    return pl.pallas_call(
        pullback_kernel,
        out_shape=jax.ShapeDtypeStruct(attributes.shape, F32),
        in_specs=[smem, pl.BlockSpec(memory_space=pl.ANY), vmem],
        out_specs=pl.BlockSpec(memory_space=pl.ANY),
        scratch_shapes=[
            pltpu.VMEM((ATTRS, 8192), F32),
            pltpu.VMEM((512, 128), F32),
            pltpu.VMEM((ATTRS, 8192), F32),
            pltpu.SemaphoreType.DMA((8,)),
            pltpu.SemaphoreType.DMA,
        ],
        name="splat_pullback",
    )(camera, attributes, feat_grad)


def solution(mesh):
    return jax.shard_map(
        shards,
        mesh=mesh,
        in_specs=(
            P(None, ("img", "cell")),
            P(),
            P(None, "img", "cell"),
            P(("img", "cell"), None),
            P("img", "cell", None),
            P("img", "cell"),
        ),
        out_specs=P(None, ("img", "cell")),
        check_vma=False,
    )
```

```python
import math

import jax
import jax.numpy as jnp
from jax import lax
from jax.experimental import pallas as pl
from jax.experimental.pallas import tpu as pltpu
from jax.sharding import PartitionSpec as P

F32 = jnp.float32
BF16 = jnp.bfloat16
I32 = jnp.int32
MESH = pl.DeviceIdType.MESH

TILE = 16
N_IMG = 8
N_CELL = 16
DEVICES = 128
LIST = 128
TILES = 32
ATTRS = 59
ROWS = 64
FEATS = 9
PAIRS = 5
EXACT = 5
BLOCKS = 8
GROUP = 4

WEIGHT_SSIM = 0.2
SMOOTHING = 0.01
STAB_ONE = 0.0001
STAB_TWO = 0.0009
BLUR_SIGMA = 1.5
SH_ZERO = 0.28209479177387814
SH_ONE = 0.4886025119029199
SH_TWO = (
    1.0925484305920792,
    -1.0925484305920792,
    0.31539156525252005,
    -1.0925484305920792,
    0.5462742152960396,
)
SH_THREE = (
    -0.5900435899266435,
    2.890611442640554,
    -0.4570457994644658,
    0.3731763325901154,
    -0.4570457994644658,
    1.445305721320277,
    -0.5900435899266435,
)


def blur_taps():
    raw = [math.exp(-((o - 5.0) ** 2) / (2.0 * BLUR_SIGMA * BLUR_SIGMA)) for o in range(11)]
    return [r / sum(raw) for r in raw]


TAPS = blur_taps()


def harmonic_basis(ux, uy, uz):
    xx, yy, zz = ux * ux, uy * uy, uz * uz
    return [
        SH_ZERO,
        -SH_ONE * uy,
        SH_ONE * uz,
        -SH_ONE * ux,
        SH_TWO[0] * ux * uy,
        SH_TWO[1] * uy * uz,
        SH_TWO[2] * (2.0 * zz - xx - yy),
        SH_TWO[3] * ux * uz,
        SH_TWO[4] * (xx - yy),
        SH_THREE[0] * uy * (3.0 * xx - yy),
        SH_THREE[1] * ux * uy * uz,
        SH_THREE[2] * uy * (4.0 * zz - xx - yy),
        SH_THREE[3] * uz * (2.0 * zz - 3.0 * xx - 3.0 * yy),
        SH_THREE[4] * ux * (4.0 * zz - xx - yy),
        SH_THREE[5] * uz * (xx - yy),
        SH_THREE[6] * ux * (xx - 3.0 * yy),
    ]


def project(rows, cam):
    pos = rows[0:3]
    scales = [jnp.exp(r) for r in rows[3:6]]
    qw = 1.5 + jnp.tanh(rows[6])
    qx, qy, qz = rows[7:10]
    inv = 1.0 / jnp.sqrt(qw * qw + qx * qx + qy * qy + qz * qz)
    qw, qx, qy, qz = qw * inv, qx * inv, qy * inv, qz * inv
    rot = [
        [1.0 - 2.0 * (qy * qy + qz * qz), 2.0 * (qx * qy - qw * qz), 2.0 * (qx * qz + qw * qy)],
        [2.0 * (qx * qy + qw * qz), 1.0 - 2.0 * (qx * qx + qz * qz), 2.0 * (qy * qz - qw * qx)],
        [2.0 * (qx * qz - qw * qy), 2.0 * (qy * qz + qw * qx), 1.0 - 2.0 * (qx * qx + qy * qy)],
    ]
    axes = [
        [
            (cam[s][0] * rot[0][k] + cam[s][1] * rot[1][k] + cam[s][2] * rot[2][k]) * scales[k]
            for k in range(3)
        ]
        for s in range(2)
    ]
    cov_a = axes[0][0] * axes[0][0] + axes[0][1] * axes[0][1] + axes[0][2] * axes[0][2] + 0.3
    cov_b = axes[0][0] * axes[1][0] + axes[0][1] * axes[1][1] + axes[0][2] * axes[1][2]
    cov_c = axes[1][0] * axes[1][0] + axes[1][1] * axes[1][1] + axes[1][2] * axes[1][2] + 0.3
    inv_det = 1.0 / (cov_a * cov_c - cov_b * cov_b)
    centers = [
        8.0
        + 7.0 * jnp.sin((cam[s][0] * pos[0] + cam[s][1] * pos[1] + cam[s][2] * pos[2]) / 3.0)
        for s in range(2)
    ]
    off = [pos[k] - cam[2][k] for k in range(3)]
    inv_dist = 1.0 / jnp.sqrt(off[0] * off[0] + off[1] * off[1] + off[2] * off[2])
    basis = harmonic_basis(off[0] * inv_dist, off[1] * inv_dist, off[2] * inv_dist)
    colours = []
    for c in range(3):
        total = 0.5 + basis[0] * rows[11 + 16 * c]
        for m in range(1, 16):
            total = total + basis[m] * rows[11 + 16 * c + m]
        colours.append(total)
    return centers + [cov_c * inv_det, -cov_b * inv_det, cov_a * inv_det] + colours


def read_camera(cam):
    return [[cam[s, k] for k in range(3)] for s in range(3)]


def spread_rows(attr, arows):
    def step(ct, carry):
        lanes = pl.ds(pl.multiple_of(ct * 128, 128), 128)
        for g in range(8):
            n = min(8, ATTRS - 8 * g)
            arows[pl.ds(pl.multiple_of(g * 512 + ct * 8, 8), n), :] = attr[8 * g : 8 * g + n, lanes]
        return carry

    lax.fori_loop(0, 64, step, 0)


def attr_rows(h):
    return [pl.ds((r // 8) * 512 + h * 64 + r % 8, 8, stride=8) for r in range(ATTRS)]


def wrap(value, count):
    return jnp.where(value >= count, value - count, value)


def ring_distance(d):
    return min(d, 4 - d)


STEPS = sorted(
    ((dy, dz) for dy in range(4) for dz in range(4)),
    key=lambda s: ring_distance(s[0]) + ring_distance(s[1]),
)


def pick(index, values):
    found = values[0]
    for n in range(1, len(values)):
        found = jnp.where(index == n, values[n], found)
    return found


class Place:
    def __init__(self, img, cell):
        self.y, self.z = lax.div(img, 2), lax.div(cell, 4)
        core, x = img - self.y * 2, cell - self.z * 4
        self.cores = [core, 1 - core]
        self.xs = [wrap(x + dx, 4) if dx else x for dx in range(4)]
        self.x_halves = [lax.div(v, 2) for v in self.xs]

    def devices(self, dy, dz):
        row, column = wrap(self.y + dy, 4) * 2, wrap(self.z + dz, 4)
        found = []
        for q in range(8):
            pi = row + self.cores[q % 2]
            found.append((pi, column * 4 + self.xs[q // 2], pi * 8 + column * 2 + self.x_halves[q // 2]))
        return found


def opposite(q):
    return (4 - q // 2) % 4 * 2 + q % 2


def each_step(place, act):
    for dy, dz in reversed(STEPS):
        seen = STEPS.index(((4 - dy) % 4, (4 - dz) % 4))
        for q, (pi, pc, half) in enumerate(place.devices(dy, dz)):
            if (dy, dz, q) != (0, 0, 0):
                act(pi, pc, half, seen * 8 + opposite(q), seen // 2)


def left_half():
    return lax.broadcasted_iota(I32, (8, 128), 1) < 64


def pack_message(values, msg, low_row, high_row):
    left = left_half()
    for i in range(PAIRS):
        a = values[2 * i]
        b = values[2 * i + 1] if 2 * i + 1 < FEATS else a
        msg[low_row(i), :] = jnp.where(left, a, pltpu.roll(b, 64, 1))
        msg[high_row(i), :] = jnp.where(left, pltpu.roll(a, 64, 1), b)


def unpack_message(msg, low_row, high_row):
    left = left_half()
    values = []
    for i in range(PAIRS):
        low, high = msg[low_row(i), :], msg[high_row(i), :]
        values.append(jnp.where(left, low, pltpu.roll(high, 64, 1)))
        if 2 * i + 1 < FEATS:
            values.append(jnp.where(left, pltpu.roll(low, 64, 1), high))
    return values


def one_hot(low):
    return jnp.where(lax.broadcasted_iota(I32, (256, 256), 0) == low, 1.0, 0.0).astype(BF16)


def split_ids(ids):
    high = lax.shift_right_logical(ids, 8)
    return high, ids - lax.shift_left(high, 8)


def row_pair(ref, at):
    both = ref[pl.ds(at, 2), :]
    return jnp.concatenate([both[0:1], both[1:2]], axis=1)


def make_parts(table, parts, thirds):
    for f in range(FEATS):
        rows = slice(32 * f, 32 * f + 32)
        for half in range(2):
            v = table[pl.ds(f * ROWS + half, 32, stride=2), :]
            top = v.astype(BF16)
            v = v - top.astype(F32)
            middle = v.astype(BF16)
            parts[rows, 128 * half : 128 * half + 128] = top
            parts[rows, 256 + 128 * half : 384 + 128 * half] = middle
            if f < EXACT:
                low = (v - middle.astype(F32)).astype(BF16)
                thirds[rows, 128 * half : 128 * half + 128] = low


def gather_blocks(parts, thirds, ids, hots):
    found, fine = [], []
    for hot in hots:
        found.append(
            jnp.dot(
                parts[...], jnp.concatenate([hot] * 2, axis=0), preferred_element_type=F32
            )
        )
        fine.append(jnp.dot(thirds[...], hot, preferred_element_type=F32))
    out = []
    for v, low, block in zip(found, fine, ids):
        mask = lax.broadcasted_iota(I32, (32, 256), 0) == split_ids(block)[0]
        rows = []
        for f in range(FEATS):
            value = v[32 * f : 32 * f + 32]
            if f < EXACT:
                value = value + low[32 * f : 32 * f + 32]
            rows.append(jnp.sum(jnp.where(mask, value, 0.0), axis=0, keepdims=True))
        out.append(rows)
    return out


def scatter_blocks(ids, grads, hots, acc):
    lhs = []
    for block, rows in zip(ids, grads):
        mask = lax.broadcasted_iota(I32, (32, 256), 0) == split_ids(block)[0]
        upper, lower = [], []
        for g in rows:
            top = g.astype(BF16).astype(F32)
            upper.append(jnp.where(mask, top, 0.0).astype(BF16))
            lower.append(jnp.where(mask, g - top, 0.0).astype(BF16))
        lhs.append(jnp.concatenate(upper + lower, axis=0))
    acc[...] += lax.dot_general(
        jnp.concatenate(lhs, axis=1),
        hots,
        (((1,), (1,)), ((), ())),
        preferred_element_type=F32,
    )


def two_parts(v):
    top = v.astype(BF16)
    return top, (v - top.astype(F32)).astype(BF16)


def swap_blocks(z):
    rows = z.shape[0]
    row_at = lax.broadcasted_iota(I32, z.shape, 0)
    lane_at = lax.broadcasted_iota(I32, z.shape, 1)
    for bit in (1, 2, 4, 8):
        row_bit = (row_at // bit) % 2
        lane_bit = (lane_at // (16 * bit)) % 2
        down = pltpu.roll(pltpu.roll(z, rows - bit, 0), 16 * bit, 1)
        up = pltpu.roll(pltpu.roll(z, bit, 0), 256 - 16 * bit, 1)
        z = jnp.where(row_bit == lane_bit, z, jnp.where(row_bit == 0, down, up))
    return z


NORTH, SOUTH, PACK_WEST, PACK_EAST, FROM_WEST, FROM_EAST = 192, 288, 384, 400, 416, 432
FROM_NW, FROM_NE, FROM_SW, FROM_SE, EXT_ROWS = 448, 456, 464, 472, 480
BORDER_ROWS = 256


def pack_columns(ext):
    lane = lax.broadcasted_iota(I32, (8, 128), 1)
    for t in range(2):
        west = jnp.zeros((8, 128), F32)
        east = west
        for k in range(6):
            here = (lane >= 16 * k) & (lane < 16 * k + 16)
            at = t * 48 + 8 * k
            first, last = ext[at : at + 8, :], ext[96 + at : 104 + at, :]
            west = jnp.where(here, pltpu.roll(first, 16 * k, 1) if k else first, west)
            east = jnp.where(here, pltpu.roll(last, 16 * k + 16, 1), east)
        ext[PACK_WEST + 8 * t : PACK_WEST + 8 * t + 8, :] = west
        ext[PACK_EAST + 8 * t : PACK_EAST + 8 * t + 8, :] = east


def border_copies(ext, img, cell, send, recv):
    west, east = jnp.where(cell == 0, N_CELL - 1, cell - 1), wrap(cell + 1, N_CELL)
    north, south = jnp.where(img == 0, N_IMG - 1, img - 1), wrap(img + 1, N_IMG)
    plan = [
        (PACK_WEST, FROM_SE, 8, north, west),
        (PACK_EAST, FROM_SW, 8, north, east),
        (PACK_WEST + 8, FROM_NE, 8, south, west),
        (PACK_EAST + 8, FROM_NW, 8, south, east),
        (PACK_WEST, FROM_EAST, 16, img, west),
        (PACK_EAST, FROM_WEST, 16, img, east),
    ]
    for k in range(2):
        plan.append((96 * k, SOUTH + 48 * k, 48, north, cell))
        plan.append((96 * k + 48, NORTH + 48 * k, 48, south, cell))
    for source, dest, count, to_img, to_cell in plan:
        pltpu.make_async_remote_copy(
            src_ref=ext.at[pl.ds(source, count)],
            dst_ref=ext.at[pl.ds(dest, count)],
            send_sem=send,
            recv_sem=recv,
            device_id=(to_img, to_cell),
            device_id_type=MESH,
        ).start()


def wait_rows(ref, count, sem):
    part = ref.at[pl.ds(0, count)]
    pltpu.make_async_copy(part, part, sem).wait()


def window(ext, img, cell, c, row_block, half):
    lane = lax.broadcasted_iota(I32, (8, 128), 1)
    at = 16 * c + 8 * half
    bases = [NORTH, 0, 48, SOUTH][row_block]
    step = 48 if row_block in (0, 3) else 96
    sides = [
        (FROM_NW, FROM_NE),
        (FROM_WEST, FROM_EAST),
        (FROM_WEST + 8, FROM_EAST + 8),
        (FROM_SW, FROM_SE),
    ][row_block]
    first = pltpu.roll(ext[bases + at : bases + at + 8, :], 64, 1)
    second = pltpu.roll(ext[bases + step + at : bases + step + at + 8, :], 64, 1)
    block = 16 * (2 * c + half)
    left = pltpu.roll(ext[sides[0] : sides[0] + 8, :], (48 - block) % 128, 1)
    right = pltpu.roll(ext[sides[1] : sides[1] + 8, :], (64 - block) % 128, 1)
    keep_left = jnp.where(cell == 0, 64, 48)
    keep_right = jnp.where(cell == N_CELL - 1, 64, 80)
    tiles = [
        jnp.where(lane < 64, jnp.where(lane >= keep_left, left, 0.0), first),
        jnp.where(lane < 64, first, second),
        jnp.where(lane < 64, second, jnp.where(lane < keep_right, right, 0.0)),
    ]
    if row_block == 0:
        tiles = [v * jnp.where(img == 0, 0.0, 1.0) for v in tiles]
    if row_block == 3:
        tiles = [v * jnp.where(img == N_IMG - 1, 0.0, 1.0) for v in tiles]
    return tiles


def blur(ref, start, stride):
    down = []
    for j in range(3):
        at = start + j * stride
        total = TAPS[5] * ref[pl.ds(at + 5, 8), :]
        for o in range(5):
            total = total + TAPS[o] * (ref[pl.ds(at + o, 8), :] + ref[pl.ds(at + 10 - o, 8), :])
        down.append(total)
    v = jnp.concatenate(down, axis=1)
    total = TAPS[5] * v
    for o in range(5):
        d = 5 - o
        total = total + TAPS[o] * (pltpu.roll(v, d, 1) + pltpu.roll(v, 384 - d, 1))
    return total


def ssim_value(mean_render, mean_target, square_render, square_target, cross_term):
    spread_render = square_render - mean_render * mean_render
    spread_target = square_target - mean_target * mean_target
    covariance = cross_term - mean_render * mean_target
    upper = (2.0 * mean_render * mean_target + STAB_ONE) * (2.0 * covariance + STAB_TWO)
    lower = (mean_render * mean_render + mean_target * mean_target + STAB_ONE) * (
        spread_render + spread_target + STAB_TWO
    )
    return upper / lower


def map_row(m, c):
    return (m * 3 + c) * 3 * 64


def step_kernel(
    cam_hbm,
    len_hbm,
    vis_hbm,
    attr_hbm,
    target_hbm,
    lists_hbm,
    out,
    cam_ref,
    len_ref,
    vis,
    target,
    lists,
    attr,
    arows,
    table,
    parts,
    thirds,
    hot_list,
    hot_own,
    ids_in,
    ids_own,
    msg,
    inbox,
    msg_back,
    inbox_back,
    ext_render,
    ext_target,
    entry,
    tri_before,
    tri_after,
    weights,
    ratio,
    tile_rows,
    moments,
    maps,
    coefs,
    blurred,
    acc,
    sems,
    id_sems,
    back_sems,
    load_sems,
):
    img = lax.axis_index("img")
    cell = lax.axis_index("cell")
    me = img * N_CELL + cell

    barrier = pltpu.get_barrier_semaphore()
    place = Place(img, cell)
    each_step(
        place,
        lambda pi, pc, *_: pl.semaphore_signal(
            barrier, 1, device_id=(pi, pc), device_id_type=MESH
        ),
    )
    load_target, load_lists, load_attr, load_cam, load_vis, load_len = loads = [
        pltpu.make_async_copy(source, dest, load_sems.at[n])
        for n, (source, dest) in enumerate(
            (
                (target_hbm, target),
                (lists_hbm, lists),
                (attr_hbm, attr),
                (cam_hbm, cam_ref),
                (vis_hbm, vis),
                (len_hbm, len_ref),
            )
        )
    ]
    for load in loads:
        load.start()

    load_target.wait()
    for k in range(2):
        for t in range(2):
            for c in range(3):
                at = 96 * k + 48 * t + 16 * c
                ext_target[at : at + 16, :] = target[
                    c, 16 * t : 16 * t + 16, 128 * k : 128 * k + 128
                ]
    pack_columns(ext_target)

    load_lists.wait()
    def list_hot(b, carry):
        hot_list[:, pl.ds(pl.multiple_of(b * 256, 256), 256)] = one_hot(
            split_ids(row_pair(lists, b * 2))[1]
        )
        return carry

    lax.fori_loop(0, TILES // 2, list_hot, 0)

    load_cam.wait()
    cam = read_camera(cam_ref)
    load_attr.wait()
    spread_rows(attr, arows)

    def project_step(h, carry):
        rows = [arows[at, :] for at in attr_rows(h)]
        feats = project(rows, cam)
        feats.insert(5, jax.nn.sigmoid(rows[10]))
        for f in range(FEATS):
            table[pl.ds(pl.multiple_of(f * ROWS + h * 8, 8), 8), :] = feats[f]
        return carry

    lax.fori_loop(0, 8, project_step, 0)
    make_parts(table, parts, thirds)

    row_at = lax.broadcasted_iota(I32, (128, 128), 0)
    lane_at = lax.broadcasted_iota(I32, (128, 128), 1)
    before = jnp.where(row_at < lane_at, 1.0, 0.0).astype(BF16)
    after = jnp.where(row_at > lane_at, 1.0, 0.0).astype(BF16)
    for half in range(2):
        tri_before[128 * half : 128 * half + 128, :] = before
        tri_after[128 * half : 128 * half + 128, :] = after

    load_vis.wait()
    load_len.wait()
    pl.semaphore_wait(barrier, DEVICES - 1)

    def send_ids(pi, pc, half, rank, group):
        pltpu.make_async_remote_copy(
            src_ref=vis.at[pl.ds(half, 1)],
            dst_ref=ids_in.at[pl.ds(rank, 1)],
            send_sem=sems.at[0],
            recv_sem=id_sems.at[group],
            device_id=(pi, pc),
            device_id_type=MESH,
        ).start()

    each_step(place, send_ids)
    pltpu.make_async_copy(
        vis.at[pl.ds(me // 2, 1)], ids_in.at[pl.ds(0, 1)], id_sems.at[0]
    ).start()
    border_copies(ext_target, img, cell, sems.at[2], sems.at[3])

    odd = me - (me // 2) * 2
    left = left_half()
    left_row = lax.broadcasted_iota(I32, (1, 128), 1) < 64

    def reply_step(g, carry):
        wait_rows(ids_in, 16, id_sems.at[g])
        at = pl.multiple_of(g * 16, 8)
        first, second = ids_in[pl.ds(at, 8), :], ids_in[pl.ds(at + 8, 8), :]
        even_form = jnp.where(left, first, pltpu.roll(second, 64, 1))
        odd_form = jnp.where(left, pltpu.roll(first, 64, 1), second)
        both = jnp.where(odd == 0, even_form, odd_form)
        ids_own[pl.ds(pl.multiple_of(g * 8, 8), 8), :] = both
        ids = [
            jnp.concatenate([both[2 * n : 2 * n + 1], both[2 * n + 1 : 2 * n + 2]], axis=1)
            for n in range(4)
        ]
        hots = [one_hot(split_ids(v)[1]) for v in ids]
        for n in range(4):
            hot_own[:, pl.ds(pl.multiple_of(g * 1024 + n * 256, 256), 256)] = hots[n]
        got = gather_blocks(parts, thirds, ids, hots)
        for n in range(4):
            for row in range(2):
                d = g * 128 + (2 * n + row) * 8
                for i in range(PAIRS):
                    low = got[n][2 * i][:, 128 * row : 128 * row + 128]
                    high = got[n][min(2 * i + 1, FEATS - 1)][:, 128 * row : 128 * row + 128]
                    msg[pl.ds(d + i, 1), :] = jnp.where(left_row, low, pltpu.roll(high, 64, 1))
                    msg[pl.ds(d + 64 + i, 1), :] = jnp.where(
                        left_row, pltpu.roll(low, 64, 1), high
                    )
        for side in range(2):
            dy = pick(g, [STEPS[2 * n + side][0] for n in range(8)])
            dz = pick(g, [STEPS[2 * n + side][1] for n in range(8)])

            for q, (pi, pc, _) in enumerate(place.devices(dy, dz)):
                copy = pltpu.make_async_remote_copy(
                    src_ref=msg.at[pl.ds(pl.multiple_of(g * 128 + side * 64 + q * 8, 8), PAIRS)],
                    dst_ref=inbox.at[pl.ds(pl.multiple_of(me * 8, 8), PAIRS)],
                    send_sem=sems.at[4],
                    recv_sem=sems.at[5],
                    device_id=(pi, pc),
                    device_id_type=MESH,
                )
                if side == 0 and q == 0:
                    pl.when(g > 0)(copy.start)
                else:
                    copy.start()
        return carry

    lax.fori_loop(0, 8, reply_step, 0)
    own = pl.ds(pl.multiple_of(me * 8, 8), PAIRS)
    inbox[own, :] = msg[0:PAIRS, :]

    wait_rows(ext_target, BORDER_ROWS, sems.at[3])
    for c in range(3):
        for row_block in range(4):
            for half in range(2):
                strips = window(ext_target, img, cell, c, row_block, half)
                for j in range(3):
                    for m, v in ((3, strips[j]), (4, strips[j] * strips[j])):
                        at = map_row(m, c) + 64 * j + 16 * row_block + 8 * half
                        maps[at : at + 8, :] = v

    def target_blur(c, carry):
        for m in range(2):
            for r in range(6):
                at = pl.multiple_of((m * 3 + c) * 48 + 8 * r, 8)
                blurred[pl.ds(at, 8), :] = blur(maps, map_row(3 + m, c) + 6 + 8 * r, 64)
        return carry

    lax.fori_loop(0, 3, target_blur, 0)

    wait_rows(inbox, (DEVICES - 1) * PAIRS, sems.at[5])

    def table_step(h, carry):
        values = unpack_message(
            inbox,
            lambda i: pl.ds(h * 128 + i, 8, stride=16),
            lambda i: pl.ds(h * 128 + 8 + i, 8, stride=16),
        )
        for f in range(FEATS):
            table[pl.ds(pl.multiple_of(f * ROWS + h * 8, 8), 8), :] = values[f]
        return carry

    lax.fori_loop(0, 8, table_step, 0)
    make_parts(table, parts, thirds)

    def list_step(k, carry):
        got = gather_blocks(
            parts,
            thirds,
            [row_pair(lists, k * 16 + 2 * n) for n in range(8)],
            [
                hot_list[:, pl.ds(pl.multiple_of(k * 2048 + n * 256, 256), 256)]
                for n in range(8)
            ],
        )
        for n in range(8):
            for row in range(2):
                for f in range(FEATS):
                    entry[pl.ds(f * TILES + k * 16 + 2 * n + row, 1), :] = got[n][f][
                        :, 128 * row : 128 * row + 128
                    ]
        return carry

    lax.fori_loop(0, 2, list_step, 0)

    def entry_row(f, t):
        return entry[pl.ds(f * TILES + t, 1), :]

    across = lax.broadcasted_iota(I32, (16, 128), 0).astype(F32) + 0.5
    lane_row = lax.broadcasted_iota(I32, (1, 128), 1)

    def spans(tile_row, k):
        return [tile_row * 16 + k * GROUP + n for n in range(GROUP)]

    def pixels_of(t):
        return pl.ds(pl.multiple_of(t * 256, 256), 256)

    for tile_row in range(2):

        def render_step(k, carry, tile_row=tile_row):
            tiles = spans(tile_row, k)
            alphas, sums = [], []
            for n, t in enumerate(tiles):
                alive = lane_row < len_ref[tile_row, k * GROUP + n]
                opacity = jnp.where(alive, entry_row(5, t), 0.0)
                dx = across - entry_row(0, t)
                center_y = entry_row(1, t)
                square_x = (-0.5 * entry_row(2, t)) * dx * dx
                mixed = -entry_row(3, t) * dx
                half_y = -0.5 * entry_row(4, t)
                alpha = []
                for y in range(16):
                    dy = (y + 0.5) - center_y
                    alpha.append(opacity * jnp.exp(square_x + dy * (mixed + half_y * dy)))
                alpha = jnp.concatenate(alpha, axis=0)
                logs = jnp.log(1.0 - alpha)
                sums.append(
                    jnp.dot(
                        jnp.concatenate(two_parts(logs), axis=1),
                        tri_before[...],
                        preferred_element_type=F32,
                    )
                )
                ratio[pixels_of(t), :] = alpha
                alphas.append(alpha)
            products = []
            for n, t in enumerate(tiles):
                weight = jnp.concatenate(two_parts(jnp.exp(sums[n]) * alphas[n]), axis=1)
                weights[pixels_of(t), :] = weight
                colour = [two_parts(entry_row(6 + c, t)) for c in range(3)]
                lhs = jnp.concatenate(
                    [c[part] for part in range(2) for c in colour] + [jnp.zeros((10, 128), BF16)],
                    axis=0,
                )
                products.append(
                    lax.dot_general(
                        jnp.concatenate([lhs, lhs], axis=1),
                        weight,
                        (((1,), (1,)), ((), ())),
                        preferred_element_type=F32,
                    )
                )
            for n in range(GROUP):
                for c in range(3):
                    tile_rows[pl.ds(tile_row * 48 + c * 16 + k * GROUP + n, 1), :] = (
                        products[n][c : c + 1] + products[n][3 + c : 4 + c]
                    )
            return carry

        lax.fori_loop(0, 16 // GROUP, render_step, 0)

    picture = swap_blocks(tile_rows[...])
    for k in range(2):
        ext_render[96 * k : 96 * k + 96, :] = picture[:, 128 * k : 128 * k + 128]
    pack_columns(ext_render)
    border_copies(ext_render, img, cell, sems.at[6], sems.at[7])

    def ratio_step(t, carry):
        alpha = ratio[pixels_of(t), :]
        ratio[pixels_of(t), :] = alpha / (1.0 - alpha)
        return carry

    lax.fori_loop(0, TILES, ratio_step, 0)
    wait_rows(ext_render, BORDER_ROWS, sems.at[7])

    for c in range(3):
        for row_block in range(4):
            for half in range(2):
                strips = window(ext_render, img, cell, c, row_block, half)
                for j in range(3):
                    at = 64 * j + 16 * row_block + 8 * half
                    v = strips[j]
                    wanted = maps[map_row(3, c) + at : map_row(3, c) + at + 8, :]
                    for m, value in ((0, v), (1, v * v), (2, v * wanted)):
                        maps[map_row(m, c) + at : map_row(m, c) + at + 8, :] = value
    row_at = lax.broadcasted_iota(I32, (8, 384), 0) + (img * 32 - 5)
    lane_at = lax.broadcasted_iota(I32, (8, 384), 1) + (cell * 256 - 64)
    inside = (lane_at >= 0) & (lane_at < N_CELL * 256)

    def similarity_step(c, carry):
        for r in range(6):
            mean, square, cross = [blur(maps, map_row(m, c) + 6 + 8 * r, 64) for m in range(3)]
            mean_target, square_target = [
                blurred[pl.ds(pl.multiple_of((m * 3 + c) * 48 + 8 * r, 8), 8), :]
                for m in range(2)
            ]
            _, pullback = jax.vjp(
                lambda x, y, z, mt=mean_target, st=square_target: ssim_value(x, mt, y, st, z),
                mean,
                square,
                cross,
            )
            keep = inside & (row_at + 8 * r >= 0) & (row_at + 8 * r < N_IMG * 32)
            for m, v in enumerate(pullback(jnp.full((8, 384), -WEIGHT_SSIM, F32))):
                v = jnp.where(keep, v, 0.0)
                for j in range(3):
                    at = pl.multiple_of(((m * 3 + c) * 3 + j) * 48 + 8 * r, 8)
                    coefs[pl.ds(at, 8), :] = v[:, 128 * j : 128 * j + 128]
        return carry

    lax.fori_loop(0, 3, similarity_step, 0)
    left = left_half()

    def image_step(c, carry):
        for r in range(4):
            back_mean, back_square, back_cross = [
                blur(coefs, (m * 3 + c) * 3 * 48 + 8 * r, 48) for m in range(3)
            ]
            found = []
            for j in range(3):
                lanes = slice(128 * j, 128 * j + 128)
                at = 64 * j + 16 + 8 * r
                image = maps[pl.ds(pl.multiple_of(map_row(0, c) + at, 8), 8), :]
                wanted = maps[pl.ds(pl.multiple_of(map_row(3, c) + at, 8), 8), :]
                difference = image - wanted
                slope = (
                    (1.0 - WEIGHT_SSIM)
                    * difference
                    / jnp.sqrt(difference * difference + SMOOTHING * SMOOTHING)
                )
                found.append(
                    pltpu.roll(
                        slope
                        + back_mean[:, lanes]
                        + 2.0 * image * back_square[:, lanes]
                        + wanted * back_cross[:, lanes],
                        64,
                        1,
                    )
                )
            at = pl.multiple_of((r // 2) * 48 + c * 16 + (r % 2) * 8, 8)
            tile_rows[pl.ds(at, 8), :] = jnp.concatenate(
                [jnp.where(left, found[0], found[1]), jnp.where(left, found[1], found[2])],
                axis=1,
            )
        return carry

    lax.fori_loop(0, 3, image_step, 0)
    tile_rows[...] = swap_blocks(tile_rows[...])

    for tile_row in range(2):

        def back_step(k, carry, tile_row=tile_row):
            tiles = spans(tile_row, k)
            grad_rows, values = [], []
            for n, t in enumerate(tiles):
                pixel_grad = [
                    two_parts(tile_rows[pl.ds(tile_row * 48 + c * 16 + k * GROUP + n, 1), :])
                    for c in range(3)
                ]
                colour = [two_parts(entry_row(6 + c, t)) for c in range(3)]
                tops, lows = [g[0] for g in pixel_grad], [g[1] for g in pixel_grad]
                grad_rows.append(
                    jnp.concatenate(tops + lows + tops + [jnp.zeros((7, 256), BF16)], axis=0)
                )
                colour_rows = jnp.concatenate(
                    [c[0] for c in colour] * 2
                    + [c[1] for c in colour]
                    + [jnp.zeros((7, 128), BF16)],
                    axis=0,
                )
                values.append(
                    lax.dot_general(
                        grad_rows[n],
                        colour_rows,
                        (((0,), (0,)), ((), ())),
                        preferred_element_type=F32,
                    )
                )
            gains, laters, mixes = [], [], []
            for n, t in enumerate(tiles):
                weight = weights[pixels_of(t), :]
                mixes.append(jnp.dot(grad_rows[n], weight, preferred_element_type=F32))
                gain = values[n] * (weight[:, :128].astype(F32) + weight[:, 128:].astype(F32))
                laters.append(
                    jnp.dot(
                        jnp.concatenate(two_parts(gain), axis=1),
                        tri_after[...],
                        preferred_element_type=F32,
                    )
                )
                gains.append(gain)
            for n, t in enumerate(tiles):
                pull = gains[n] - ratio[pixels_of(t), :] * laters[n]
                dx = across - entry_row(0, t)
                center_y = entry_row(1, t)
                sum_0 = sum_y = sum_yy = None
                for y in range(16):
                    dy = (y + 0.5) - center_y
                    part = pull[16 * y : 16 * y + 16]
                    part_y = part * dy
                    part_yy = part_y * dy
                    sum_0 = part if y == 0 else sum_0 + part
                    sum_y = part_y if y == 0 else sum_y + part_y
                    sum_yy = part_yy if y == 0 else sum_yy + part_yy
                sum_x = sum_0 * dx
                found = [sum_0, sum_x, sum_y, sum_x * dx, sum_y * dx, sum_yy]
                for m in range(6):
                    moments[pl.ds(m * TILES + t, 1), :] = jnp.sum(
                        found[m], axis=0, keepdims=True
                    )
                for c in range(3):
                    both = mixes[n][c : c + 1] + mixes[n][3 + c : 4 + c]
                    moments[pl.ds((6 + c) * TILES + t, 1), :] = both[:, :128] + both[:, 128:]
            return carry

        lax.fori_loop(0, 16 // GROUP, back_step, 0)

    feat = [entry[f * TILES : (f + 1) * TILES, :] for f in range(6)]
    mom = [moments[m * TILES : (m + 1) * TILES, :] for m in range(6)]
    entry[0:TILES, :] = feat[2] * mom[1] + feat[3] * mom[2]
    entry[TILES : 2 * TILES, :] = feat[3] * mom[1] + feat[4] * mom[2]
    entry[2 * TILES : 3 * TILES, :] = -0.5 * mom[3]
    entry[3 * TILES : 4 * TILES, :] = -mom[4]
    entry[4 * TILES : 5 * TILES, :] = -0.5 * mom[5]
    entry[5 * TILES : 6 * TILES, :] = mom[0]
    entry[6 * TILES : 9 * TILES, :] = moments[6 * TILES : 9 * TILES, :]

    acc[...] = jnp.zeros_like(acc)

    def slot_step(k, carry):
        at = [k * 2 * BLOCKS + 2 * n for n in range(BLOCKS)]
        scatter_blocks(
            [row_pair(lists, a) for a in at],
            [[row_pair(entry, f * TILES + a) for f in range(FEATS)] for a in at],
            hot_list[:, pl.ds(pl.multiple_of(k * 256 * BLOCKS, 256), 256 * BLOCKS)],
            acc,
        )
        return carry

    lax.fori_loop(0, TILES // (2 * BLOCKS), slot_step, 0)

    def total_rows(f, h):
        a = acc[pl.ds(pl.multiple_of(f * 32 + h * 8, 8), 8), :]
        b = acc[pl.ds(pl.multiple_of(288 + f * 32 + h * 8, 8), 8), :]
        return a + b

    def back_pack(h, carry):
        totals = [total_rows(f, h) for f in range(FEATS)]
        for half in range(2):
            pack_message(
                [v[:, 128 * half : 128 * half + 128] for v in totals],
                msg_back,
                lambda i: pl.ds(h * 256 + (2 * half) * 8 + i, 8, stride=32),
                lambda i: pl.ds(h * 256 + (2 * half + 1) * 8 + i, 8, stride=32),
            )
        return carry

    lax.fori_loop(0, 4, back_pack, 0)

    def send_back(pi, pc, half, rank, group):
        pltpu.make_async_remote_copy(
            src_ref=msg_back.at[pl.ds(pl.multiple_of((pi * N_CELL + pc) * 8, 8), PAIRS)],
            dst_ref=inbox_back.at[pl.ds(pl.multiple_of(rank * 8, 8), PAIRS)],
            send_sem=sems.at[8],
            recv_sem=back_sems.at[group],
            device_id=(pi, pc),
            device_id_type=MESH,
        ).start()

    each_step(place, send_back)
    pltpu.make_async_copy(
        msg_back.at[own], inbox_back.at[pl.ds(0, PAIRS)], back_sems.at[0]
    ).start()

    acc[...] = jnp.zeros_like(acc)

    def owner_step(k, carry):
        for side in range(BLOCKS // 4):
            g = k * (BLOCKS // 4) + side
            wait_rows(inbox_back, 16 * PAIRS, back_sems.at[g])
            values = unpack_message(
                inbox_back,
                lambda i: pl.ds(g * 128 + i, 8, stride=8),
                lambda i: pl.ds(g * 128 + 64 + i, 8, stride=8),
            )
            for f in range(FEATS):
                table[pl.ds(pl.multiple_of(f * ROWS + g * 8, 8), 8), :] = values[f]
        at = [k * 2 * BLOCKS + 2 * n for n in range(BLOCKS)]
        scatter_blocks(
            [row_pair(ids_own, a) for a in at],
            [[row_pair(table, f * ROWS + a) for f in range(FEATS)] for a in at],
            hot_own[:, pl.ds(pl.multiple_of(k * 256 * BLOCKS, 256), 256 * BLOCKS)],
            acc,
        )
        return carry

    lax.fori_loop(0, ROWS // (2 * BLOCKS), owner_step, 0)

    def finish(h, carry):
        for f in range(FEATS):
            v = total_rows(f, h)
            for half in range(2):
                out[pl.ds(f * ROWS + h * 16 + half, 8, stride=2), :] = v[
                    :, 128 * half : 128 * half + 128
                ]
        return carry

    lax.fori_loop(0, 4, finish, 0)

    wait_rows(ids_in, DEVICES - 1, sems.at[0])
    wait_rows(ext_target, BORDER_ROWS, sems.at[2])
    wait_rows(msg, (DEVICES - 1) * PAIRS, sems.at[4])
    wait_rows(ext_render, BORDER_ROWS, sems.at[6])
    wait_rows(msg_back, (DEVICES - 1) * PAIRS, sems.at[8])


def pullback_kernel(
    cam_hbm,
    attr_hbm,
    grad_hbm,
    out_hbm,
    cam_ref,
    attr,
    feat_grad,
    arows,
    result,
    load_sems,
    save_sem,
):
    def block(h):
        return pl.ds(pl.multiple_of(h * 1024, 1024), 1024)

    def load(h):
        return pltpu.make_async_copy(
            attr_hbm.at[:, block(h)], attr.at[:, block(h)], load_sems.at[h]
        )

    load_cam = pltpu.make_async_copy(cam_hbm, cam_ref, load_sems.at[8])
    load_grad = pltpu.make_async_copy(grad_hbm, feat_grad, load_sems.at[9])
    load(0).start()
    load_cam.start()
    load_grad.start()
    for h in range(1, 8):
        load(h).start()
    load_cam.wait()
    load_grad.wait()
    cam = read_camera(cam_ref)

    def step(h, carry):
        load(h).wait()
        for k in range(8):
            lanes = pl.ds(pl.multiple_of(h * 1024 + k * 128, 128), 128)
            for g in range(8):
                n = min(8, ATTRS - 8 * g)
                arows[g * 64 + 8 * k : g * 64 + 8 * k + n, :] = attr[8 * g : 8 * g + n, lanes]
        places = [pl.ds((r // 8) * 64 + r % 8, 8, stride=8) for r in range(ATTRS)]
        rows = [arows[at, :] for at in places]
        _, pullback = jax.vjp(lambda r: project(r, cam), rows)
        grads = [
            feat_grad[pl.ds(pl.multiple_of(f * ROWS + h * 8, 8), 8), :] for f in range(FEATS)
        ]
        log_opacity = grads.pop(5)
        (found,) = pullback(grads)
        found[10] = log_opacity * (1.0 - jax.nn.sigmoid(rows[10]))
        for at, v in zip(places, found):
            arows[at, :] = v
        for k in range(8):
            lanes = pl.ds(pl.multiple_of(h * 1024 + k * 128, 128), 128)
            for g in range(8):
                n = min(8, ATTRS - 8 * g)
                result[8 * g : 8 * g + n, lanes] = arows[g * 64 + 8 * k : g * 64 + 8 * k + n, :]
        pltpu.make_async_copy(result.at[:, block(h)], out_hbm.at[:, block(h)], save_sem).start()
        return carry

    lax.fori_loop(0, 8, step, 0)
    pltpu.make_async_copy(result, out_hbm, save_sem).wait()


def shards(attributes, camera, target, visible_index, tile_lists, tile_len):
    vmem = pl.BlockSpec(memory_space=pltpu.VMEM)
    anywhere = pl.BlockSpec(memory_space=pl.ANY)
    feat_grad = pl.pallas_call(
        step_kernel,
        out_shape=jax.ShapeDtypeStruct((FEATS * ROWS, 128), F32),
        in_specs=[anywhere] * 6,
        out_specs=vmem,
        scratch_shapes=[
            pltpu.SMEM((3, 3), F32),
            pltpu.SMEM((2, 16), I32),
            pltpu.VMEM((ROWS, 128), I32),
            pltpu.VMEM((3, 32, 256), F32),
            pltpu.VMEM((TILES, LIST), I32),
            pltpu.VMEM((ATTRS, 8192), F32),
            pltpu.VMEM((4096, 128), F32),
            pltpu.VMEM((FEATS * ROWS, 128), F32),
            pltpu.VMEM((FEATS * 32, 512), BF16),
            pltpu.VMEM((EXACT * 32, 256), BF16),
            pltpu.VMEM((256, TILES * LIST), BF16),
            pltpu.VMEM((256, ROWS * 128), BF16),
            pltpu.VMEM((DEVICES, 128), I32),
            pltpu.VMEM((ROWS, 128), I32),
            pltpu.VMEM((DEVICES * 8, 128), F32),
            pltpu.VMEM((DEVICES * 8, 128), F32),
            pltpu.VMEM((DEVICES * 8, 128), F32),
            pltpu.VMEM((DEVICES * 8, 128), F32),
            pltpu.VMEM((EXT_ROWS, 128), F32),
            pltpu.VMEM((EXT_ROWS, 128), F32),
            pltpu.VMEM((FEATS * TILES, 128), F32),
            pltpu.VMEM((256, 128), BF16),
            pltpu.VMEM((256, 128), BF16),
            pltpu.VMEM((TILES * 256, 256), BF16),
            pltpu.VMEM((TILES * 256, 128), F32),
            pltpu.VMEM((96, 256), F32),
            pltpu.VMEM((FEATS * TILES, 128), F32),
            pltpu.VMEM((5 * 3 * 3 * 64, 128), F32),
            pltpu.VMEM((3 * 3 * 3 * 48, 128), F32),
            pltpu.VMEM((2 * 3 * 48, 384), F32),
            pltpu.VMEM((2 * FEATS * 32, 256), F32),
            pltpu.SemaphoreType.DMA((10,)),
            pltpu.SemaphoreType.DMA((8,)),
            pltpu.SemaphoreType.DMA((8,)),
            pltpu.SemaphoreType.DMA((6,)),
        ],
        compiler_params=pltpu.CompilerParams(
            collective_id=0, has_side_effects=True, vmem_limit_bytes=58 * 1024 * 1024
        ),
        name="splat_step",
    )(
        camera,
        tile_len,
        visible_index.reshape(ROWS, 128),
        attributes,
        target,
        tile_lists.reshape(TILES, LIST),
    )
    return pl.pallas_call(
        pullback_kernel,
        out_shape=jax.ShapeDtypeStruct(attributes.shape, F32),
        in_specs=[anywhere] * 3,
        out_specs=anywhere,
        scratch_shapes=[
            pltpu.SMEM((3, 3), F32),
            pltpu.VMEM((ATTRS, 8192), F32),
            pltpu.VMEM((FEATS * ROWS, 128), F32),
            pltpu.VMEM((512, 128), F32),
            pltpu.VMEM((ATTRS, 8192), F32),
            pltpu.SemaphoreType.DMA((10,)),
            pltpu.SemaphoreType.DMA,
        ],
        name="splat_pullback",
    )(camera, attributes, feat_grad)


def solution(mesh):
    return jax.shard_map(
        shards,
        mesh=mesh,
        in_specs=(
            P(None, ("img", "cell")),
            P(),
            P(None, "img", "cell"),
            P(("img", "cell"), None),
            P("img", "cell", None),
            P("img", "cell"),
        ),
        out_specs=P(None, ("img", "cell")),
        check_vma=False,
    )
```

```python
import math

import jax
import jax.numpy as jnp
from jax import lax
from jax.experimental import pallas as pl
from jax.experimental.pallas import tpu as pltpu
from jax.sharding import PartitionSpec as P

F32 = jnp.float32
BF16 = jnp.bfloat16
I32 = jnp.int32
MESH = pl.DeviceIdType.MESH

TILE = 16
N_IMG = 8
N_CELL = 16
DEVICES = 128
LIST = 128
TILES = 32
ATTRS = 59
ROWS = 64
FEATS = 9
PAIRS = 5
EXACT = 5
BLOCKS = 8
GROUP = 8

WEIGHT_SSIM = 0.2
SMOOTHING = 0.01
STAB_ONE = 0.0001
STAB_TWO = 0.0009
BLUR_SIGMA = 1.5
SH_ZERO = 0.28209479177387814
SH_ONE = 0.4886025119029199
SH_TWO = (
    1.0925484305920792,
    -1.0925484305920792,
    0.31539156525252005,
    -1.0925484305920792,
    0.5462742152960396,
)
SH_THREE = (
    -0.5900435899266435,
    2.890611442640554,
    -0.4570457994644658,
    0.3731763325901154,
    -0.4570457994644658,
    1.445305721320277,
    -0.5900435899266435,
)


def blur_taps():
    raw = [math.exp(-((o - 5.0) ** 2) / (2.0 * BLUR_SIGMA * BLUR_SIGMA)) for o in range(11)]
    return [r / sum(raw) for r in raw]


TAPS = blur_taps()


def harmonic_basis(ux, uy, uz):
    xx, yy, zz = ux * ux, uy * uy, uz * uz
    return [
        SH_ZERO,
        -SH_ONE * uy,
        SH_ONE * uz,
        -SH_ONE * ux,
        SH_TWO[0] * ux * uy,
        SH_TWO[1] * uy * uz,
        SH_TWO[2] * (2.0 * zz - xx - yy),
        SH_TWO[3] * ux * uz,
        SH_TWO[4] * (xx - yy),
        SH_THREE[0] * uy * (3.0 * xx - yy),
        SH_THREE[1] * ux * uy * uz,
        SH_THREE[2] * uy * (4.0 * zz - xx - yy),
        SH_THREE[3] * uz * (2.0 * zz - 3.0 * xx - 3.0 * yy),
        SH_THREE[4] * ux * (4.0 * zz - xx - yy),
        SH_THREE[5] * uz * (xx - yy),
        SH_THREE[6] * ux * (xx - 3.0 * yy),
    ]


def project(rows, cam):
    pos = rows[0:3]
    scales = [jnp.exp(r) for r in rows[3:6]]
    qw = 1.5 + jnp.tanh(rows[6])
    qx, qy, qz = rows[7:10]
    inv = 1.0 / jnp.sqrt(qw * qw + qx * qx + qy * qy + qz * qz)
    qw, qx, qy, qz = qw * inv, qx * inv, qy * inv, qz * inv
    rot = [
        [1.0 - 2.0 * (qy * qy + qz * qz), 2.0 * (qx * qy - qw * qz), 2.0 * (qx * qz + qw * qy)],
        [2.0 * (qx * qy + qw * qz), 1.0 - 2.0 * (qx * qx + qz * qz), 2.0 * (qy * qz - qw * qx)],
        [2.0 * (qx * qz - qw * qy), 2.0 * (qy * qz + qw * qx), 1.0 - 2.0 * (qx * qx + qy * qy)],
    ]
    axes = [
        [
            (cam[s][0] * rot[0][k] + cam[s][1] * rot[1][k] + cam[s][2] * rot[2][k]) * scales[k]
            for k in range(3)
        ]
        for s in range(2)
    ]
    cov_a = axes[0][0] * axes[0][0] + axes[0][1] * axes[0][1] + axes[0][2] * axes[0][2] + 0.3
    cov_b = axes[0][0] * axes[1][0] + axes[0][1] * axes[1][1] + axes[0][2] * axes[1][2]
    cov_c = axes[1][0] * axes[1][0] + axes[1][1] * axes[1][1] + axes[1][2] * axes[1][2] + 0.3
    inv_det = 1.0 / (cov_a * cov_c - cov_b * cov_b)
    centers = [
        8.0
        + 7.0 * jnp.sin((cam[s][0] * pos[0] + cam[s][1] * pos[1] + cam[s][2] * pos[2]) / 3.0)
        for s in range(2)
    ]
    off = [pos[k] - cam[2][k] for k in range(3)]
    inv_dist = 1.0 / jnp.sqrt(off[0] * off[0] + off[1] * off[1] + off[2] * off[2])
    basis = harmonic_basis(off[0] * inv_dist, off[1] * inv_dist, off[2] * inv_dist)
    colours = []
    for c in range(3):
        total = 0.5 + basis[0] * rows[11 + 16 * c]
        for m in range(1, 16):
            total = total + basis[m] * rows[11 + 16 * c + m]
        colours.append(total)
    return centers + [cov_c * inv_det, -cov_b * inv_det, cov_a * inv_det] + colours


def read_camera(cam):
    return [[cam[s, k] for k in range(3)] for s in range(3)]


def spread_rows(attr, arows):
    def step(ct, carry):
        lanes = pl.ds(pl.multiple_of(ct * 128, 128), 128)
        for g in range(8):
            n = min(8, ATTRS - 8 * g)
            arows[pl.ds(pl.multiple_of(g * 512 + ct * 8, 8), n), :] = attr[8 * g : 8 * g + n, lanes]
        return carry

    lax.fori_loop(0, 64, step, 0)


def attr_rows(h):
    return [pl.ds((r // 8) * 512 + h * 64 + r % 8, 8, stride=8) for r in range(ATTRS)]


def wrap(value, count):
    return jnp.where(value >= count, value - count, value)


def ring_distance(d):
    return min(d, 4 - d)


STEPS = sorted(
    ((dy, dz) for dy in range(4) for dz in range(4)),
    key=lambda s: ring_distance(s[0]) + ring_distance(s[1]),
)


def pick(index, values):
    found = values[0]
    for n in range(1, len(values)):
        found = jnp.where(index == n, values[n], found)
    return found


class Place:
    def __init__(self, img, cell):
        self.y, self.z = lax.div(img, 2), lax.div(cell, 4)
        core, x = img - self.y * 2, cell - self.z * 4
        self.cores = [core, 1 - core]
        self.xs = [wrap(x + dx, 4) if dx else x for dx in range(4)]
        self.x_halves = [lax.div(v, 2) for v in self.xs]

    def devices(self, dy, dz):
        row, column = wrap(self.y + dy, 4) * 2, wrap(self.z + dz, 4)
        found = []
        for q in range(8):
            pi = row + self.cores[q % 2]
            found.append((pi, column * 4 + self.xs[q // 2], pi * 8 + column * 2 + self.x_halves[q // 2]))
        return found


def opposite(q):
    return (4 - q // 2) % 4 * 2 + q % 2


def each_step(place, act):
    for dy, dz in reversed(STEPS):
        seen = STEPS.index(((4 - dy) % 4, (4 - dz) % 4))
        for q, (pi, pc, half) in enumerate(place.devices(dy, dz)):
            if (dy, dz, q) != (0, 0, 0):
                act(pi, pc, half, seen * 8 + opposite(q), seen // 2)


def left_half():
    return lax.broadcasted_iota(I32, (8, 128), 1) < 64


def pack_message(values, msg, low_row, high_row):
    left = left_half()
    for i in range(PAIRS):
        a = values[2 * i]
        b = values[2 * i + 1] if 2 * i + 1 < FEATS else a
        msg[low_row(i), :] = jnp.where(left, a, pltpu.roll(b, 64, 1))
        msg[high_row(i), :] = jnp.where(left, pltpu.roll(a, 64, 1), b)


def unpack_message(msg, low_row, high_row):
    left = left_half()
    values = []
    for i in range(PAIRS):
        low, high = msg[low_row(i), :], msg[high_row(i), :]
        values.append(jnp.where(left, low, pltpu.roll(high, 64, 1)))
        if 2 * i + 1 < FEATS:
            values.append(jnp.where(left, pltpu.roll(low, 64, 1), high))
    return values


def one_hot(low):
    return jnp.where(lax.broadcasted_iota(I32, (256, 256), 0) == low, 1.0, 0.0).astype(BF16)


def split_ids(ids):
    high = lax.shift_right_logical(ids, 8)
    return high, ids - lax.shift_left(high, 8)


def row_pair(ref, at):
    both = ref[pl.ds(at, 2), :]
    return jnp.concatenate([both[0:1], both[1:2]], axis=1)


def make_parts(table, parts, thirds):
    for f in range(FEATS):
        rows = slice(32 * f, 32 * f + 32)
        for half in range(2):
            v = table[pl.ds(f * ROWS + half, 32, stride=2), :]
            top = v.astype(BF16)
            v = v - top.astype(F32)
            middle = v.astype(BF16)
            parts[rows, 128 * half : 128 * half + 128] = top
            parts[rows, 256 + 128 * half : 384 + 128 * half] = middle
            if f < EXACT:
                low = (v - middle.astype(F32)).astype(BF16)
                thirds[rows, 128 * half : 128 * half + 128] = low


def gather_blocks(parts, thirds, ids, hots):
    found, fine = [], []
    for hot in hots:
        found.append(
            jnp.dot(
                parts[...], jnp.concatenate([hot] * 2, axis=0), preferred_element_type=F32
            )
        )
        fine.append(jnp.dot(thirds[...], hot, preferred_element_type=F32))
    out = []
    for v, low, block in zip(found, fine, ids):
        mask = lax.broadcasted_iota(I32, (32, 256), 0) == split_ids(block)[0]
        rows = []
        for f in range(FEATS):
            value = v[32 * f : 32 * f + 32]
            if f < EXACT:
                value = value + low[32 * f : 32 * f + 32]
            rows.append(jnp.sum(jnp.where(mask, value, 0.0), axis=0, keepdims=True))
        out.append(rows)
    return out


def scatter_blocks(ids, grads, hots, acc):
    lhs = []
    for block, rows in zip(ids, grads):
        mask = lax.broadcasted_iota(I32, (32, 256), 0) == split_ids(block)[0]
        upper, lower = [], []
        for g in rows:
            top = g.astype(BF16).astype(F32)
            upper.append(jnp.where(mask, top, 0.0).astype(BF16))
            lower.append(jnp.where(mask, g - top, 0.0).astype(BF16))
        lhs.append(jnp.concatenate(upper + lower, axis=0))
    acc[...] += lax.dot_general(
        jnp.concatenate(lhs, axis=1),
        hots,
        (((1,), (1,)), ((), ())),
        preferred_element_type=F32,
    )


def two_parts(v):
    top = v.astype(BF16)
    return top, (v - top.astype(F32)).astype(BF16)


def swap_blocks(z):
    rows = z.shape[0]
    row_at = lax.broadcasted_iota(I32, z.shape, 0)
    lane_at = lax.broadcasted_iota(I32, z.shape, 1)
    for bit in (1, 2, 4, 8):
        row_bit = (row_at // bit) % 2
        lane_bit = (lane_at // (16 * bit)) % 2
        down = pltpu.roll(pltpu.roll(z, rows - bit, 0), 16 * bit, 1)
        up = pltpu.roll(pltpu.roll(z, bit, 0), 256 - 16 * bit, 1)
        z = jnp.where(row_bit == lane_bit, z, jnp.where(row_bit == 0, down, up))
    return z


NORTH, SOUTH, PACK_WEST, PACK_EAST, FROM_WEST, FROM_EAST = 192, 288, 384, 400, 416, 432
FROM_NW, FROM_NE, FROM_SW, FROM_SE, EXT_ROWS = 448, 456, 464, 472, 480
BORDER_ROWS = 256


def pack_columns(ext):
    lane = lax.broadcasted_iota(I32, (8, 128), 1)
    for t in range(2):
        west = jnp.zeros((8, 128), F32)
        east = west
        for k in range(6):
            here = (lane >= 16 * k) & (lane < 16 * k + 16)
            at = t * 48 + 8 * k
            first, last = ext[at : at + 8, :], ext[96 + at : 104 + at, :]
            west = jnp.where(here, pltpu.roll(first, 16 * k, 1) if k else first, west)
            east = jnp.where(here, pltpu.roll(last, 16 * k + 16, 1), east)
        ext[PACK_WEST + 8 * t : PACK_WEST + 8 * t + 8, :] = west
        ext[PACK_EAST + 8 * t : PACK_EAST + 8 * t + 8, :] = east


def border_copies(ext, img, cell, send, recv):
    west, east = jnp.where(cell == 0, N_CELL - 1, cell - 1), wrap(cell + 1, N_CELL)
    north, south = jnp.where(img == 0, N_IMG - 1, img - 1), wrap(img + 1, N_IMG)
    plan = [
        (PACK_WEST, FROM_SE, 8, north, west),
        (PACK_EAST, FROM_SW, 8, north, east),
        (PACK_WEST + 8, FROM_NE, 8, south, west),
        (PACK_EAST + 8, FROM_NW, 8, south, east),
        (PACK_WEST, FROM_EAST, 16, img, west),
        (PACK_EAST, FROM_WEST, 16, img, east),
    ]
    for k in range(2):
        plan.append((96 * k, SOUTH + 48 * k, 48, north, cell))
        plan.append((96 * k + 48, NORTH + 48 * k, 48, south, cell))
    for source, dest, count, to_img, to_cell in plan:
        pltpu.make_async_remote_copy(
            src_ref=ext.at[pl.ds(source, count)],
            dst_ref=ext.at[pl.ds(dest, count)],
            send_sem=send,
            recv_sem=recv,
            device_id=(to_img, to_cell),
            device_id_type=MESH,
        ).start()


def wait_rows(ref, count, sem):
    part = ref.at[pl.ds(0, count)]
    pltpu.make_async_copy(part, part, sem).wait()


def window(ext, img, cell, c, row_block, half):
    lane = lax.broadcasted_iota(I32, (8, 128), 1)
    at = 16 * c + 8 * half
    bases = [NORTH, 0, 48, SOUTH][row_block]
    step = 48 if row_block in (0, 3) else 96
    sides = [
        (FROM_NW, FROM_NE),
        (FROM_WEST, FROM_EAST),
        (FROM_WEST + 8, FROM_EAST + 8),
        (FROM_SW, FROM_SE),
    ][row_block]
    first = pltpu.roll(ext[bases + at : bases + at + 8, :], 64, 1)
    second = pltpu.roll(ext[bases + step + at : bases + step + at + 8, :], 64, 1)
    block = 16 * (2 * c + half)
    left = pltpu.roll(ext[sides[0] : sides[0] + 8, :], (48 - block) % 128, 1)
    right = pltpu.roll(ext[sides[1] : sides[1] + 8, :], (64 - block) % 128, 1)
    keep_left = jnp.where(cell == 0, 64, 48)
    keep_right = jnp.where(cell == N_CELL - 1, 64, 80)
    tiles = [
        jnp.where(lane < 64, jnp.where(lane >= keep_left, left, 0.0), first),
        jnp.where(lane < 64, first, second),
        jnp.where(lane < 64, second, jnp.where(lane < keep_right, right, 0.0)),
    ]
    if row_block == 0:
        tiles = [v * jnp.where(img == 0, 0.0, 1.0) for v in tiles]
    if row_block == 3:
        tiles = [v * jnp.where(img == N_IMG - 1, 0.0, 1.0) for v in tiles]
    return tiles


def blur(ref, start, stride):
    down = []
    for j in range(3):
        at = start + j * stride
        total = TAPS[5] * ref[pl.ds(at + 5, 8), :]
        for o in range(5):
            total = total + TAPS[o] * (ref[pl.ds(at + o, 8), :] + ref[pl.ds(at + 10 - o, 8), :])
        down.append(total)
    v = jnp.concatenate(down, axis=1)
    total = TAPS[5] * v
    for o in range(5):
        d = 5 - o
        total = total + TAPS[o] * (pltpu.roll(v, d, 1) + pltpu.roll(v, 384 - d, 1))
    return total


def ssim_value(mean_render, mean_target, square_render, square_target, cross_term):
    spread_render = square_render - mean_render * mean_render
    spread_target = square_target - mean_target * mean_target
    covariance = cross_term - mean_render * mean_target
    upper = (2.0 * mean_render * mean_target + STAB_ONE) * (2.0 * covariance + STAB_TWO)
    lower = (mean_render * mean_render + mean_target * mean_target + STAB_ONE) * (
        spread_render + spread_target + STAB_TWO
    )
    return upper / lower


def map_row(m, c):
    return (m * 3 + c) * 3 * 64


def step_kernel(
    cam_hbm,
    len_hbm,
    vis_hbm,
    attr_hbm,
    target_hbm,
    lists_hbm,
    out,
    cam_ref,
    len_ref,
    vis,
    target,
    lists,
    attr,
    arows,
    table,
    parts,
    thirds,
    hot_list,
    hot_own,
    ids_in,
    ids_own,
    msg,
    inbox,
    msg_back,
    inbox_back,
    ext_render,
    ext_target,
    entry,
    tri_before,
    tri_after,
    weights,
    ratio,
    tile_rows,
    moments,
    maps,
    coefs,
    blurred,
    acc,
    sems,
    id_sems,
    back_sems,
    load_sems,
):
    img = lax.axis_index("img")
    cell = lax.axis_index("cell")
    me = img * N_CELL + cell

    barrier = pltpu.get_barrier_semaphore()
    place = Place(img, cell)
    each_step(
        place,
        lambda pi, pc, *_: pl.semaphore_signal(
            barrier, 1, device_id=(pi, pc), device_id_type=MESH
        ),
    )
    load_target, load_lists, load_attr, load_cam, load_vis, load_len = loads = [
        pltpu.make_async_copy(source, dest, load_sems.at[n])
        for n, (source, dest) in enumerate(
            (
                (target_hbm, target),
                (lists_hbm, lists),
                (attr_hbm, attr),
                (cam_hbm, cam_ref),
                (vis_hbm, vis),
                (len_hbm, len_ref),
            )
        )
    ]
    for load in loads:
        load.start()

    load_target.wait()
    for k in range(2):
        for t in range(2):
            for c in range(3):
                at = 96 * k + 48 * t + 16 * c
                ext_target[at : at + 16, :] = target[
                    c, 16 * t : 16 * t + 16, 128 * k : 128 * k + 128
                ]
    pack_columns(ext_target)

    load_lists.wait()
    def list_hot(b, carry):
        hot_list[:, pl.ds(pl.multiple_of(b * 256, 256), 256)] = one_hot(
            split_ids(row_pair(lists, b * 2))[1]
        )
        return carry

    lax.fori_loop(0, TILES // 2, list_hot, 0)

    load_cam.wait()
    cam = read_camera(cam_ref)
    load_attr.wait()
    spread_rows(attr, arows)

    def project_step(h, carry):
        rows = [arows[at, :] for at in attr_rows(h)]
        feats = project(rows, cam)
        feats.insert(5, jax.nn.sigmoid(rows[10]))
        for f in range(FEATS):
            table[pl.ds(pl.multiple_of(f * ROWS + h * 8, 8), 8), :] = feats[f]
        return carry

    lax.fori_loop(0, 8, project_step, 0)
    make_parts(table, parts, thirds)

    row_at = lax.broadcasted_iota(I32, (128, 128), 0)
    lane_at = lax.broadcasted_iota(I32, (128, 128), 1)
    before = jnp.where(row_at < lane_at, 1.0, 0.0).astype(BF16)
    after = jnp.where(row_at > lane_at, 1.0, 0.0).astype(BF16)
    for half in range(2):
        tri_before[128 * half : 128 * half + 128, :] = before
        tri_after[128 * half : 128 * half + 128, :] = after

    load_vis.wait()
    load_len.wait()
    pl.semaphore_wait(barrier, DEVICES - 1)

    def send_ids(pi, pc, half, rank, group):
        pltpu.make_async_remote_copy(
            src_ref=vis.at[pl.ds(half, 1)],
            dst_ref=ids_in.at[pl.ds(rank, 1)],
            send_sem=sems.at[0],
            recv_sem=id_sems.at[group],
            device_id=(pi, pc),
            device_id_type=MESH,
        ).start()

    each_step(place, send_ids)
    pltpu.make_async_copy(
        vis.at[pl.ds(me // 2, 1)], ids_in.at[pl.ds(0, 1)], id_sems.at[0]
    ).start()
    border_copies(ext_target, img, cell, sems.at[2], sems.at[3])

    odd = me - (me // 2) * 2
    left = left_half()
    left_row = lax.broadcasted_iota(I32, (1, 128), 1) < 64

    def reply_step(g, carry):
        wait_rows(ids_in, 16, id_sems.at[g])
        at = pl.multiple_of(g * 16, 8)
        first, second = ids_in[pl.ds(at, 8), :], ids_in[pl.ds(at + 8, 8), :]
        even_form = jnp.where(left, first, pltpu.roll(second, 64, 1))
        odd_form = jnp.where(left, pltpu.roll(first, 64, 1), second)
        both = jnp.where(odd == 0, even_form, odd_form)
        ids_own[pl.ds(pl.multiple_of(g * 8, 8), 8), :] = both
        ids = [
            jnp.concatenate([both[2 * n : 2 * n + 1], both[2 * n + 1 : 2 * n + 2]], axis=1)
            for n in range(4)
        ]
        hots = [one_hot(split_ids(v)[1]) for v in ids]
        for n in range(4):
            hot_own[:, pl.ds(pl.multiple_of(g * 1024 + n * 256, 256), 256)] = hots[n]
        got = gather_blocks(parts, thirds, ids, hots)
        for n in range(4):
            for row in range(2):
                d = g * 128 + (2 * n + row) * 8
                for i in range(PAIRS):
                    low = got[n][2 * i][:, 128 * row : 128 * row + 128]
                    high = got[n][min(2 * i + 1, FEATS - 1)][:, 128 * row : 128 * row + 128]
                    msg[pl.ds(d + i, 1), :] = jnp.where(left_row, low, pltpu.roll(high, 64, 1))
                    msg[pl.ds(d + 64 + i, 1), :] = jnp.where(
                        left_row, pltpu.roll(low, 64, 1), high
                    )
        for side in range(2):
            dy = pick(g, [STEPS[2 * n + side][0] for n in range(8)])
            dz = pick(g, [STEPS[2 * n + side][1] for n in range(8)])

            for q, (pi, pc, _) in enumerate(place.devices(dy, dz)):
                copy = pltpu.make_async_remote_copy(
                    src_ref=msg.at[pl.ds(pl.multiple_of(g * 128 + side * 64 + q * 8, 8), PAIRS)],
                    dst_ref=inbox.at[pl.ds(pl.multiple_of(me * 8, 8), PAIRS)],
                    send_sem=sems.at[4],
                    recv_sem=sems.at[5],
                    device_id=(pi, pc),
                    device_id_type=MESH,
                )
                if side == 0 and q == 0:
                    pl.when(g > 0)(copy.start)
                else:
                    copy.start()
        return carry

    lax.fori_loop(0, 8, reply_step, 0)
    own = pl.ds(pl.multiple_of(me * 8, 8), PAIRS)
    inbox[own, :] = msg[0:PAIRS, :]

    wait_rows(ext_target, BORDER_ROWS, sems.at[3])
    for c in range(3):
        for row_block in range(4):
            for half in range(2):
                strips = window(ext_target, img, cell, c, row_block, half)
                for j in range(3):
                    for m, v in ((3, strips[j]), (4, strips[j] * strips[j])):
                        at = map_row(m, c) + 64 * j + 16 * row_block + 8 * half
                        maps[at : at + 8, :] = v

    def target_blur(c, carry):
        for m in range(2):
            for r in range(6):
                at = pl.multiple_of((m * 3 + c) * 48 + 8 * r, 8)
                blurred[pl.ds(at, 8), :] = blur(maps, map_row(3 + m, c) + 6 + 8 * r, 64)
        return carry

    lax.fori_loop(0, 3, target_blur, 0)

    wait_rows(inbox, (DEVICES - 1) * PAIRS, sems.at[5])

    def table_step(h, carry):
        values = unpack_message(
            inbox,
            lambda i: pl.ds(h * 128 + i, 8, stride=16),
            lambda i: pl.ds(h * 128 + 8 + i, 8, stride=16),
        )
        for f in range(FEATS):
            table[pl.ds(pl.multiple_of(f * ROWS + h * 8, 8), 8), :] = values[f]
        return carry

    lax.fori_loop(0, 8, table_step, 0)
    make_parts(table, parts, thirds)

    def list_step(k, carry):
        got = gather_blocks(
            parts,
            thirds,
            [row_pair(lists, k * 16 + 2 * n) for n in range(8)],
            [
                hot_list[:, pl.ds(pl.multiple_of(k * 2048 + n * 256, 256), 256)]
                for n in range(8)
            ],
        )
        for n in range(8):
            for row in range(2):
                for f in range(FEATS):
                    entry[pl.ds(f * TILES + k * 16 + 2 * n + row, 1), :] = got[n][f][
                        :, 128 * row : 128 * row + 128
                    ]
        return carry

    lax.fori_loop(0, 2, list_step, 0)

    def entry_row(f, t):
        return entry[pl.ds(f * TILES + t, 1), :]

    across = lax.broadcasted_iota(I32, (16, 128), 0).astype(F32) + 0.5
    lane_row = lax.broadcasted_iota(I32, (1, 128), 1)

    def spans(tile_row, k):
        return [tile_row * 16 + k * GROUP + n for n in range(GROUP)]

    def pixels_of(t):
        return pl.ds(pl.multiple_of(t * 256, 256), 256)

    for tile_row in range(2):

        def render_step(k, carry, tile_row=tile_row):
            tiles = spans(tile_row, k)
            alphas, sums = [], []
            for n, t in enumerate(tiles):
                alive = lane_row < len_ref[tile_row, k * GROUP + n]
                opacity = jnp.where(alive, entry_row(5, t), 0.0)
                dx = across - entry_row(0, t)
                center_y = entry_row(1, t)
                square_x = (-0.5 * entry_row(2, t)) * dx * dx
                mixed = -entry_row(3, t) * dx
                half_y = -0.5 * entry_row(4, t)
                alpha = []
                for y in range(16):
                    dy = (y + 0.5) - center_y
                    alpha.append(opacity * jnp.exp(square_x + dy * (mixed + half_y * dy)))
                alpha = jnp.concatenate(alpha, axis=0)
                logs = jnp.log(1.0 - alpha)
                sums.append(
                    jnp.dot(
                        jnp.concatenate(two_parts(logs), axis=1),
                        tri_before[...],
                        preferred_element_type=F32,
                    )
                )
                ratio[pixels_of(t), :] = alpha
                alphas.append(alpha)
            products = []
            for n, t in enumerate(tiles):
                weight = jnp.concatenate(two_parts(jnp.exp(sums[n]) * alphas[n]), axis=1)
                weights[pixels_of(t), :] = weight
                colour = [two_parts(entry_row(6 + c, t)) for c in range(3)]
                lhs = jnp.concatenate(
                    [c[part] for part in range(2) for c in colour] + [jnp.zeros((10, 128), BF16)],
                    axis=0,
                )
                products.append(
                    lax.dot_general(
                        jnp.concatenate([lhs, lhs], axis=1),
                        weight,
                        (((1,), (1,)), ((), ())),
                        preferred_element_type=F32,
                    )
                )
            for n in range(GROUP):
                for c in range(3):
                    tile_rows[pl.ds(tile_row * 48 + c * 16 + k * GROUP + n, 1), :] = (
                        products[n][c : c + 1] + products[n][3 + c : 4 + c]
                    )
            return carry

        lax.fori_loop(0, 16 // GROUP, render_step, 0)

    picture = swap_blocks(tile_rows[...])
    for k in range(2):
        ext_render[96 * k : 96 * k + 96, :] = picture[:, 128 * k : 128 * k + 128]
    pack_columns(ext_render)
    border_copies(ext_render, img, cell, sems.at[6], sems.at[7])

    def ratio_step(t, carry):
        alpha = ratio[pixels_of(t), :]
        ratio[pixels_of(t), :] = alpha / (1.0 - alpha)
        return carry

    lax.fori_loop(0, TILES, ratio_step, 0)
    wait_rows(ext_render, BORDER_ROWS, sems.at[7])

    for c in range(3):
        for row_block in range(4):
            for half in range(2):
                strips = window(ext_render, img, cell, c, row_block, half)
                for j in range(3):
                    at = 64 * j + 16 * row_block + 8 * half
                    v = strips[j]
                    wanted = maps[map_row(3, c) + at : map_row(3, c) + at + 8, :]
                    for m, value in ((0, v), (1, v * v), (2, v * wanted)):
                        maps[map_row(m, c) + at : map_row(m, c) + at + 8, :] = value
    row_at = lax.broadcasted_iota(I32, (8, 384), 0) + (img * 32 - 5)
    lane_at = lax.broadcasted_iota(I32, (8, 384), 1) + (cell * 256 - 64)
    inside = (lane_at >= 0) & (lane_at < N_CELL * 256)

    def similarity_step(c, carry):
        for r in range(6):
            mean, square, cross = [blur(maps, map_row(m, c) + 6 + 8 * r, 64) for m in range(3)]
            mean_target, square_target = [
                blurred[pl.ds(pl.multiple_of((m * 3 + c) * 48 + 8 * r, 8), 8), :]
                for m in range(2)
            ]
            _, pullback = jax.vjp(
                lambda x, y, z, mt=mean_target, st=square_target: ssim_value(x, mt, y, st, z),
                mean,
                square,
                cross,
            )
            keep = inside & (row_at + 8 * r >= 0) & (row_at + 8 * r < N_IMG * 32)
            for m, v in enumerate(pullback(jnp.full((8, 384), -WEIGHT_SSIM, F32))):
                v = jnp.where(keep, v, 0.0)
                for j in range(3):
                    at = pl.multiple_of(((m * 3 + c) * 3 + j) * 48 + 8 * r, 8)
                    coefs[pl.ds(at, 8), :] = v[:, 128 * j : 128 * j + 128]
        return carry

    lax.fori_loop(0, 3, similarity_step, 0)
    left = left_half()

    def image_step(c, carry):
        for r in range(4):
            back_mean, back_square, back_cross = [
                blur(coefs, (m * 3 + c) * 3 * 48 + 8 * r, 48) for m in range(3)
            ]
            found = []
            for j in range(3):
                lanes = slice(128 * j, 128 * j + 128)
                at = 64 * j + 16 + 8 * r
                image = maps[pl.ds(pl.multiple_of(map_row(0, c) + at, 8), 8), :]
                wanted = maps[pl.ds(pl.multiple_of(map_row(3, c) + at, 8), 8), :]
                difference = image - wanted
                slope = (
                    (1.0 - WEIGHT_SSIM)
                    * difference
                    / jnp.sqrt(difference * difference + SMOOTHING * SMOOTHING)
                )
                found.append(
                    pltpu.roll(
                        slope
                        + back_mean[:, lanes]
                        + 2.0 * image * back_square[:, lanes]
                        + wanted * back_cross[:, lanes],
                        64,
                        1,
                    )
                )
            at = pl.multiple_of((r // 2) * 48 + c * 16 + (r % 2) * 8, 8)
            tile_rows[pl.ds(at, 8), :] = jnp.concatenate(
                [jnp.where(left, found[0], found[1]), jnp.where(left, found[1], found[2])],
                axis=1,
            )
        return carry

    lax.fori_loop(0, 3, image_step, 0)
    tile_rows[...] = swap_blocks(tile_rows[...])

    for tile_row in range(2):

        def back_step(k, carry, tile_row=tile_row):
            tiles = spans(tile_row, k)
            grad_rows, values = [], []
            for n, t in enumerate(tiles):
                pixel_grad = [
                    two_parts(tile_rows[pl.ds(tile_row * 48 + c * 16 + k * GROUP + n, 1), :])
                    for c in range(3)
                ]
                colour = [two_parts(entry_row(6 + c, t)) for c in range(3)]
                tops, lows = [g[0] for g in pixel_grad], [g[1] for g in pixel_grad]
                grad_rows.append(
                    jnp.concatenate(tops + lows + tops + [jnp.zeros((7, 256), BF16)], axis=0)
                )
                colour_rows = jnp.concatenate(
                    [c[0] for c in colour] * 2
                    + [c[1] for c in colour]
                    + [jnp.zeros((7, 128), BF16)],
                    axis=0,
                )
                values.append(
                    lax.dot_general(
                        grad_rows[n],
                        colour_rows,
                        (((0,), (0,)), ((), ())),
                        preferred_element_type=F32,
                    )
                )
            gains, laters, mixes = [], [], []
            for n, t in enumerate(tiles):
                weight = weights[pixels_of(t), :]
                mixes.append(jnp.dot(grad_rows[n], weight, preferred_element_type=F32))
                gain = values[n] * (weight[:, :128].astype(F32) + weight[:, 128:].astype(F32))
                laters.append(
                    jnp.dot(
                        jnp.concatenate(two_parts(gain), axis=1),
                        tri_after[...],
                        preferred_element_type=F32,
                    )
                )
                gains.append(gain)
            for n, t in enumerate(tiles):
                pull = gains[n] - ratio[pixels_of(t), :] * laters[n]
                dx = across - entry_row(0, t)
                center_y = entry_row(1, t)
                sum_0 = sum_y = sum_yy = None
                for y in range(16):
                    dy = (y + 0.5) - center_y
                    part = pull[16 * y : 16 * y + 16]
                    part_y = part * dy
                    part_yy = part_y * dy
                    sum_0 = part if y == 0 else sum_0 + part
                    sum_y = part_y if y == 0 else sum_y + part_y
                    sum_yy = part_yy if y == 0 else sum_yy + part_yy
                sum_x = sum_0 * dx
                found = [sum_0, sum_x, sum_y, sum_x * dx, sum_y * dx, sum_yy]
                for m in range(6):
                    moments[pl.ds(m * TILES + t, 1), :] = jnp.sum(
                        found[m], axis=0, keepdims=True
                    )
                for c in range(3):
                    both = mixes[n][c : c + 1] + mixes[n][3 + c : 4 + c]
                    moments[pl.ds((6 + c) * TILES + t, 1), :] = both[:, :128] + both[:, 128:]
            return carry

        lax.fori_loop(0, 16 // GROUP, back_step, 0)

    feat = [entry[f * TILES : (f + 1) * TILES, :] for f in range(6)]
    mom = [moments[m * TILES : (m + 1) * TILES, :] for m in range(6)]
    entry[0:TILES, :] = feat[2] * mom[1] + feat[3] * mom[2]
    entry[TILES : 2 * TILES, :] = feat[3] * mom[1] + feat[4] * mom[2]
    entry[2 * TILES : 3 * TILES, :] = -0.5 * mom[3]
    entry[3 * TILES : 4 * TILES, :] = -mom[4]
    entry[4 * TILES : 5 * TILES, :] = -0.5 * mom[5]
    entry[5 * TILES : 6 * TILES, :] = mom[0]
    entry[6 * TILES : 9 * TILES, :] = moments[6 * TILES : 9 * TILES, :]

    acc[...] = jnp.zeros_like(acc)

    def slot_step(k, carry):
        at = [k * 2 * BLOCKS + 2 * n for n in range(BLOCKS)]
        scatter_blocks(
            [row_pair(lists, a) for a in at],
            [[row_pair(entry, f * TILES + a) for f in range(FEATS)] for a in at],
            hot_list[:, pl.ds(pl.multiple_of(k * 256 * BLOCKS, 256), 256 * BLOCKS)],
            acc,
        )
        return carry

    lax.fori_loop(0, TILES // (2 * BLOCKS), slot_step, 0)

    def total_rows(f, h):
        a = acc[pl.ds(pl.multiple_of(f * 32 + h * 8, 8), 8), :]
        b = acc[pl.ds(pl.multiple_of(288 + f * 32 + h * 8, 8), 8), :]
        return a + b

    def back_pack(h, carry):
        totals = [total_rows(f, h) for f in range(FEATS)]
        for half in range(2):
            pack_message(
                [v[:, 128 * half : 128 * half + 128] for v in totals],
                msg_back,
                lambda i: pl.ds(h * 256 + (2 * half) * 8 + i, 8, stride=32),
                lambda i: pl.ds(h * 256 + (2 * half + 1) * 8 + i, 8, stride=32),
            )
        return carry

    lax.fori_loop(0, 4, back_pack, 0)

    def send_back(pi, pc, half, rank, group):
        pltpu.make_async_remote_copy(
            src_ref=msg_back.at[pl.ds(pl.multiple_of((pi * N_CELL + pc) * 8, 8), PAIRS)],
            dst_ref=inbox_back.at[pl.ds(pl.multiple_of(rank * 8, 8), PAIRS)],
            send_sem=sems.at[8],
            recv_sem=back_sems.at[group],
            device_id=(pi, pc),
            device_id_type=MESH,
        ).start()

    each_step(place, send_back)
    pltpu.make_async_copy(
        msg_back.at[own], inbox_back.at[pl.ds(0, PAIRS)], back_sems.at[0]
    ).start()

    acc[...] = jnp.zeros_like(acc)

    def owner_step(k, carry):
        for side in range(BLOCKS // 4):
            g = k * (BLOCKS // 4) + side
            wait_rows(inbox_back, 16 * PAIRS, back_sems.at[g])
            values = unpack_message(
                inbox_back,
                lambda i: pl.ds(g * 128 + i, 8, stride=8),
                lambda i: pl.ds(g * 128 + 64 + i, 8, stride=8),
            )
            for f in range(FEATS):
                table[pl.ds(pl.multiple_of(f * ROWS + g * 8, 8), 8), :] = values[f]
        at = [k * 2 * BLOCKS + 2 * n for n in range(BLOCKS)]
        scatter_blocks(
            [row_pair(ids_own, a) for a in at],
            [[row_pair(table, f * ROWS + a) for f in range(FEATS)] for a in at],
            hot_own[:, pl.ds(pl.multiple_of(k * 256 * BLOCKS, 256), 256 * BLOCKS)],
            acc,
        )
        return carry

    lax.fori_loop(0, ROWS // (2 * BLOCKS), owner_step, 0)

    def finish(h, carry):
        for f in range(FEATS):
            v = total_rows(f, h)
            for half in range(2):
                out[pl.ds(f * ROWS + h * 16 + half, 8, stride=2), :] = v[
                    :, 128 * half : 128 * half + 128
                ]
        return carry

    lax.fori_loop(0, 4, finish, 0)

    wait_rows(ids_in, DEVICES - 1, sems.at[0])
    wait_rows(ext_target, BORDER_ROWS, sems.at[2])
    wait_rows(msg, (DEVICES - 1) * PAIRS, sems.at[4])
    wait_rows(ext_render, BORDER_ROWS, sems.at[6])
    wait_rows(msg_back, (DEVICES - 1) * PAIRS, sems.at[8])


def pullback_kernel(
    cam_hbm,
    attr_hbm,
    grad_hbm,
    out_hbm,
    cam_ref,
    attr,
    feat_grad,
    arows,
    result,
    load_sems,
    save_sem,
):
    def block(h):
        return pl.ds(pl.multiple_of(h * 1024, 1024), 1024)

    def load(h):
        return pltpu.make_async_copy(
            attr_hbm.at[:, block(h)], attr.at[:, block(h)], load_sems.at[h]
        )

    load_cam = pltpu.make_async_copy(cam_hbm, cam_ref, load_sems.at[8])
    load_grad = pltpu.make_async_copy(grad_hbm, feat_grad, load_sems.at[9])
    load(0).start()
    load_cam.start()
    load_grad.start()
    for h in range(1, 8):
        load(h).start()
    load_cam.wait()
    load_grad.wait()
    cam = read_camera(cam_ref)

    def step(h, carry):
        load(h).wait()
        for k in range(8):
            lanes = pl.ds(pl.multiple_of(h * 1024 + k * 128, 128), 128)
            for g in range(8):
                n = min(8, ATTRS - 8 * g)
                arows[g * 64 + 8 * k : g * 64 + 8 * k + n, :] = attr[8 * g : 8 * g + n, lanes]
        places = [pl.ds((r // 8) * 64 + r % 8, 8, stride=8) for r in range(ATTRS)]
        rows = [arows[at, :] for at in places]
        _, pullback = jax.vjp(lambda r: project(r, cam), rows)
        grads = [
            feat_grad[pl.ds(pl.multiple_of(f * ROWS + h * 8, 8), 8), :] for f in range(FEATS)
        ]
        log_opacity = grads.pop(5)
        (found,) = pullback(grads)
        found[10] = log_opacity * (1.0 - jax.nn.sigmoid(rows[10]))
        for at, v in zip(places, found):
            arows[at, :] = v
        for k in range(8):
            lanes = pl.ds(pl.multiple_of(h * 1024 + k * 128, 128), 128)
            for g in range(8):
                n = min(8, ATTRS - 8 * g)
                result[8 * g : 8 * g + n, lanes] = arows[g * 64 + 8 * k : g * 64 + 8 * k + n, :]
        pltpu.make_async_copy(result.at[:, block(h)], out_hbm.at[:, block(h)], save_sem).start()
        return carry

    lax.fori_loop(0, 8, step, 0)
    pltpu.make_async_copy(result, out_hbm, save_sem).wait()


def shards(attributes, camera, target, visible_index, tile_lists, tile_len):
    vmem = pl.BlockSpec(memory_space=pltpu.VMEM)
    anywhere = pl.BlockSpec(memory_space=pl.ANY)
    feat_grad = pl.pallas_call(
        step_kernel,
        out_shape=jax.ShapeDtypeStruct((FEATS * ROWS, 128), F32),
        in_specs=[anywhere] * 6,
        out_specs=vmem,
        scratch_shapes=[
            pltpu.SMEM((3, 3), F32),
            pltpu.SMEM((2, 16), I32),
            pltpu.VMEM((ROWS, 128), I32),
            pltpu.VMEM((3, 32, 256), F32),
            pltpu.VMEM((TILES, LIST), I32),
            pltpu.VMEM((ATTRS, 8192), F32),
            pltpu.VMEM((4096, 128), F32),
            pltpu.VMEM((FEATS * ROWS, 128), F32),
            pltpu.VMEM((FEATS * 32, 512), BF16),
            pltpu.VMEM((EXACT * 32, 256), BF16),
            pltpu.VMEM((256, TILES * LIST), BF16),
            pltpu.VMEM((256, ROWS * 128), BF16),
            pltpu.VMEM((DEVICES, 128), I32),
            pltpu.VMEM((ROWS, 128), I32),
            pltpu.VMEM((DEVICES * 8, 128), F32),
            pltpu.VMEM((DEVICES * 8, 128), F32),
            pltpu.VMEM((DEVICES * 8, 128), F32),
            pltpu.VMEM((DEVICES * 8, 128), F32),
            pltpu.VMEM((EXT_ROWS, 128), F32),
            pltpu.VMEM((EXT_ROWS, 128), F32),
            pltpu.VMEM((FEATS * TILES, 128), F32),
            pltpu.VMEM((256, 128), BF16),
            pltpu.VMEM((256, 128), BF16),
            pltpu.VMEM((TILES * 256, 256), BF16),
            pltpu.VMEM((TILES * 256, 128), F32),
            pltpu.VMEM((96, 256), F32),
            pltpu.VMEM((FEATS * TILES, 128), F32),
            pltpu.VMEM((5 * 3 * 3 * 64, 128), F32),
            pltpu.VMEM((3 * 3 * 3 * 48, 128), F32),
            pltpu.VMEM((2 * 3 * 48, 384), F32),
            pltpu.VMEM((2 * FEATS * 32, 256), F32),
            pltpu.SemaphoreType.DMA((10,)),
            pltpu.SemaphoreType.DMA((8,)),
            pltpu.SemaphoreType.DMA((8,)),
            pltpu.SemaphoreType.DMA((6,)),
        ],
        compiler_params=pltpu.CompilerParams(
            collective_id=0, has_side_effects=True, vmem_limit_bytes=58 * 1024 * 1024
        ),
        name="splat_step",
    )(
        camera,
        tile_len,
        visible_index.reshape(ROWS, 128),
        attributes,
        target,
        tile_lists.reshape(TILES, LIST),
    )
    return pl.pallas_call(
        pullback_kernel,
        out_shape=jax.ShapeDtypeStruct(attributes.shape, F32),
        in_specs=[anywhere] * 3,
        out_specs=anywhere,
        scratch_shapes=[
            pltpu.SMEM((3, 3), F32),
            pltpu.VMEM((ATTRS, 8192), F32),
            pltpu.VMEM((FEATS * ROWS, 128), F32),
            pltpu.VMEM((512, 128), F32),
            pltpu.VMEM((ATTRS, 8192), F32),
            pltpu.SemaphoreType.DMA((10,)),
            pltpu.SemaphoreType.DMA,
        ],
        name="splat_pullback",
    )(camera, attributes, feat_grad)


def solution(mesh):
    return jax.shard_map(
        shards,
        mesh=mesh,
        in_specs=(
            P(None, ("img", "cell")),
            P(),
            P(None, "img", "cell"),
            P(("img", "cell"), None),
            P("img", "cell", None),
            P("img", "cell"),
        ),
        out_specs=P(None, ("img", "cell")),
        check_vma=False,
    )
```
